32 devices in a mesh: seq: 4 (over z), ctx: 8 (over y, x, core).
Axes of the slice: x: 2, y: 2, z: 4, core: 2. Of those that a mesh axis runs over, the one named last changes fastest.
Arguments:
- hidden_states: bfloat16 [4, 1024, 1024], P('seq', 'ctx'), may hold values from -6 to 6
- positions: int32 [4, 1024], P('seq'), may hold values from 0 to 1023, as said below
- gain_first: bfloat16 [1024], P(('seq', 'ctx')), may hold values from 0.25 to 1.75
- weight_query: bfloat16 [1024, 2048], P(('seq', 'ctx')), may hold values from -0.1875 to 0.1875
- key_weight_matrix: bfloat16 [1024, 1024], P(('seq', 'ctx')), may hold values from -0.1875 to 0.1875
- value_weight_matrix: bfloat16 [1024, 1024], P(('seq', 'ctx')), may hold values from -0.1875 to 0.1875
- gain_query: bfloat16 [128], P(('seq', 'ctx')), may hold values from 0.25 to 1.75
- gain_key: bfloat16 [128], P(('seq', 'ctx')), may hold values from 0.25 to 1.75
- weight_output: bfloat16 [2048, 1024], P(('seq', 'ctx')), may hold values from -2 to 2
- gain_second: bfloat16 [1024], P(('seq', 'ctx')), may hold values from 0.25 to 1.75
- weight_gate: bfloat16 [1024, 3072], P(('seq', 'ctx')), may hold values from -0.1875 to 0.1875
- weight_up: bfloat16 [1024, 3072], P(('seq', 'ctx')), may hold values from -0.1875 to 0.1875
- weight_down: bfloat16 [3072, 1024], P(('seq', 'ctx')), may hold values from -0.109375 to 0.109375
- output_cotangent: bfloat16 [4, 1024, 1024], P('seq', 'ctx'), may hold values from -6 to 6
Outputs:
- layer_output: bfloat16 [4, 1024, 1024], P('seq', 'ctx')
- hidden_gradient: float32 [4, 1024, 1024], P('seq', 'ctx')
- change_first: float32 [1024], P(('seq', 'ctx'))
- delta_query: float32 [1024, 2048], P(('seq', 'ctx'))
- delta_key: float32 [1024, 1024], P(('seq', 'ctx'))
- delta_value: float32 [1024, 1024], P(('seq', 'ctx'))
- change_query: float32 [128], P(('seq', 'ctx'))
- change_key: float32 [128], P(('seq', 'ctx'))
- delta_output: float32 [2048, 1024], P(('seq', 'ctx'))
- change_second: float32 [1024], P(('seq', 'ctx'))
- delta_gate: float32 [1024, 3072], P(('seq', 'ctx'))
- delta_up: float32 [1024, 3072], P(('seq', 'ctx'))
- delta_down: float32 [3072, 1024], P(('seq', 'ctx'))
The draws below stay inside these ranges and needn't reach their ends.
Inputs may be any that keep to these rules, and one draw needn't show every extreme that they name: In every sequence each position 0 to 1023 occurs once; the 128 stored tokens of one device of ctx are two runs of 64 consecutive ascending positions, each run starting at a multiple of 64, and their two run numbers sum to 15.
All inputs are finite; a program needn't handle non-finite values.
Results may differ from the reference program's by a relative error of at most 0.023.
Values may be sent and summed in bfloat16 or wider, within the bound.
A program may use at most 104 MiB of HBM per device.

```python
import jax
import jax.numpy as jnp
from jax import lax

MODEL_WIDTH = 1024
QUERY_HEAD_COUNT = 16
KEY_VALUE_HEADS = 8
HEAD_DIMENSION = 128
FF = 3072
TOK_DEV = 128
BATCH = 4
L = 1024


def draw_positions(key, part):
    members = L // TOK_DEV
    half_block = TOK_DEV // 2
    offsets = jnp.arange(half_block, dtype=jnp.int32)

    def one_sequence(sequence_key):
        order_key, flip_key = jax.random.split(sequence_key)
        first_block = jax.random.permutation(order_key, members).astype(jnp.int32)
        second_block = 2 * members - 1 - first_block
        flipped = jax.random.randint(flip_key, (members,), 0, 2).astype(jnp.int32)
        first_run = jnp.where(flipped == 1, second_block, first_block)
        second_run = jnp.where(flipped == 1, first_block, second_block)
        block_runs = jnp.stack([first_run, second_run], axis=1)
        places = block_runs[:, :, None] * half_block + offsets[None, None, :]
        return places.reshape(members * TOK_DEV)
    sequence_keys = jax.random.split(key, BATCH)
    return jax.vmap(one_sequence)(sequence_keys).astype(jnp.int32)


def shard_levels(stream_key, dims, pieces, low, top_value):
    level = 1.0
    for axis_at, blocks in pieces:
        heights = jax.random.uniform(jax.random.fold_in(jax.random.fold_in(stream_key, 6), axis_at), (blocks,), jnp.float32, low / len(pieces), top_value / len(pieces))
        level = level * jnp.repeat(jnp.exp(heights), dims[axis_at] // blocks).reshape((-1,) + (1,) * (len(dims) - 1 - axis_at))
    return level


def bell_draw(stream_key, shape, spread, most, cuts=(), kind=jnp.bfloat16):
    array = spread * jax.random.normal(stream_key, shape, jnp.float32)
    if cuts:
        array = array * shard_levels(stream_key, shape, cuts, -0.22, 0.18)
    return jnp.clip(array, -most, most).astype(kind)


def setup_inputs(seed: int = 0) -> dict:
    keys = jax.random.split(jax.random.key(seed), 15)
    hidden_states = bell_draw(keys[0], (BATCH, L, MODEL_WIDTH), 1.0, 6.0, ((0, 4), (1, 8)))
    positions = draw_positions(jax.random.fold_in(keys[14], 71), 0)
    gain_first = jnp.clip(1.0 + 0.15 * jax.random.normal(keys[2], (MODEL_WIDTH,), jnp.float32), 0.25, 1.75).astype(jnp.bfloat16)
    weight_query = bell_draw(keys[3], (MODEL_WIDTH, QUERY_HEAD_COUNT * HEAD_DIMENSION), MODEL_WIDTH ** -0.5, 0.1875, ((0, 32),))
    key_weight_matrix = bell_draw(keys[4], (MODEL_WIDTH, KEY_VALUE_HEADS * HEAD_DIMENSION), MODEL_WIDTH ** -0.5, 0.1875, ((0, 32),))
    value_weight_matrix = bell_draw(keys[5], (MODEL_WIDTH, KEY_VALUE_HEADS * HEAD_DIMENSION), MODEL_WIDTH ** -0.5, 0.1875, ((0, 32),))
    gain_query = jnp.clip(1.0 + 0.15 * jax.random.normal(keys[6], (HEAD_DIMENSION,), jnp.float32), 0.25, 1.75).astype(jnp.bfloat16)
    gain_key = jnp.clip(1.0 + 0.15 * jax.random.normal(keys[7], (HEAD_DIMENSION,), jnp.float32), 0.25, 1.75).astype(jnp.bfloat16)
    weight_output = bell_draw(keys[8], (QUERY_HEAD_COUNT * HEAD_DIMENSION, MODEL_WIDTH), (max(QUERY_HEAD_COUNT * HEAD_DIMENSION // 256, 1)) ** -0.5, 2.0, ((0, 32),))
    gain_second = jnp.clip(1.0 + 0.15 * jax.random.normal(keys[9], (MODEL_WIDTH,), jnp.float32), 0.25, 1.75).astype(jnp.bfloat16)
    weight_gate = bell_draw(keys[10], (MODEL_WIDTH, FF), MODEL_WIDTH ** -0.5, 0.1875, ((0, 32),))
    weight_up = bell_draw(keys[11], (MODEL_WIDTH, FF), MODEL_WIDTH ** -0.5, 0.1875, ((0, 32),))
    weight_down = bell_draw(keys[12], (FF, MODEL_WIDTH), FF ** -0.5, 0.109375, ((0, 32),))
    output_cotangent = bell_draw(keys[13], (BATCH, L, MODEL_WIDTH), 1.0, 6.0, ((0, 4), (1, 8)))
    return dict(hidden_states=hidden_states, positions=positions, gain_first=gain_first, weight_query=weight_query, key_weight_matrix=key_weight_matrix, value_weight_matrix=value_weight_matrix, gain_query=gain_query, gain_key=gain_key, weight_output=weight_output, gain_second=gain_second, weight_gate=weight_gate, weight_up=weight_up, weight_down=weight_down, output_cotangent=output_cotangent)


@jax.custom_vjp
def low(v):
    return lax.optimization_barrier(v.astype(jnp.bfloat16)).astype(jnp.float32)

@jax.custom_vjp
def low_back(v):
    return v

def low_keep(v):
    return (low(v), None)

def low_pass(kept, grad):
    return (grad,)

def back_keep(v):
    return (v, None)

def back_low(kept, grad):
    return (low(grad),)
low.defvjp(low_keep, low_pass)
low_back.defvjp(back_keep, back_low)
EPS = 1e-06
THETA = 1000000.0
NEGATIVE = -1e+30

def matrix_product(left, right):
    return jnp.dot(left, right, precision=lax.Precision.HIGHEST)

def normalize(values):
    return values * lax.rsqrt(lax.optimization_barrier(jnp.mean(values * values, axis=-1, keepdims=True)) + EPS)

def angles(places):
    half_size = HEAD_DIMENSION // 2
    frequency = jnp.power(THETA, -jnp.arange(half_size, dtype=jnp.float32) * (2.0 / HEAD_DIMENSION))
    phases = places.astype(jnp.float32)[:, None] * frequency[None, :]
    phases = jnp.concatenate([phases, phases], axis=-1)
    return (jnp.cos(phases), jnp.sin(phases))

def rotate(values, cosines, sines):
    half_size = values.shape[-1] // 2
    turned = jnp.concatenate([-values[..., half_size:], values[..., :half_size]], axis=-1)
    return values * cosines + turned * sines

def layer_forward(sequence, places, gain_first, weight_query, key_weight_matrix, value_weight_matrix, gain_query, gain_key, weight_output, gain_second, weight_gate, weight_up, weight_down):
    sequence_length = sequence.shape[0]
    group_width = QUERY_HEAD_COUNT // KEY_VALUE_HEADS
    leading_input = low(normalize(sequence) * gain_first)
    query_linear = low_back(matrix_product(leading_input, weight_query)).reshape(sequence_length, QUERY_HEAD_COUNT, HEAD_DIMENSION)
    key_projected = low_back(matrix_product(leading_input, key_weight_matrix)).reshape(sequence_length, KEY_VALUE_HEADS, HEAD_DIMENSION)
    value_hidden = low(low_back(matrix_product(leading_input, value_weight_matrix))).reshape(sequence_length, KEY_VALUE_HEADS, HEAD_DIMENSION)
    cosines, sines = angles(places)
    rotary_query = low(rotate(normalize(query_linear) * gain_query, cosines[:, None, :], sines[:, None, :]))
    key_rotated = low(rotate(normalize(key_projected) * gain_key, cosines[:, None, :], sines[:, None, :]))
    causal_mask = places[None, :] <= places[:, None]
    query_grouping = jnp.transpose(rotary_query.reshape(sequence_length, KEY_VALUE_HEADS, group_width, HEAD_DIMENSION), (1, 0, 2, 3))
    key_groups = jnp.transpose(key_rotated, (1, 0, 2))
    value_groups = jnp.transpose(value_hidden, (1, 0, 2))

    def head_attention(block):
        query_block, key_block, value_block = block
        raw_scores = low_back(jnp.einsum('qgd,kd->gqk', query_block, key_block, precision=lax.Precision.HIGHEST)) * HEAD_DIMENSION ** (-0.5)
        scores = jnp.where(causal_mask[None], raw_scores, NEGATIVE)
        weights = jax.nn.softmax(scores, axis=-1)
        return jnp.einsum('gqk,kd->qgd', low(weights), value_block, precision=lax.Precision.HIGHEST)
    head_outputs = lax.map(jax.checkpoint(head_attention), (query_grouping, key_groups, value_groups))
    attention = jnp.transpose(head_outputs, (1, 0, 2, 3)).reshape(sequence_length, QUERY_HEAD_COUNT * HEAD_DIMENSION)
    attention = low_back(low(attention))
    middle = sequence + low_back(matrix_product(attention, weight_output))
    second_input = low(normalize(middle) * gain_second)
    gate_linear = low_back(matrix_product(second_input, weight_gate))
    up_linear = low_back(matrix_product(second_input, weight_up))
    activation = low(jax.nn.silu(gate_linear) * up_linear)
    return middle + low_back(matrix_product(activation, weight_down))

def reference(hidden_states, positions, gain_first, weight_query, key_weight_matrix, value_weight_matrix, gain_query, gain_key, weight_output, gain_second, weight_gate, weight_up, weight_down, output_cotangent):
    params = (gain_first.astype(jnp.float32), weight_query.astype(jnp.float32), key_weight_matrix.astype(jnp.float32), value_weight_matrix.astype(jnp.float32), gain_query.astype(jnp.float32), gain_key.astype(jnp.float32), weight_output.astype(jnp.float32), gain_second.astype(jnp.float32), weight_gate.astype(jnp.float32), weight_up.astype(jnp.float32), weight_down.astype(jnp.float32))
    inputs = hidden_states.astype(jnp.float32)

    def forward(states, *weights):

        def one_sequence(block):
            sequence, places = block
            return layer_forward(sequence, places, *weights)
        return lax.map(jax.checkpoint(one_sequence), (states, positions))
    output, pullback = jax.vjp(forward, inputs, *params)
    grads = pullback(output_cotangent.astype(jnp.float32))
    return (output.astype(jnp.bfloat16), grads[0], grads[1], grads[2], grads[3], grads[4], grads[5], grads[6], grads[7], grads[8], grads[9], grads[10], grads[11])
```

```python
import jax
import jax.numpy as jnp
from jax import lax
from jax.sharding import PartitionSpec as P

QUERY_HEAD_COUNT = 16
KEY_VALUE_HEADS = 8
HEAD_DIMENSION = 128

EPS = 1e-06
THETA = 1000000.0
NEGATIVE = -1e30
BF = jnp.bfloat16
F32 = jnp.float32


def inverse_root(values):
    return lax.rsqrt(jnp.mean(values * values, axis=-1, keepdims=True) + EPS)


def angles(places, head_size):
    half_size = head_size // 2
    frequency = jnp.power(THETA, -jnp.arange(half_size, dtype=F32) * (2.0 / head_size))
    phases = places.astype(F32)[:, None] * frequency[None, :]
    phases = jnp.concatenate([phases, phases], axis=-1)
    return (jnp.cos(phases), jnp.sin(phases))


def rotate(values, cosines, sines):
    half_size = values.shape[-1] // 2
    turned = jnp.concatenate([-values[..., half_size:], values[..., :half_size]], axis=-1)
    return values * cosines + turned * sines


def rotate_back(upstream, cosines, sines):
    half_size = upstream.shape[-1] // 2
    scaled = upstream * sines
    turned = jnp.concatenate([scaled[..., half_size:], -scaled[..., :half_size]], axis=-1)
    return upstream * cosines + turned


def norm_backward(normed_grad, normed, inverse):
    return inverse * (normed_grad - normed * jnp.mean(normed_grad * normed, axis=-1, keepdims=True))


def dot(a, b):
    return jnp.dot(a, b, preferred_element_type=F32)


def local_of(mesh):
    seqs, ranks = mesh.shape["seq"], mesh.shape["ctx"]
    devices = seqs * ranks
    axes = ("seq", "ctx")

    def spread(shard, heads):
        rows, columns = shard.shape
        if heads and heads < ranks:
            blocks = shard.reshape(rows, heads, 1, columns // heads)
            blocks = jnp.broadcast_to(blocks, (rows, heads, ranks // heads, columns // heads))
            return blocks.reshape(rows, ranks, columns // heads)
        return shard.reshape(rows, ranks, columns // ranks)

    def fold(blocks, heads):
        rows, count, width = blocks.shape
        if heads and heads < ranks:
            return blocks.reshape(rows, heads, count // heads, width).sum(2).reshape(rows, heads * width)
        return blocks.reshape(rows, count * width)

    forth = [(seqs * r + j, j * ranks + r) for r in range(ranks) for j in range(seqs)]
    back = [(b, a) for a, b in forth]

    def local(
        hidden_states, positions, gain_first, weight_query, key_weight_matrix, value_weight_matrix,
        gain_query, gain_key, weight_output, gain_second, weight_gate, weight_up, weight_down,
        output_cotangent,
    ):
        tokens = hidden_states.shape[1]
        length = positions.shape[1]
        size = HEAD_DIMENSION
        group = QUERY_HEAD_COUNT // KEY_VALUE_HEADS
        my_q = QUERY_HEAD_COUNT // ranks
        my_k = max(1, KEY_VALUE_HEADS // ranks)
        scale = size ** (-0.5)
        places = positions[0]
        cosines, sines = angles(places, size)
        cosines, sines = cosines[:, None, :], sines[:, None, :]

        gains = jnp.concatenate([gain_first, gain_second, gain_query, gain_key])
        gains = lax.all_gather(gains, axes, axis=0).astype(F32)
        n1, n2, n3, n4 = (g.shape[0] for g in (gain_first, gain_second, gain_query, gain_key))
        first_scale = gains[:, :n1].reshape(-1)
        second_scale = gains[:, n1 : n1 + n2].reshape(-1)
        query_scale = gains[:, n1 + n2 : n1 + n2 + n3].reshape(-1)
        key_scale = gains[:, n1 + n2 + n3 :].reshape(-1)

        column_weights = jnp.concatenate(
            [
                spread(weight_query, 0),
                spread(key_weight_matrix, KEY_VALUE_HEADS),
                spread(value_weight_matrix, KEY_VALUE_HEADS),
                spread(weight_gate, 0),
                spread(weight_up, 0),
            ],
            axis=2,
        )
        column_weights = lax.all_to_all(column_weights, "ctx", split_axis=1, concat_axis=0, tiled=True)
        column_weights = lax.all_gather(column_weights[:, 0], "seq", axis=0, tiled=True)
        row_weights = jnp.concatenate([weight_output, weight_down], axis=0)
        row_weights = lax.all_gather(lax.ppermute(row_weights, axes, forth), "seq", axis=0)
        o_rows, d_rows = weight_output.shape[0], weight_down.shape[0]
        width = weight_output.shape[1]
        w_o = row_weights[:, :o_rows].reshape(-1, width)
        w_d = row_weights[:, o_rows:].reshape(-1, width)
        units = w_d.shape[0]
        attn_columns = (my_q + 2 * my_k) * size
        w_qkv = column_weights[:, :attn_columns]
        w_gu = column_weights[:, attn_columns:]

        x = lax.all_gather(hidden_states[0], "ctx", axis=0, tiled=True).astype(F32)
        g_low = lax.all_gather(output_cotangent[0], "ctx", axis=0, tiled=True)
        first_inverse = inverse_root(x)
        h1 = (x * first_inverse * first_scale).astype(BF)
        qkv = dot(h1, w_qkv)
        q_lin = qkv[:, : my_q * size].reshape(length, my_q, size)
        k_lin = qkv[:, my_q * size : (my_q + my_k) * size].reshape(length, my_k, size)
        v = qkv[:, (my_q + my_k) * size :].astype(BF).reshape(length, my_k, size)
        rq, rk = inverse_root(q_lin), inverse_root(k_lin)
        nq, nk = q_lin * rq, k_lin * rk
        qr = rotate(nq * query_scale, cosines, sines).astype(BF)
        kr = rotate(nk * key_scale, cosines, sines).astype(BF)
        mask = places[None, :] <= places[:, None]

        def scores(h):
            e = lax.dot_general(
                qr[:, h], kr[:, h // group], (((1,), (1,)), ((), ())), preferred_element_type=F32
            )
            return jnp.where(mask, e * scale, NEGATIVE)

        outs, probs = [], []
        for h in range(my_q):
            e = scores(h)
            p = jnp.exp(e - jnp.max(e, axis=-1, keepdims=True))
            p = p / jnp.sum(p, axis=-1, keepdims=True)
            probs.append(p)
            outs.append(dot(p.astype(BF), v[:, h // group]))
        o = jnp.concatenate(outs, axis=1).astype(BF)

        def scatter(part):
            return lax.psum_scatter(part.astype(BF), "ctx", scatter_dimension=0, tiled=True).astype(F32)

        x_own = hidden_states[0].astype(F32)
        y1 = x_own + scatter(dot(o, w_o))
        r2 = inverse_root(y1)
        second_normed = y1 * r2
        h2 = lax.all_gather((second_normed * second_scale).astype(BF), "ctx", axis=0, tiled=True)
        gu = dot(h2, w_gu)
        gate, up = gu[:, :units], gu[:, units:]
        sig = jax.nn.sigmoid(gate)
        silu = gate * sig
        act = (silu * up).astype(BF)
        layer_output = (y1 + scatter(dot(act, w_d))).astype(BF)

        d_act = dot(g_low, w_d.T)
        d_gate = (d_act * up * sig * (1.0 + gate * (1.0 - sig))).astype(BF)
        d_up = (d_act * silu).astype(BF)
        d_gu = jnp.concatenate([d_gate, d_up], axis=1)
        d_h2 = scatter(dot(d_gu, w_gu.T))
        second_term = jnp.sum(d_h2 * second_normed, axis=0)
        d_y1 = output_cotangent[0].astype(F32) + norm_backward(d_h2 * second_scale, second_normed, r2)
        d_y1_low = lax.all_gather(d_y1.astype(BF), "ctx", axis=0, tiled=True)
        d_o = dot(d_y1_low, w_o.T).astype(BF).reshape(length, my_q, size)

        d_q, d_k, d_v = [], [0.0] * my_k, [0.0] * my_k
        for h in range(my_q):
            p = probs[h]
            dp = lax.dot_general(
                d_o[:, h], v[:, h // group], (((1,), (1,)), ((), ())), preferred_element_type=F32
            )
            row = jnp.sum(p * dp, axis=-1, keepdims=True)
            de = (p * (dp - row) * scale).astype(BF)
            d_q.append(dot(de, kr[:, h // group]))
            d_k[h // group] += dot(de.T, qr[:, h])
            d_v[h // group] += dot(p.astype(BF).T, d_o[:, h])
        d_q, d_k, d_v = jnp.stack(d_q, 1), jnp.stack(d_k, 1), jnp.stack(d_v, 1)
        d_gq, d_gk = rotate_back(d_q, cosines, sines), rotate_back(d_k, cosines, sines)
        query_term = jnp.sum(d_gq * nq, axis=(0, 1))
        key_term = jnp.sum(d_gk * nk, axis=(0, 1))
        d_qlin = norm_backward(d_gq * query_scale, nq, rq).reshape(length, -1)
        d_klin = norm_backward(d_gk * key_scale, nk, rk).reshape(length, -1)
        d_qkv = jnp.concatenate([d_qlin, d_klin, d_v.reshape(length, -1)], axis=1).astype(BF)
        d_h1 = scatter(dot(d_qkv, w_qkv.T))
        r1 = inverse_root(x_own)
        first_normed = x_own * r1
        first_term = jnp.sum(d_h1 * first_normed, axis=0)
        hidden_gradient = d_y1 + norm_backward(d_h1 * first_scale, first_normed, r1)

        def rows_sum(part):
            part = lax.psum_scatter(part.astype(BF), "seq", scatter_dimension=0, tiled=True)
            return lax.ppermute(part, axes, back).astype(F32)

        delta_rows = jnp.concatenate(
            [dot(o.T, d_y1_low).reshape(seqs, o_rows, width), dot(act.T, g_low).reshape(seqs, d_rows, width)],
            axis=1,
        ).reshape(-1, width)
        delta_rows = rows_sum(delta_rows)
        delta_columns = jnp.concatenate([dot(h1.T, d_qkv), dot(h2.T, d_gu)], axis=1).astype(BF)
        delta_columns = lax.psum_scatter(delta_columns, "seq", scatter_dimension=0, tiled=True)
        own = delta_columns.shape[0] // ranks
        delta_columns = lax.all_to_all(
            delta_columns.reshape(ranks, own, -1), "ctx", split_axis=0, concat_axis=0, tiled=True
        )
        delta_columns = jnp.moveaxis(delta_columns, 0, 1).astype(F32)
        cuts = [my_q * size, (my_q + my_k) * size, (my_q + 2 * my_k) * size, attn_columns + units]
        parts = jnp.split(delta_columns, cuts, axis=2)
        delta_query = fold(parts[0], 0)
        delta_key = fold(parts[1], KEY_VALUE_HEADS)
        delta_value = fold(parts[2], KEY_VALUE_HEADS)
        delta_gate, delta_up = fold(parts[3], 0), fold(parts[4], 0)

        terms = lax.psum(jnp.concatenate([first_term, second_term, query_term, key_term]), axes)
        me = lax.axis_index("seq") * ranks + lax.axis_index("ctx")
        w = width

        def mine(start, n):
            return lax.dynamic_slice_in_dim(terms, start + me * n, n)

        return (
            layer_output[None],
            hidden_gradient[None],
            mine(0, n1),
            delta_query,
            delta_key,
            delta_value,
            mine(2 * w, n3),
            mine(2 * w + size, n4),
            delta_rows[:o_rows],
            mine(w, n2),
            delta_gate,
            delta_up,
            delta_rows[o_rows:],
        )

    return local


def solution(mesh):
    token = P("seq", "ctx", None)
    flat = P(("seq", "ctx"))
    rows = P(("seq", "ctx"), None)
    return jax.shard_map(
        local_of(mesh),
        mesh=mesh,
        in_specs=(token, P("seq", None), flat, rows, rows, rows, flat, flat, rows, flat, rows, rows, rows, token),
        out_specs=(token, token, flat, rows, rows, rows, flat, flat, rows, flat, rows, rows, rows),
        check_vma=False,
    )
```

```python
import types

import jax
import jax.numpy as jnp
import numpy as np
from jax import lax
from jax.experimental import pallas as pl
from jax.experimental.pallas import tpu as pltpu
from jax.sharding import PartitionSpec as P

QUERY_HEAD_COUNT = 16
KEY_VALUE_HEADS = 8
HEAD_DIMENSION = 128

EPS = 1e-06
THETA = 1000000.0
NEGATIVE = -1e30
BF = jnp.bfloat16
F32 = jnp.float32
MESH = pl.DeviceIdType.MESH
RUN = 64
BLOCK = 256


def nn(a, b):
    return jnp.dot(a, b, preferred_element_type=F32)


def nt(a, b):
    return lax.dot_general(a, b, (((1,), (1,)), ((), ())), preferred_element_type=F32)


def tn(a, b):
    return lax.dot_general(a, b, (((0,), (0,)), ((), ())), preferred_element_type=F32)


def loop(low, high, body):
    def step(i, carry):
        body(i)
        return carry

    lax.fori_loop(low, high, step, 0)


def rows_of(start, size):
    return pl.ds(pl.multiple_of(start, size), size)


def inverse_root(values):
    return lax.rsqrt(jnp.mean(values * values, axis=-1, keepdims=True) + EPS)


def norm_backward(normed_grad, normed, inverse):
    return inverse * (normed_grad - normed * jnp.mean(normed_grad * normed, axis=-1, keepdims=True))


def layer_kernel(dims, refs):
    S, C, T, L, D = dims.S, dims.C, dims.T, dims.L, dims.D
    H, RW, OR, DR, AC, U = dims.H, dims.RW, dims.OR, dims.DR, dims.AC, dims.U
    HD = HEAD_DIMENSION
    PR = C * RW
    NR = L // RUN
    NB = L // BLOCK
    CH = C // 2
    scale = HD ** (-0.5)
    r = refs
    s = lax.axis_index("seq")
    c = lax.axis_index("ctx")
    chip = lax.div(c, 2)
    core = lax.rem(c, 2)
    chip_y, chip_x = lax.div(chip, 2), lax.rem(chip, 2)
    sibling = chip * 2 + (1 - core)
    flat = s * C + c
    to_s, to_c = lax.rem(flat, S), lax.div(flat, S)
    from_flat = S * c + s
    from_s, from_c = lax.div(from_flat, C), lax.rem(from_flat, C)
    moved = (to_s * C + to_c) != flat

    def partner(i):
        x = lax.rem(chip_x + lax.rem(i, 2), 2)
        y = lax.rem(chip_y + lax.div(i, 2), 2)
        return y * 2 + x

    def remote(src, dst, send, recv, **where):
        return pltpu.make_async_remote_copy(
            src_ref=src, dst_ref=dst, send_sem=send, recv_sem=recv, device_id=where, device_id_type=MESH
        )

    def local(src, dst, sem):
        return pltpu.make_async_copy(src, dst, sem)

    def arrived(dst, sem):
        pltpu.make_async_copy(dst, dst, sem).wait()

    barrier = pltpu.get_barrier_semaphore()

    def hello(**where):
        pl.semaphore_signal(barrier, inc=1, device_id=where, device_id_type=MESH)

    loop(1, C, lambda i: hello(ctx=lax.rem(c + i, C)))
    loop(1, S, lambda i: hello(seq=lax.rem(s + i, S)))

    @pl.when(moved)
    def _():
        hello(seq=to_s, ctx=to_c)
        hello(seq=from_s, ctx=from_c)

    @pl.when(moved)
    def _():
        pl.semaphore_wait(barrier, C + S)

    @pl.when(jnp.logical_not(moved))
    def _():
        pl.semaphore_wait(barrier, C + S - 2)

    def runs_of(b):
        return pl.ds(b * (BLOCK // RUN), BLOCK // RUN)

    def own_x():
        return r.x_all[pl.ds(c * (T // RUN), T // RUN)].reshape(T, D).astype(F32)

    X, G, H2, DY = 0, 1, 2, 3
    whole = {X: r.x_all, G: r.g_all, H2: r.h2_all, DY: r.dy_all}

    def block(kind, j):
        if kind == X:
            return whole[kind].at[pl.ds(j * (T // RUN), T // RUN)]
        return whole[kind].at[rows_of(j * T, T)]

    def gather_send(kind, src):
        def go(i):
            remote(src, block(kind, c), r.ag_send.at[kind, i], r.ag_recv.at[kind, c],
                   ctx=partner(i) * 2 + core).start()

        loop(1, CH, go)
        remote(src, block(kind, c), r.ag_send.at[kind, 0], r.ag_recv.at[kind, c], ctx=sibling).start()

    def gather_relay(kind, i):
        j = partner(i) * 2 + core
        arrived(block(kind, j), r.ag_recv.at[kind, j])
        remote(block(kind, j), block(kind, j), r.ag_send.at[kind, CH - 1 + i], r.ag_recv.at[kind, j],
               ctx=sibling).start()

    def gather_other(kind, i):
        j = partner(i) * 2 + (1 - core)
        arrived(block(kind, j), r.ag_recv.at[kind, j])

    def gather_done(kind):
        def go(i):
            arrived(block(kind, c), r.ag_send.at[kind, i])

        loop(0, 2 * CH - 1, go)

    def scatter_pair(kind, i, partial):
        r.pair[i] = partial
        r.s1[i] = r.pair[i, rows_of((1 - core) * T, T), :].astype(BF)
        remote(r.s1.at[i], r.r1.at[1 if kind == 1 else 0, i], r.rs_send.at[kind, i],
               r.r1_recv.at[kind, i], ctx=sibling).start()

    def scatter_chips(kind):
        bank = 1 if kind == 1 else 0

        def go(i):
            arrived(r.r1.at[bank, i], r.r1_recv.at[kind, i])
            mine = r.pair[i, rows_of(core * T, T), :] + r.r1[bank, i].astype(F32)
            r.s2[i] = mine.astype(BF)
            remote(r.s2.at[i], r.r2.at[bank, i], r.rs_send.at[kind, CH + i],
                   r.r2_recv.at[kind, i], ctx=partner(i) * 2 + core).start()

        loop(1, CH, go)

    def scatter_sum(kind):
        bank = 1 if kind == 1 else 0
        arrived(r.r1.at[bank, 0], r.r1_recv.at[kind, 0])
        total = r.pair[0, rows_of(core * T, T), :] + r.r1[bank, 0].astype(F32)
        for i in range(1, CH):
            arrived(r.r2.at[bank, i], r.r2_recv.at[kind, i])
            total = total + r.r2[bank, i].astype(F32)
        return total

    def scatter_done(kind):
        loop(0, CH, lambda i: arrived(r.s1.at[0], r.rs_send.at[kind, i]))
        loop(1, CH, lambda i: arrived(r.s2.at[1], r.rs_send.at[kind, CH + i]))

    QKV, OUT, GU, DOWN = 0, 1, 2, 3
    held = {QKV: (r.w_qkv, PR), OUT: (r.w_o, OR), GU: (r.w_gu, PR), DOWN: (r.w_d, DR)}

    def plane(w, b):
        ref, size = held[w]
        return ref.at[rows_of(b * size, size)]

    def weight_start(w):
        @pl.when(s < S - 1)
        def _():
            remote(plane(w, s), plane(w, s), r.z_send.at[w, 0, 0], r.z_recv.at[w, s], seq=s + 1).start()

        @pl.when(s > 0)
        def _():
            remote(plane(w, s), plane(w, s), r.z_send.at[w, 1, 0], r.z_recv.at[w, s], seq=s - 1).start()

    def weight_hop(w, t):
        below, above = s - 1 - t, s + 1 + t

        @pl.when(below >= 0)
        def _():
            arrived(plane(w, below), r.z_recv.at[w, below])

            @pl.when(s < S - 1)
            def _():
                remote(plane(w, below), plane(w, below), r.z_send.at[w, 0, t + 1],
                       r.z_recv.at[w, below], seq=s + 1).start()

        @pl.when(above <= S - 1)
        def _():
            arrived(plane(w, above), r.z_recv.at[w, above])

            @pl.when(s > 0)
            def _():
                remote(plane(w, above), plane(w, above), r.z_send.at[w, 1, t + 1],
                       r.z_recv.at[w, above], seq=s - 1).start()

    def weight_done(w):
        for t in range(S - 1):
            @pl.when(jnp.logical_and(s - t >= 0, s < S - 1))
            def _():
                arrived(plane(w, s), r.z_send.at[w, 0, t])

            @pl.when(jnp.logical_and(s + t <= S - 1, s > 0))
            def _():
                arrived(plane(w, s), r.z_send.at[w, 1, t])

    sent = {QKV: (r.g_qkv, PR), OUT: (r.g_o, OR), GU: (r.g_gu, PR), DOWN: (r.g_d, DR)}
    got = {QKV: r.t_qkv, OUT: r.t_o, GU: r.t_gu, DOWN: r.t_d}
    summed = {QKV: r.u_qkv, OUT: r.u_o, GU: r.u_gu, DOWN: r.u_d}

    def grad_send(w, i, p):
        ref, size = sent[w]
        remote(ref.at[rows_of(p * size, size)], got[w].at[s], r.gz_send.at[w, i], r.gz_recv.at[w, s],
               seq=p).start()

    def grad_sum(w):
        ref, size = sent[w]
        total = ref[rows_of(s * size, size), :].astype(F32)
        for i in range(1, S):
            p = lax.rem(s + i, S)
            arrived(got[w].at[p], r.gz_recv.at[w, p])
            total = total + got[w][p].astype(F32)
        summed[w][...] = total.astype(BF)

    def grad_done(w):
        loop(1, S, lambda i: arrived(got[w].at[0], r.gz_send.at[w, i]))

    final = {QKV: r.f_qkv, GU: r.f_gu, OUT: r.f_o, DOWN: r.f_d}

    def columns_send(n, w):
        def go(i):
            j = lax.rem(c + i, C)
            remote(summed[w].at[rows_of(j * RW, RW)], final[w].at[c], r.gp_send.at[n, i],
                   r.gp_recv.at[n, c], ctx=j).start()

        loop(1, C, go)
        final[w][c] = summed[w][rows_of(c * RW, RW), :]

    def columns_arrive(n, w):
        loop(1, C, lambda i: arrived(final[w].at[lax.rem(c + i, C)], r.gp_recv.at[n, lax.rem(c + i, C)]))

    def columns_done(n, w):
        loop(1, C, lambda i: arrived(final[w].at[0], r.gp_send.at[n, i]))

    def rows_send(n, w):
        @pl.when(moved)
        def _():
            remote(summed[w], final[w], r.row_send.at[n], r.row_recv.at[n], seq=from_s, ctx=from_c).start()

        @pl.when(jnp.logical_not(moved))
        def _():
            final[w][...] = summed[w][...]

    def rows_arrive(n, w):
        @pl.when(moved)
        def _():
            arrived(final[w], r.row_recv.at[n])

    def rows_done(n, w):
        @pl.when(moved)
        def _():
            arrived(final[w], r.row_send.at[n])

    gains_own = r.gains_all.at[flat]
    gain_copy = local(r.gains_in, gains_own, r.gain_recv.at[s])
    gain_copy.start()

    def gain_go(i):
        remote(r.gains_in, gains_own, r.gain_send.at[i], r.gain_recv.at[s],
               ctx=lax.rem(c + i, C)).start()

    loop(1, C, gain_go)

    def qkv_piece(j):
        return (
            (r.wq_in.at[:, rows_of(j * H * HD, H * HD)], slice(0, H * HD)),
            (r.wk_in.at[:, rows_of(j * HD, HD)], slice(H * HD, (H + 1) * HD)),
            (r.wv_in.at[:, rows_of(j * HD, HD)], slice((H + 1) * HD, (H + 2) * HD)),
        )

    def gu_piece(j):
        return (
            (r.wg_in.at[:, rows_of(j * U, U)], slice(0, U)),
            (r.wu_in.at[:, rows_of(j * U, U)], slice(U, 2 * U)),
        )

    def spread(n, w, piece):
        ref = held[w][0]
        own = rows_of(s * PR + c * RW, RW)

        def go(i):
            j = lax.rem(c + i, C)
            for src, columns in piece(j):
                remote(src, ref.at[own, columns], r.w_send.at[n], r.w_recv.at[n], ctx=j).start()

        loop(1, C, go)
        for src, columns in piece(c):
            local(src, ref.at[own, columns], r.w_recv.at[n]).start()

    def spread_arrive(n, w):
        arrived(plane(w, s), r.w_recv.at[n])

    def spread_done(n, w):
        ref = held[w][0]
        arrived(ref.at[pl.ds(0, (C - 1) * RW)], r.w_send.at[n])

    def move(n, w, src):
        @pl.when(moved)
        def _():
            remote(src, held[w][0].at[rows_of(to_s * held[w][1], held[w][1])], r.m_send.at[n],
                   r.m_recv.at[n], seq=to_s, ctx=to_c).start()

        @pl.when(jnp.logical_not(moved))
        def _():
            local(src, plane(w, s), r.m_recv.at[n]).start()

    def move_arrive(n, w):
        arrived(plane(w, s), r.m_recv.at[n])

    def move_done(n, w):
        @pl.when(moved)
        def _():
            arrived(plane(w, s), r.m_send.at[n])

    spread(0, QKV, qkv_piece)
    local(r.x_in, block(X, c), r.local_sem.at[0]).start()
    local(r.table_in, r.table, r.local_sem.at[1]).start()
    gather_send(X, r.x_in)
    move(0, OUT, r.wo_in)

    arrived(r.gains_all.at[pl.ds(s * C, C)], r.gain_recv.at[s])

    def gain_far(i):
        mine = r.gains_all.at[pl.ds(s * C, C)]
        remote(mine, mine, r.gain_send.at[C + i], r.gain_recv.at[s], seq=lax.rem(s + i, S)).start()

    loop(1, S, gain_far)
    spread_arrive(0, QKV)
    weight_start(QKV)
    move_arrive(0, OUT)
    weight_start(OUT)
    spread(1, GU, gu_piece)
    move(1, DOWN, r.wd_in)

    arrived(r.table, r.local_sem.at[1])

    def tables(b):
        rows = rows_of(b * T, T)
        both = r.table[rows, :]
        other = pltpu.roll(both, HD // 2, 1)
        first = lax.broadcasted_iota(jnp.int32, (T, HD), 1) < HD // 2
        r.cosine[rows, :] = jnp.where(first, both, other)
        r.sine[rows, :] = jnp.where(first, -other, both)

    loop(0, L // T, tables)

    def gain_block(i):
        p = lax.rem(s + i, S)
        arrived(r.gains_all.at[pl.ds(p * C, C)], r.gain_recv.at[p])

    loop(1, S, gain_block)
    gains = jnp.sum(r.gains_all[...], axis=1).astype(BF)

    def gain_vector(offset, count):
        width = count * S * C
        shift = count.bit_length() - 1
        column = lax.broadcasted_iota(jnp.int32, (HD, width), 1)
        row = lax.broadcasted_iota(jnp.int32, (HD, width), 0)
        pick = jnp.where(row == offset + (column & (count - 1)), 1.0, 0.0).astype(BF)
        spread_out = nn(gains, pick)
        owner = lax.broadcasted_iota(jnp.int32, (S * C, width), 0)
        place = lax.broadcasted_iota(jnp.int32, (S * C, width), 1) >> shift
        return jnp.sum(jnp.where(owner == place, spread_out, 0.0), axis=0, keepdims=True)

    n1 = D // (S * C)
    n3 = HD // (S * C)
    r.gain1[...] = gain_vector(0, n1)
    r.gain2[...] = gain_vector(n1, n1)
    r.gainq[...] = gain_vector(2 * n1, n3)
    r.gaink[...] = gain_vector(2 * n1 + n3, n3)

    arrived(block(X, c), r.local_sem.at[0])
    loop(1, CH, lambda i: gather_relay(X, i))
    arrived(block(X, sibling), r.ag_recv.at[X, sibling])
    loop(1, CH, lambda i: gather_other(X, i))
    weight_hop(QKV, 0)
    local(r.g_in, block(G, c), r.local_sem.at[2]).start()
    gather_send(G, r.g_in)

    def first_norm(k):
        x = r.x_all[r.order[1, k]].astype(F32)
        r.h1[rows_of(k * RUN, RUN), :] = (x * inverse_root(x) * r.gain1[...]).astype(BF)

    loop(0, NR, first_norm)
    weight_hop(OUT, 0)
    weight_hop(QKV, 1)
    weight_hop(OUT, 1)
    spread_arrive(1, GU)
    weight_start(GU)
    weight_hop(QKV, 2)
    weight_hop(OUT, 2)

    def rotate(u, rows):
        return u * r.cosine[rows, :] + pltpu.roll(u, HD // 2, 1) * r.sine[rows, :]

    def rotate_back(u, rows):
        return u * r.cosine[rows, :] - pltpu.roll(u, HD // 2, 1) * r.sine[rows, :]

    def project(b):
        rows = rows_of(b * BLOCK, BLOCK)
        acc = nn(r.h1[rows, :], r.w_qkv[...])
        for h in range(H):
            u = acc[:, h * HD : (h + 1) * HD]
            r.q_lin[h, rows, :] = u
            r.q_rot[h, rows, :] = rotate(u * inverse_root(u) * r.gainq[...], rows).astype(BF)
        u = acc[:, H * HD : (H + 1) * HD]
        r.k_lin[rows, :] = u
        k = rotate(u * inverse_root(u) * r.gaink[...], rows)
        r.k_rot[rows, :] = k.astype(BF)
        r.k_t[:, rows] = k.T.astype(BF)
        v = acc[:, (H + 1) * HD :]
        r.v[rows, :] = v.astype(BF)
        r.v_t[:, rows] = v.T.astype(BF)

    loop(0, NB, project)
    gather_relay_g = lambda i: gather_relay(G, i)
    loop(1, CH, gather_relay_g)

    def attend(qb):
        cols = rows_of(qb * BLOCK, BLOCK)

        def keys(kb, carry):
            rows = rows_of(kb * BLOCK, BLOCK)
            key = r.k_rot[rows, :]
            value_t = r.v_t[:, rows]
            ahead = lax.broadcasted_iota(jnp.int32, (BLOCK, BLOCK), 0) - lax.broadcasted_iota(
                jnp.int32, (BLOCK, BLOCK), 1
            )
            allowed = ahead <= (qb - kb) * BLOCK
            out = []
            for h in range(H):
                acc, total = carry[2 * h], carry[2 * h + 1]
                e = jnp.exp(nt(key, r.q_rot[h, cols, :]) * scale)
                e = jnp.where(allowed, e, 0.0)
                low = e.astype(BF)
                r.e[h, rows, cols] = low
                out += [acc + nn(value_t, low), total + jnp.sum(e, axis=0, keepdims=True)]
            return tuple(out)

        zero = (jnp.zeros((HD, BLOCK), F32), jnp.zeros((1, BLOCK), F32)) * H
        done = lax.fori_loop(0, qb + 1, keys, zero)
        for h in range(H):
            inverse = 1.0 / done[2 * h + 1]
            o = done[2 * h] * inverse
            r.l_inv[h, :, cols] = jnp.broadcast_to(inverse, (8, BLOCK))
            r.o_t[h, :, cols] = o
            r.o_sorted[runs_of(qb), :, h * HD : (h + 1) * HD] = o.T.astype(BF).reshape(-1, RUN, HD)

    loop(0, NB, attend)
    weight_hop(GU, 0)
    move_arrive(1, DOWN)
    weight_start(DOWN)

    def unsort(i):
        r.o[rows_of(i * RUN, RUN), :] = r.o_sorted[r.order[0, i]]

    loop(0, NR, unsort)

    def out_chip(i):
        scatter_pair(0, i, nn(r.o[rows_of(partner(i) * 2 * T, 2 * T), :], r.w_o[...]))

    loop(0, CH, out_chip)
    scatter_chips(0)
    weight_hop(GU, 1)
    y1 = own_x() + scatter_sum(0)
    scatter_done(0)
    r.y1[...] = y1
    h2_own = (y1 * inverse_root(y1) * r.gain2[...]).astype(BF)
    r.h2_all[rows_of(c * T, T), :] = h2_own
    gather_send(H2, block(H2, c))

    weight_hop(GU, 2)
    weight_hop(DOWN, 0)
    weight_hop(DOWN, 1)
    arrived(block(G, c), r.local_sem.at[2])
    arrived(block(G, sibling), r.ag_recv.at[G, sibling])
    loop(1, CH, lambda i: gather_other(G, i))
    weight_hop(DOWN, 2)

    def act_grad(b):
        rows = rows_of(b * BLOCK, BLOCK)
        r.d_act[rows, :] = nt(r.g_all[rows, :], r.w_d[...])

    loop(0, NB, act_grad)
    arrived(block(H2, sibling), r.ag_recv.at[H2, sibling])

    def feed(i):
        @pl.when(i > 0)
        def _():
            gather_relay(H2, i)
            gather_other(H2, i)

        rows = rows_of(partner(i) * 2 * T, 2 * T)
        h2 = r.h2_all[rows, :]
        gate = nn(h2, r.w_gu[:, :U])
        up = nn(h2, r.w_gu[:, U:])
        sig = 1.0 / (1.0 + jnp.exp(-gate))
        silu = gate * sig
        r.act[rows, :] = (silu * up).astype(BF)
        d_act = r.d_act[rows, :]
        d_gate = (d_act * up * sig * (1.0 + gate * (1.0 - sig))).astype(BF)
        d_up = (d_act * silu).astype(BF)
        r.d_gu[rows, :U] = d_gate
        r.d_gu[rows, U:] = d_up
        scatter_pair(2, i, nt(r.d_gu[rows, :], r.w_gu[...]))

    loop(0, CH, feed)
    scatter_chips(2)

    def down_grad(m):
        cols = rows_of(m * HD, HD)
        r.g_d[cols, :] = tn(r.act[:, cols], r.g_all[...]).astype(BF)

    loop(0, U // HD, down_grad)
    loop(1, S, lambda i: grad_send(DOWN, i, lax.rem(s + i, S)))

    def gu_grad(i):
        p = lax.rem(s + i, S)
        cols = rows_of(p * PR, PR)
        r.g_gu[cols, :] = tn(r.h2_all[:, cols], r.d_gu[...]).astype(BF)

        @pl.when(i < S)
        def _():
            grad_send(GU, i, p)

    loop(1, S + 1, gu_grad)

    d_h2 = scatter_sum(2)
    scatter_done(2)
    y1 = r.y1[...]
    r2 = inverse_root(y1)
    normed = y1 * r2
    term2 = jnp.sum(d_h2 * normed, axis=0, keepdims=True)
    d_y1 = r.g_all[rows_of(c * T, T), :].astype(F32) + norm_backward(d_h2 * r.gain2[...], normed, r2)
    r.d_y1[...] = d_y1
    r.dy_all[rows_of(c * T, T), :] = d_y1.astype(BF)
    gather_send(DY, block(DY, c))
    WT = D // HD
    for k in range(WT):
        r.terms[WT + k : WT + k + 1, :] = term2[:, k * HD : (k + 1) * HD]

    def last_chip(i):
        scatter_pair(1, i, nn(r.act[rows_of(partner(i) * 2 * T, 2 * T), :], r.w_d[...]))

    loop(0, CH, last_chip)
    arrived(block(DY, sibling), r.ag_recv.at[DY, sibling])

    def out_grad(i):
        @pl.when(i > 0)
        def _():
            gather_relay(DY, i)
            gather_other(DY, i)

        rows = rows_of(partner(i) * 2 * T, 2 * T)
        d_o = nt(r.dy_all[rows, :], r.w_o[...]).astype(BF)
        r.d_o[pl.ds(partner(i) * (2 * T // RUN), 2 * T // RUN)] = d_o.reshape(-1, RUN, H * HD)

    loop(0, CH, out_grad)
    scatter_chips(1)

    def out_weight(m):
        cols = rows_of(m * HD, HD)
        r.g_o[cols, :] = tn(r.o[:, cols], r.dy_all[...]).astype(BF)

    loop(0, H * HD // HD, out_weight)
    loop(1, S, lambda i: grad_send(OUT, i, lax.rem(s + i, S)))

    def sort(k):
        r.d_o_sorted[rows_of(k * RUN, RUN), :] = r.d_o[r.order[1, k]]

    loop(0, NR, sort)
    r.d_k[...] = jnp.zeros_like(r.d_k)
    r.d_v[...] = jnp.zeros_like(r.d_v)
    r.sums[...] = jnp.zeros_like(r.sums)

    def attend_back(qb):
        cols = rows_of(qb * BLOCK, BLOCK)
        d_o_t, d_o_low, row, factor = [], [], [], []
        for h in range(H):
            t = r.d_o_sorted[cols, h * HD : (h + 1) * HD].astype(F32).T
            inverse = r.l_inv[h, 0:1, cols]
            row.append(jnp.sum(t * r.o_t[h, :, cols], axis=0, keepdims=True))
            factor.append(inverse * scale)
            r.do_t[h] = t.astype(BF)
            r.do_l[h] = (t * inverse).T.astype(BF)

        def keys(kb, carry):
            rows = rows_of(kb * BLOCK, BLOCK)
            value = r.v[rows, :]
            key_t = r.k_t[:, rows]
            out = []
            d_k = r.d_k[rows, :]
            d_v = r.d_v[rows, :]
            for h in range(H):
                e = r.e[h, rows, cols]
                dp = nn(value, r.do_t[h])
                de = (e.astype(F32) * ((dp - row[h]) * factor[h])).astype(BF)
                out.append(carry[h] + nn(key_t, de))
                d_k = d_k + nn(de, r.q_rot[h, cols, :])
                d_v = d_v + nn(e, r.do_l[h])
            r.d_k[rows, :] = d_k
            r.d_v[rows, :] = d_v
            return tuple(out)

        done = lax.fori_loop(0, qb + 1, keys, (jnp.zeros((HD, BLOCK), F32),) * H)
        for h in range(H):
            d_g = rotate_back(done[h].T, cols)
            u = r.q_lin[h, cols, :]
            inverse = inverse_root(u)
            normed = u * inverse
            r.sums[0:1, :] += jnp.sum(d_g * normed, axis=0, keepdims=True)
            d_lin = norm_backward(d_g * r.gainq[...], normed, inverse).astype(BF)
            r.d_qkv[runs_of(qb), :, h * HD : (h + 1) * HD] = d_lin.reshape(-1, RUN, HD)

    loop(0, NB, attend_back)

    def key_back(b):
        rows = rows_of(b * BLOCK, BLOCK)
        d_g = rotate_back(r.d_k[rows, :], rows)
        u = r.k_lin[rows, :]
        inverse = inverse_root(u)
        normed = u * inverse
        r.sums[1:2, :] += jnp.sum(d_g * normed, axis=0, keepdims=True)
        d_lin = norm_backward(d_g * r.gaink[...], normed, inverse).astype(BF)
        r.d_qkv[runs_of(b), :, H * HD : (H + 1) * HD] = d_lin.reshape(-1, RUN, HD)
        r.d_qkv[runs_of(b), :, (H + 1) * HD :] = r.d_v[rows, :].astype(BF).reshape(-1, RUN, HD)

    loop(0, NB, key_back)

    def qkv_grad(i):
        p = lax.rem(s + i, S)
        cols = rows_of(p * PR, PR)
        r.g_qkv[cols, :] = tn(r.h1[:, cols], r.d_qkv[...].reshape(L, AC)).astype(BF)

        @pl.when(i < S)
        def _():
            grad_send(QKV, i, p)

    loop(1, S + 1, qkv_grad)

    r.layer_out[...] = (r.y1[...] + scatter_sum(1)).astype(BF)
    scatter_done(1)

    def in_chip(i):
        j = partner(i) * 2
        parts = []
        for k in range(2 * T // RUN):
            parts.append(r.d_qkv[r.order[0, j * (T // RUN) + k]])
        scatter_pair(3, i, nt(jnp.concatenate(parts, axis=0), r.w_qkv[...]))

    loop(0, CH, in_chip)
    scatter_chips(3)
    grad_sum(DOWN)
    rows_send(1, DOWN)
    grad_sum(GU)
    columns_send(1, GU)
    grad_sum(OUT)
    rows_send(0, OUT)
    d_h1 = scatter_sum(3)
    x = own_x()
    r1 = inverse_root(x)
    normed = x * r1
    term1 = jnp.sum(d_h1 * normed, axis=0, keepdims=True)
    r.hidden_grad[...] = r.d_y1[...] + norm_backward(d_h1 * r.gain1[...], normed, r1)
    for k in range(WT):
        r.terms[k : k + 1, :] = term1[:, k * HD : (k + 1) * HD]
    r.terms[2 * WT : 2 * WT + 8, :] = r.sums[...]

    def terms_far(i):
        remote(r.terms, r.terms_z.at[s], r.t_send.at[i], r.t_recv.at[s],
               seq=lax.rem(s + i, S)).start()

    loop(1, S, terms_far)
    grad_sum(QKV)
    columns_send(0, QKV)
    total = r.terms[...]
    for i in range(1, S):
        p = lax.rem(s + i, S)
        arrived(r.terms_z.at[p], r.t_recv.at[p])
        total = total + r.terms_z[p]
    r.terms_sum[...] = total

    def terms_near(i):
        remote(r.terms_sum, r.terms_p.at[c], r.t_send.at[S + i], r.t_recv.at[S + c],
               ctx=lax.rem(c + i, C)).start()

    loop(1, C, terms_near)

    rows_arrive(1, DOWN)
    r.delta_down[...] = r.f_d[...].astype(F32)
    rows_arrive(0, OUT)
    r.delta_out[...] = r.f_o[...].astype(F32)
    columns_arrive(1, GU)
    for j in range(C):
        r.delta_gate[:, j * U : (j + 1) * U] = r.f_gu[j, :, :U].astype(F32)
        r.delta_up[:, j * U : (j + 1) * U] = r.f_gu[j, :, U:].astype(F32)
    columns_arrive(0, QKV)
    for j in range(C):
        r.delta_query[:, j * H * HD : (j + 1) * H * HD] = r.f_qkv[j, :, : H * HD].astype(F32)
        r.delta_key[:, j * HD : (j + 1) * HD] = r.f_qkv[j, :, H * HD : (H + 1) * HD].astype(F32)
        r.delta_value[:, j * HD : (j + 1) * HD] = r.f_qkv[j, :, (H + 1) * HD :].astype(F32)
    total = r.terms_sum[...]
    for i in range(1, C):
        j = lax.rem(c + i, C)
        arrived(r.terms_p.at[j], r.t_recv.at[S + j])
        total = total + r.terms_p[j]
    r.terms_out[...] = total

    loop(1, C, lambda i: arrived(gains_own, r.gain_send.at[i]))
    loop(1, S, lambda i: arrived(r.gains_all.at[pl.ds(0, C)], r.gain_send.at[C + i]))
    for kind in (X, G, H2, DY):
        gather_done(kind)
    spread_done(0, QKV)
    spread_done(1, GU)
    move_done(0, OUT)
    move_done(1, DOWN)
    for w in (QKV, OUT, GU, DOWN):
        weight_done(w)
        grad_done(w)
    columns_done(0, QKV)
    columns_done(1, GU)
    rows_done(0, OUT)
    rows_done(1, DOWN)
    scatter_done(3)
    loop(1, S, lambda i: arrived(r.terms, r.t_send.at[i]))
    loop(1, C, lambda i: arrived(r.terms, r.t_send.at[S + i]))


def fused_layer(mesh, args):
    (x, positions, gain1, wq, wk, wv, gainq, gaink, wo, gain2, wg, wu, wd, g) = args
    S, C = mesh.shape["seq"], mesh.shape["ctx"]
    T, D = x.shape[1:]
    L = positions.shape[1]
    HD = HEAD_DIMENSION
    H = QUERY_HEAD_COUNT // C
    RW, OR, DR = wq.shape[0], wo.shape[0], wd.shape[0]
    U = wg.shape[1] // C
    AC = (H + 2) * HD
    PR = C * RW
    CH = C // 2
    dims = types.SimpleNamespace(S=S, C=C, T=T, L=L, D=D, H=H, RW=RW, OR=OR, DR=DR, AC=AC, U=U)
    packed = jnp.concatenate([gain1, gain2, gainq, gaink]).astype(F32)
    packed = jnp.pad(packed[None, :], ((0, 7), (0, HD - packed.shape[0])))
    half = HD // 2
    frequency = np.power(THETA, -np.arange(half) * (2.0 / HD))
    phases = np.arange(L)[:, None] * frequency[None, :]
    table = jnp.asarray(np.concatenate([np.cos(phases), np.sin(phases)], axis=1), F32)
    TR = 2 * (D // HD) + 8
    run = positions[0, ::RUN] // RUN
    spot = jnp.arange(L // RUN, dtype=jnp.int32)
    place = jnp.sum(jnp.where(run[None, :] == spot[:, None], spot[None, :], 0), axis=1)
    order = jnp.stack([run, place]).astype(jnp.int32)
    inputs = dict(
        order=order, x_in=x.reshape(T // RUN, RUN, D), g_in=g[0], gains_in=packed, wq_in=wq, wk_in=wk, wv_in=wv, wo_in=wo,
        wg_in=wg, wu_in=wu, wd_in=wd, table_in=table,
    )
    outputs = dict(
        layer_out=((T, D), BF), hidden_grad=((T, D), F32), delta_query=((RW, C * H * HD), F32),
        delta_key=((RW, C * HD), F32), delta_value=((RW, C * HD), F32), delta_out=((OR, D), F32),
        delta_gate=((RW, C * U), F32), delta_up=((RW, C * U), F32), delta_down=((DR, D), F32),
        terms_out=((TR, HD), F32),
    )
    V, DMA = pltpu.VMEM, pltpu.SemaphoreType.DMA
    scratch = dict(
        x_all=V((L // RUN, RUN, D), BF), g_all=V((L, D), BF), h2_all=V((L, D), BF), dy_all=V((L, D), BF),
        h1=V((L, D), BF), w_qkv=V((D, AC), BF), w_o=V((H * HD, D), BF), w_gu=V((D, 2 * U), BF),
        w_d=V((U, D), BF), gains_all=V((S * C, 8, HD), F32), table=V((L, HD), F32),
        cosine=V((L, HD), F32), sine=V((L, HD), F32), gain1=V((1, D), F32), gain2=V((1, D), F32),
        gainq=V((1, HD), F32), gaink=V((1, HD), F32), q_lin=V((H, L, HD), F32), k_lin=V((L, HD), F32),
        q_rot=V((H, L, HD), BF), k_rot=V((L, HD), BF), v=V((L, HD), BF), k_t=V((HD, L), BF),
        v_t=V((HD, L), BF), e=V((H, L, L), BF), l_inv=V((H, 8, L), F32), o_t=V((H, HD, L), F32),
        o_sorted=V((L // RUN, RUN, H * HD), BF), o=V((L, H * HD), BF), y1=V((T, D), F32), d_act=V((L, U), F32),
        act=V((L, U), BF), d_gu=V((L, 2 * U), BF), d_y1=V((T, D), F32), d_o=V((L // RUN, RUN, H * HD), BF),
        d_o_sorted=V((L, H * HD), BF), do_t=V((H, HD, BLOCK), BF), do_l=V((H, BLOCK, HD), BF),
        d_k=V((L, HD), F32), d_v=V((L, HD), F32), d_qkv=V((L // RUN, RUN, AC), BF), sums=V((8, HD), F32),
        pair=V((CH, 2 * T, D), F32), s1=V((CH, T, D), BF), r1=V((2, CH, T, D), BF),
        s2=V((CH, T, D), BF), r2=V((2, CH, T, D), BF),
        g_qkv=V((D, AC), BF), g_o=V((H * HD, D), BF), g_gu=V((D, 2 * U), BF), g_d=V((U, D), BF),
        t_qkv=V((S, PR, AC), BF), t_o=V((S, OR, D), BF), t_gu=V((S, PR, 2 * U), BF), t_d=V((S, DR, D), BF),
        u_qkv=V((PR, AC), BF), u_o=V((OR, D), BF), u_gu=V((PR, 2 * U), BF), u_d=V((DR, D), BF),
        f_qkv=V((C, RW, AC), BF), f_o=V((OR, D), BF), f_gu=V((C, RW, 2 * U), BF), f_d=V((DR, D), BF),
        terms=V((TR, HD), F32), terms_z=V((S, TR, HD), F32), terms_sum=V((TR, HD), F32),
        terms_p=V((C, TR, HD), F32),
        ag_send=DMA((4, 2 * CH)), ag_recv=DMA((4, C)), rs_send=DMA((4, 2 * CH)), r1_recv=DMA((4, CH)),
        r2_recv=DMA((4, CH)), z_send=DMA((4, 2, S)), z_recv=DMA((4, S)), gz_send=DMA((4, S)),
        gz_recv=DMA((4, S)), gp_send=DMA((2, C)), gp_recv=DMA((2, C)), row_send=DMA((2,)),
        row_recv=DMA((2,)), w_send=DMA((2,)), w_recv=DMA((2,)), m_send=DMA((2,)), m_recv=DMA((2,)),
        gain_send=DMA((C + S,)), gain_recv=DMA((S,)), t_send=DMA((S + C,)), t_recv=DMA((S + C,)),
        local_sem=DMA((3,)),
    )
    names = list(inputs) + list(outputs) + list(scratch)

    def kernel(*refs):
        layer_kernel(dims, types.SimpleNamespace(**dict(zip(names, refs))))

    in_specs = [
        pl.BlockSpec(memory_space=pltpu.SMEM if name == "order" else pl.ANY) for name in inputs
    ]
    results = pl.pallas_call(
        kernel,
        out_shape=[jax.ShapeDtypeStruct(*v) for v in outputs.values()],
        in_specs=in_specs,
        out_specs=[pl.BlockSpec(memory_space=pltpu.VMEM)] * len(outputs),
        scratch_shapes=list(scratch.values()),
        compiler_params=pltpu.CompilerParams(
            collective_id=0, has_side_effects=True, vmem_limit_bytes=67043328
        ),
        name="layer",
    )(*inputs.values())
    out = types.SimpleNamespace(**dict(zip(outputs, results)))
    terms = out.terms_out.reshape(-1)
    me = lax.axis_index("seq") * C + lax.axis_index("ctx")

    def mine(start, array):
        n = array.shape[0]
        return lax.dynamic_slice_in_dim(terms, start + me * n, n)

    return (
        out.layer_out[None], out.hidden_grad[None], mine(0, gain1), out.delta_query,
        out.delta_key, out.delta_value, mine(2 * D, gainq), mine(2 * D + HD, gaink),
        out.delta_out, mine(D, gain2), out.delta_gate, out.delta_up, out.delta_down,
    )


def angles(places, head_size):
    half_size = head_size // 2
    frequency = jnp.power(THETA, -jnp.arange(half_size, dtype=F32) * (2.0 / head_size))
    phases = places.astype(F32)[:, None] * frequency[None, :]
    phases = jnp.concatenate([phases, phases], axis=-1)
    return (jnp.cos(phases), jnp.sin(phases))


def rotate(values, cosines, sines):
    half_size = values.shape[-1] // 2
    turned = jnp.concatenate([-values[..., half_size:], values[..., :half_size]], axis=-1)
    return values * cosines + turned * sines


def rotate_back(upstream, cosines, sines):
    half_size = upstream.shape[-1] // 2
    scaled = upstream * sines
    turned = jnp.concatenate([scaled[..., half_size:], -scaled[..., :half_size]], axis=-1)
    return upstream * cosines + turned


def dot(a, b):
    return jnp.dot(a, b, preferred_element_type=F32)


def local_of(mesh):
    seqs, ranks = mesh.shape["seq"], mesh.shape["ctx"]
    devices = seqs * ranks
    axes = ("seq", "ctx")

    def spread(shard, heads):
        rows, columns = shard.shape
        if heads and heads < ranks:
            blocks = shard.reshape(rows, heads, 1, columns // heads)
            blocks = jnp.broadcast_to(blocks, (rows, heads, ranks // heads, columns // heads))
            return blocks.reshape(rows, ranks, columns // heads)
        return shard.reshape(rows, ranks, columns // ranks)

    def fold(blocks, heads):
        rows, count, width = blocks.shape
        if heads and heads < ranks:
            return blocks.reshape(rows, heads, count // heads, width).sum(2).reshape(rows, heads * width)
        return blocks.reshape(rows, count * width)

    forth = [(seqs * r + j, j * ranks + r) for r in range(ranks) for j in range(seqs)]
    back = [(b, a) for a, b in forth]

    def local(
        hidden_states, positions, gain_first, weight_query, key_weight_matrix, value_weight_matrix,
        gain_query, gain_key, weight_output, gain_second, weight_gate, weight_up, weight_down,
        output_cotangent,
    ):
        tokens = hidden_states.shape[1]
        length = positions.shape[1]
        size = HEAD_DIMENSION
        group = QUERY_HEAD_COUNT // KEY_VALUE_HEADS
        my_q = QUERY_HEAD_COUNT // ranks
        my_k = max(1, KEY_VALUE_HEADS // ranks)
        scale = size ** (-0.5)
        places = positions[0]
        cosines, sines = angles(places, size)
        cosines, sines = cosines[:, None, :], sines[:, None, :]

        gains = jnp.concatenate([gain_first, gain_second, gain_query, gain_key])
        gains = lax.all_gather(gains, axes, axis=0).astype(F32)
        n1, n2, n3, n4 = (g.shape[0] for g in (gain_first, gain_second, gain_query, gain_key))
        first_scale = gains[:, :n1].reshape(-1)
        second_scale = gains[:, n1 : n1 + n2].reshape(-1)
        query_scale = gains[:, n1 + n2 : n1 + n2 + n3].reshape(-1)
        key_scale = gains[:, n1 + n2 + n3 :].reshape(-1)

        column_weights = jnp.concatenate(
            [
                spread(weight_query, 0),
                spread(key_weight_matrix, KEY_VALUE_HEADS),
                spread(value_weight_matrix, KEY_VALUE_HEADS),
                spread(weight_gate, 0),
                spread(weight_up, 0),
            ],
            axis=2,
        )
        column_weights = lax.all_to_all(column_weights, "ctx", split_axis=1, concat_axis=0, tiled=True)
        column_weights = lax.all_gather(column_weights[:, 0], "seq", axis=0, tiled=True)
        row_weights = jnp.concatenate([weight_output, weight_down], axis=0)
        row_weights = lax.all_gather(lax.ppermute(row_weights, axes, forth), "seq", axis=0)
        o_rows, d_rows = weight_output.shape[0], weight_down.shape[0]
        width = weight_output.shape[1]
        w_o = row_weights[:, :o_rows].reshape(-1, width)
        w_d = row_weights[:, o_rows:].reshape(-1, width)
        units = w_d.shape[0]
        attn_columns = (my_q + 2 * my_k) * size
        w_qkv = column_weights[:, :attn_columns]
        w_gu = column_weights[:, attn_columns:]

        x = lax.all_gather(hidden_states[0], "ctx", axis=0, tiled=True).astype(F32)
        g_low = lax.all_gather(output_cotangent[0], "ctx", axis=0, tiled=True)
        first_inverse = inverse_root(x)
        h1 = (x * first_inverse * first_scale).astype(BF)
        qkv = dot(h1, w_qkv)
        q_lin = qkv[:, : my_q * size].reshape(length, my_q, size)
        k_lin = qkv[:, my_q * size : (my_q + my_k) * size].reshape(length, my_k, size)
        v = qkv[:, (my_q + my_k) * size :].astype(BF).reshape(length, my_k, size)
        rq, rk = inverse_root(q_lin), inverse_root(k_lin)
        nq, nk = q_lin * rq, k_lin * rk
        qr = rotate(nq * query_scale, cosines, sines).astype(BF)
        kr = rotate(nk * key_scale, cosines, sines).astype(BF)
        mask = places[None, :] <= places[:, None]

        def scores(h):
            e = lax.dot_general(
                qr[:, h], kr[:, h // group], (((1,), (1,)), ((), ())), preferred_element_type=F32
            )
            return jnp.where(mask, e * scale, NEGATIVE)

        outs, probs = [], []
        for h in range(my_q):
            e = scores(h)
            p = jnp.exp(e - jnp.max(e, axis=-1, keepdims=True))
            p = p / jnp.sum(p, axis=-1, keepdims=True)
            probs.append(p)
            outs.append(dot(p.astype(BF), v[:, h // group]))
        o = jnp.concatenate(outs, axis=1).astype(BF)

        def scatter(part):
            return lax.psum_scatter(part.astype(BF), "ctx", scatter_dimension=0, tiled=True).astype(F32)

        x_own = hidden_states[0].astype(F32)
        y1 = x_own + scatter(dot(o, w_o))
        r2 = inverse_root(y1)
        second_normed = y1 * r2
        h2 = lax.all_gather((second_normed * second_scale).astype(BF), "ctx", axis=0, tiled=True)
        gu = dot(h2, w_gu)
        gate, up = gu[:, :units], gu[:, units:]
        sig = jax.nn.sigmoid(gate)
        silu = gate * sig
        act = (silu * up).astype(BF)
        layer_output = (y1 + scatter(dot(act, w_d))).astype(BF)

        d_act = dot(g_low, w_d.T)
        d_gate = (d_act * up * sig * (1.0 + gate * (1.0 - sig))).astype(BF)
        d_up = (d_act * silu).astype(BF)
        d_gu = jnp.concatenate([d_gate, d_up], axis=1)
        d_h2 = scatter(dot(d_gu, w_gu.T))
        second_term = jnp.sum(d_h2 * second_normed, axis=0)
        d_y1 = output_cotangent[0].astype(F32) + norm_backward(d_h2 * second_scale, second_normed, r2)
        d_y1_low = lax.all_gather(d_y1.astype(BF), "ctx", axis=0, tiled=True)
        d_o = dot(d_y1_low, w_o.T).astype(BF).reshape(length, my_q, size)

        d_q, d_k, d_v = [], [0.0] * my_k, [0.0] * my_k
        for h in range(my_q):
            p = probs[h]
            dp = lax.dot_general(
                d_o[:, h], v[:, h // group], (((1,), (1,)), ((), ())), preferred_element_type=F32
            )
            row = jnp.sum(p * dp, axis=-1, keepdims=True)
            de = (p * (dp - row) * scale).astype(BF)
            d_q.append(dot(de, kr[:, h // group]))
            d_k[h // group] += dot(de.T, qr[:, h])
            d_v[h // group] += dot(p.astype(BF).T, d_o[:, h])
        d_q, d_k, d_v = jnp.stack(d_q, 1), jnp.stack(d_k, 1), jnp.stack(d_v, 1)
        d_gq, d_gk = rotate_back(d_q, cosines, sines), rotate_back(d_k, cosines, sines)
        query_term = jnp.sum(d_gq * nq, axis=(0, 1))
        key_term = jnp.sum(d_gk * nk, axis=(0, 1))
        d_qlin = norm_backward(d_gq * query_scale, nq, rq).reshape(length, -1)
        d_klin = norm_backward(d_gk * key_scale, nk, rk).reshape(length, -1)
        d_qkv = jnp.concatenate([d_qlin, d_klin, d_v.reshape(length, -1)], axis=1).astype(BF)
        d_h1 = scatter(dot(d_qkv, w_qkv.T))
        r1 = inverse_root(x_own)
        first_normed = x_own * r1
        first_term = jnp.sum(d_h1 * first_normed, axis=0)
        hidden_gradient = d_y1 + norm_backward(d_h1 * first_scale, first_normed, r1)

        def rows_sum(part):
            part = lax.psum_scatter(part.astype(BF), "seq", scatter_dimension=0, tiled=True)
            return lax.ppermute(part, axes, back).astype(F32)

        delta_rows = jnp.concatenate(
            [dot(o.T, d_y1_low).reshape(seqs, o_rows, width), dot(act.T, g_low).reshape(seqs, d_rows, width)],
            axis=1,
        ).reshape(-1, width)
        delta_rows = rows_sum(delta_rows)
        delta_columns = jnp.concatenate([dot(h1.T, d_qkv), dot(h2.T, d_gu)], axis=1).astype(BF)
        delta_columns = lax.psum_scatter(delta_columns, "seq", scatter_dimension=0, tiled=True)
        own = delta_columns.shape[0] // ranks
        delta_columns = lax.all_to_all(
            delta_columns.reshape(ranks, own, -1), "ctx", split_axis=0, concat_axis=0, tiled=True
        )
        delta_columns = jnp.moveaxis(delta_columns, 0, 1).astype(F32)
        cuts = [my_q * size, (my_q + my_k) * size, (my_q + 2 * my_k) * size, attn_columns + units]
        parts = jnp.split(delta_columns, cuts, axis=2)
        delta_query = fold(parts[0], 0)
        delta_key = fold(parts[1], KEY_VALUE_HEADS)
        delta_value = fold(parts[2], KEY_VALUE_HEADS)
        delta_gate, delta_up = fold(parts[3], 0), fold(parts[4], 0)

        terms = lax.psum(jnp.concatenate([first_term, second_term, query_term, key_term]), axes)
        me = lax.axis_index("seq") * ranks + lax.axis_index("ctx")
        w = width

        def mine(start, n):
            return lax.dynamic_slice_in_dim(terms, start + me * n, n)

        return (
            layer_output[None],
            hidden_gradient[None],
            mine(0, n1),
            delta_query,
            delta_key,
            delta_value,
            mine(2 * w, n3),
            mine(2 * w + size, n4),
            delta_rows[:o_rows],
            mine(w, n2),
            delta_gate,
            delta_up,
            delta_rows[o_rows:],
        )

    return local


def solution(mesh):
    token = P("seq", "ctx", None)
    flat = P(("seq", "ctx"))
    rows = P(("seq", "ctx"), None)
    general = local_of(mesh)

    def body(*args):
        tokens, length = args[0].shape[1], args[1].shape[1]
        fits = (
            mesh.shape["ctx"] == KEY_VALUE_HEADS == 8
            and length <= 1024
            and length % BLOCK == 0
            and tokens % RUN == 0
            and HEAD_DIMENSION % (mesh.shape["seq"] * mesh.shape["ctx"]) == 0
        )
        return fused_layer(mesh, args) if fits else general(*args)

    return jax.shard_map(
        body,
        mesh=mesh,
        in_specs=(token, P("seq", None), flat, rows, rows, rows, flat, flat, rows, flat, rows, rows, rows, token),
        out_specs=(token, token, flat, rows, rows, rows, flat, flat, rows, flat, rows, rows, rows),
        check_vma=False,
    )
```

```python
import types

import jax
import jax.numpy as jnp
import numpy as np
from jax import lax
from jax.experimental import pallas as pl
from jax.experimental.pallas import tpu as pltpu
from jax.sharding import PartitionSpec as P

QUERY_HEAD_COUNT = 16
KEY_VALUE_HEADS = 8
HEAD_DIMENSION = 128

EPS = 1e-06
THETA = 1000000.0
NEGATIVE = -1e30
BF = jnp.bfloat16
F32 = jnp.float32
MESH = pl.DeviceIdType.MESH
RUN = 64
BLOCK = 256


def nn(a, b):
    return jnp.dot(a, b, preferred_element_type=F32)


def nt(a, b):
    return lax.dot_general(a, b, (((1,), (1,)), ((), ())), preferred_element_type=F32)


def tn(a, b):
    return lax.dot_general(a, b, (((0,), (0,)), ((), ())), preferred_element_type=F32)


def loop(low, high, body):
    def step(i, carry):
        body(i)
        return carry

    lax.fori_loop(low, high, step, 0)


def rows_of(start, size):
    return pl.ds(pl.multiple_of(start, size), size)


def inverse_root(values):
    return lax.rsqrt(jnp.mean(values * values, axis=-1, keepdims=True) + EPS)


def norm_backward(normed_grad, normed, inverse):
    return inverse * (normed_grad - normed * jnp.mean(normed_grad * normed, axis=-1, keepdims=True))


def layer_kernel(dims, refs):
    S, C, T, L, D = dims.S, dims.C, dims.T, dims.L, dims.D
    H, RW, OR, DR, AC, U = dims.H, dims.RW, dims.OR, dims.DR, dims.AC, dims.U
    HD = HEAD_DIMENSION
    PR = C * RW
    NR = L // RUN
    NB = L // BLOCK
    CH = C // 2
    scale = HD ** (-0.5)
    r = refs
    s = lax.axis_index("seq")
    c = lax.axis_index("ctx")
    chip = lax.div(c, 2)
    core = lax.rem(c, 2)
    chip_y, chip_x = lax.div(chip, 2), lax.rem(chip, 2)
    sibling = chip * 2 + (1 - core)
    flat = s * C + c
    to_s, to_c = lax.rem(flat, S), lax.div(flat, S)
    from_flat = S * c + s
    from_s, from_c = lax.div(from_flat, C), lax.rem(from_flat, C)
    moved = (to_s * C + to_c) != flat

    def partner(i):
        x = lax.rem(chip_x + lax.rem(i, 2), 2)
        y = lax.rem(chip_y + lax.div(i, 2), 2)
        return y * 2 + x

    def remote(src, dst, send, recv, **where):
        return pltpu.make_async_remote_copy(
            src_ref=src, dst_ref=dst, send_sem=send, recv_sem=recv, device_id=where, device_id_type=MESH
        )

    def local(src, dst, sem):
        return pltpu.make_async_copy(src, dst, sem)

    def arrived(dst, sem):
        pltpu.make_async_copy(dst, dst, sem).wait()

    barrier = pltpu.get_barrier_semaphore()

    def hello(**where):
        pl.semaphore_signal(barrier, inc=1, device_id=where, device_id_type=MESH)

    loop(1, C, lambda i: hello(ctx=lax.rem(c + i, C)))
    loop(1, S, lambda i: hello(seq=lax.rem(s + i, S)))

    @pl.when(moved)
    def _():
        hello(seq=to_s, ctx=to_c)
        hello(seq=from_s, ctx=from_c)

    @pl.when(moved)
    def _():
        pl.semaphore_wait(barrier, C + S)

    @pl.when(jnp.logical_not(moved))
    def _():
        pl.semaphore_wait(barrier, C + S - 2)

    def runs_of(b):
        return pl.ds(b * (BLOCK // RUN), BLOCK // RUN)

    def own_x():
        return r.x_all[pl.ds(c * (T // RUN), T // RUN)].reshape(T, D).astype(F32)

    X, G, H2, DY = 0, 1, 2, 3
    whole = {X: r.x_all, G: r.g_all, H2: r.h2_all, DY: r.dy_all}

    def block(kind, j):
        if kind == X:
            return whole[kind].at[pl.ds(j * (T // RUN), T // RUN)]
        return whole[kind].at[rows_of(j * T, T)]

    def gather_send(kind, src):
        def go(i):
            remote(src, block(kind, c), r.ag_send.at[kind, i], r.ag_recv.at[kind, c],
                   ctx=partner(i) * 2 + core).start()

        loop(1, CH, go)
        remote(src, block(kind, c), r.ag_send.at[kind, 0], r.ag_recv.at[kind, c], ctx=sibling).start()

    def gather_relay(kind, i):
        j = partner(i) * 2 + core
        arrived(block(kind, j), r.ag_recv.at[kind, j])
        remote(block(kind, j), block(kind, j), r.ag_send.at[kind, CH - 1 + i], r.ag_recv.at[kind, j],
               ctx=sibling).start()

    def gather_other(kind, i):
        j = partner(i) * 2 + (1 - core)
        arrived(block(kind, j), r.ag_recv.at[kind, j])

    def gather_done(kind):
        def go(i):
            arrived(block(kind, c), r.ag_send.at[kind, i])

        loop(0, 2 * CH - 1, go)

    def scatter_pair(kind, i, partial):
        r.pair[i] = partial
        r.s1[i] = r.pair[i, rows_of((1 - core) * T, T), :].astype(BF)
        remote(r.s1.at[i], r.r1.at[1 if kind == 1 else 0, i], r.rs_send.at[kind, i],
               r.r1_recv.at[kind, i], ctx=sibling).start()

    def scatter_chip(kind, i):
        bank = 1 if kind == 1 else 0
        arrived(r.r1.at[bank, i], r.r1_recv.at[kind, i])
        mine = r.pair[i, rows_of(core * T, T), :] + r.r1[bank, i].astype(F32)
        r.s2[i] = mine.astype(BF)
        remote(r.s2.at[i], r.r2.at[bank, i], r.rs_send.at[kind, CH + i],
               r.r2_recv.at[kind, i], ctx=partner(i) * 2 + core).start()

    def scatter(kind, partial):
        def go(k):
            i = lax.rem(k + 1, CH)
            scatter_pair(kind, i, partial(i))

            @pl.when(k > 0)
            def _():
                scatter_chip(kind, k)

        loop(0, CH, go)

    def scatter_sum(kind):
        bank = 1 if kind == 1 else 0
        arrived(r.r1.at[bank, 0], r.r1_recv.at[kind, 0])
        total = r.pair[0, rows_of(core * T, T), :] + r.r1[bank, 0].astype(F32)
        for i in range(1, CH):
            arrived(r.r2.at[bank, i], r.r2_recv.at[kind, i])
            total = total + r.r2[bank, i].astype(F32)
        return total

    def scatter_done(kind):
        loop(0, CH, lambda i: arrived(r.s1.at[0], r.rs_send.at[kind, i]))
        loop(1, CH, lambda i: arrived(r.s2.at[1], r.rs_send.at[kind, CH + i]))

    QKV, GATE, UP, OUT, DOWN = 0, 1, 2, 3, 4

    def plane(w, b):
        if w == QKV:
            return r.w_qkv.at[rows_of(b * PR, PR)]
        if w == GATE:
            return r.w_gu.at[rows_of(b * PR, PR), pl.ds(0, U)]
        if w == UP:
            return r.w_gu.at[rows_of(b * PR, PR), pl.ds(U, U)]
        return (r.z_o if w == OUT else r.z_d).at[b]

    def weight_start(w, src=None):
        src = plane(w, s) if src is None else src

        @pl.when(s < S - 1)
        def _():
            remote(src, plane(w, s), r.z_send.at[w, 0, 0], r.z_recv.at[w, s], seq=s + 1).start()

        @pl.when(s > 0)
        def _():
            remote(src, plane(w, s), r.z_send.at[w, 1, 0], r.z_recv.at[w, s], seq=s - 1).start()

    def weight_hop(w, t):
        below, above = s - 1 - t, s + 1 + t

        @pl.when(below >= 0)
        def _():
            arrived(plane(w, below), r.z_recv.at[w, below])

            @pl.when(s < S - 1)
            def _():
                remote(plane(w, below), plane(w, below), r.z_send.at[w, 0, t + 1],
                       r.z_recv.at[w, below], seq=s + 1).start()

        @pl.when(above <= S - 1)
        def _():
            arrived(plane(w, above), r.z_recv.at[w, above])

            @pl.when(s > 0)
            def _():
                remote(plane(w, above), plane(w, above), r.z_send.at[w, 1, t + 1],
                       r.z_recv.at[w, above], seq=s - 1).start()

    def weight_done(w):
        for t in range(S - 1):
            @pl.when(jnp.logical_and(s - t >= 0, s < S - 1))
            def _():
                arrived(plane(w, s), r.z_send.at[w, 0, t])

            @pl.when(jnp.logical_and(s + t <= S - 1, s > 0))
            def _():
                arrived(plane(w, s), r.z_send.at[w, 1, t])

    GU = GATE
    sent = {QKV: (r.g_qkv, PR), OUT: (r.g_o, OR), GU: (r.g_gu, PR), DOWN: (r.g_d, DR)}
    got = {QKV: r.t_qkv, OUT: r.t_o, GU: r.t_gu, DOWN: r.t_d}
    halfway = {QKV: r.c_qkv, OUT: r.c_o, GU: r.c_gu, DOWN: r.c_d}
    summed = {QKV: r.u_qkv, OUT: r.u_o, GU: r.u_gu, DOWN: r.u_d}
    side = jnp.where(s >= 2, 1, 0)

    def grad_rows(w, p):
        ref, size = sent[w]
        return ref.at[rows_of(p * size, size)]

    def grad_order(i):
        return jnp.where(s < 2, lax.rem(3 - i + s, S), lax.rem(i + (3 - s) * 3, S))

    def grad_direct(w, p):
        remote(grad_rows(w, p), got[w].at[side], r.gz_send.at[w, p], r.gz_recv.at[w, side], seq=p).start()

    def grad_out(w, p):
        far_up = jnp.logical_and(s == 0, p >= 2)
        far_down = jnp.logical_and(s == S - 1, p <= 1)
        later = jnp.logical_or(
            jnp.logical_and(s == 1, p >= 2), jnp.logical_and(s == 2, p <= 1)
        )

        @pl.when(far_up)
        def _():
            remote(grad_rows(w, p), halfway[w].at[p - 2], r.gz_send.at[w, p], r.gc_recv.at[w, p - 2],
                   seq=1).start()

        @pl.when(far_down)
        def _():
            remote(grad_rows(w, p), halfway[w].at[p], r.gz_send.at[w, p], r.gc_recv.at[w, p], seq=2).start()

        others = jnp.logical_or(jnp.logical_or(far_up, far_down), jnp.logical_or(later, p == s))

        @pl.when(jnp.logical_not(others))
        def _():
            grad_direct(w, p)

    def grad_combine(w, k):
        @pl.when(jnp.logical_or(s == 1, s == 2))
        def _():
            p = jnp.where(s == 1, 3 - k, k)
            slot = jnp.where(s == 1, 1 - k, k)
            ref, size = sent[w]
            rows = rows_of(p * size, size)
            arrived(halfway[w].at[slot], r.gc_recv.at[w, slot])
            ref[rows, :] = (ref[rows, :].astype(F32) + halfway[w][slot].astype(F32)).astype(BF)
            grad_direct(w, p)

    def grad_sum(w):
        ref, size = sent[w]
        total = ref[rows_of(s * size, size), :].astype(F32)
        for i in range(2):
            arrived(got[w].at[i], r.gz_recv.at[w, i])
            total = total + got[w][i].astype(F32)
        summed[w][...] = total.astype(BF)

    def grad_done(w):
        loop(1, S, lambda i: arrived(got[w].at[0], r.gz_send.at[w, lax.rem(s + i, S)]))

    final = {QKV: r.f_qkv, GU: r.f_gu, OUT: r.f_o, DOWN: r.f_d}

    def columns_send(n, w):
        def go(i):
            j = lax.rem(c + i, C)
            remote(summed[w].at[rows_of(j * RW, RW)], final[w].at[c], r.gp_send.at[n, i],
                   r.gp_recv.at[n, c], ctx=j).start()

        loop(1, C, go)
        final[w][c] = summed[w][rows_of(c * RW, RW), :]

    def columns_arrive(n, w):
        loop(1, C, lambda i: arrived(final[w].at[lax.rem(c + i, C)], r.gp_recv.at[n, lax.rem(c + i, C)]))

    def columns_done(n, w):
        loop(1, C, lambda i: arrived(final[w].at[0], r.gp_send.at[n, i]))

    def rows_send(n, w):
        @pl.when(moved)
        def _():
            remote(summed[w], final[w], r.row_send.at[n], r.row_recv.at[n], seq=from_s, ctx=from_c).start()

        @pl.when(jnp.logical_not(moved))
        def _():
            final[w][...] = summed[w][...]

    def rows_arrive(n, w):
        @pl.when(moved)
        def _():
            arrived(final[w], r.row_recv.at[n])

    def rows_done(n, w):
        @pl.when(moved)
        def _():
            arrived(final[w], r.row_send.at[n])

    gains_own = r.gains_all.at[flat]
    gain_copy = local(r.gains_in, gains_own, r.gain_recv.at[s])
    gain_copy.start()

    def gain_go(i):
        remote(r.gains_in, gains_own, r.gain_send.at[i], r.gain_recv.at[s],
               ctx=lax.rem(c + i, C)).start()

    loop(1, C, gain_go)

    def qkv_piece(j):
        return (
            (r.wq_in.at[:, rows_of(j * H * HD, H * HD)], slice(0, H * HD)),
            (r.wk_in.at[:, rows_of(j * HD, HD)], slice(H * HD, (H + 1) * HD)),
            (r.wv_in.at[:, rows_of(j * HD, HD)], slice((H + 1) * HD, (H + 2) * HD)),
        )

    def gu_piece(j):
        return (
            (r.wg_in.at[:, rows_of(j * U, U)], slice(0, U)),
            (r.wu_in.at[:, rows_of(j * U, U)], slice(U, 2 * U)),
        )

    columns_of = {QKV: r.w_qkv, GU: r.w_gu}

    def spread(n, w, piece):
        ref = columns_of[w]
        own = rows_of(s * PR + c * RW, RW)

        def go(i):
            j = lax.rem(c + i, C)
            for src, columns in piece(j):
                remote(src, ref.at[own, columns], r.w_send.at[n], r.w_recv.at[n], ctx=j).start()

        loop(1, C, go)
        for src, columns in piece(c):
            local(src, ref.at[own, columns], r.w_recv.at[n]).start()

    def spread_arrive(n, w):
        arrived(columns_of[w].at[rows_of(s * PR, PR)], r.w_recv.at[n])

    def spread_done(n, w):
        arrived(columns_of[w].at[pl.ds(0, (C - 1) * RW)], r.w_send.at[n])

    rows_ref = {OUT: (r.w_o, OR), DOWN: (r.w_d, DR)}

    def deal(n, w):
        ref, size = rows_ref[w]

        def go(b):
            d = C * b + c
            rank, spot = lax.div(d, S), lax.rem(d, S)
            dst = ref.at[rows_of(spot * size, size)]

            @pl.when(rank != c)
            def _():
                remote(plane(w, b), dst, r.m_send.at[n, b], r.m_recv.at[n], ctx=rank).start()

            @pl.when(rank == c)
            def _():
                local(plane(w, b), dst, r.m_recv.at[n]).start()

        loop(0, S, go)

    def deal_arrive(n, w):
        arrived(rows_ref[w][0], r.m_recv.at[n])

    def deal_done(n, w):
        def go(b):
            @pl.when(lax.div(C * b + c, S) != c)
            def _():
                arrived(plane(w, 0), r.m_send.at[n, b])

        loop(0, S, go)

    def own_rows(n, w, src):
        local(src, plane(w, s), r.local_sem.at[3 + n]).start()
        weight_start(w, src)

    own_rows(0, OUT, r.wo_in)
    spread(0, QKV, qkv_piece)
    local(r.x_in, block(X, c), r.local_sem.at[0]).start()
    local(r.table_in, r.table, r.local_sem.at[1]).start()
    gather_send(X, r.x_in)
    spread(1, GU, gu_piece)
    weight_hop(OUT, 0)
    spread_arrive(0, QKV)
    weight_start(QKV)
    arrived(r.gains_all.at[pl.ds(s * C, C)], r.gain_recv.at[s])

    def gain_far(i):
        mine = r.gains_all.at[pl.ds(s * C, C)]
        remote(mine, mine, r.gain_send.at[C + i], r.gain_recv.at[s], seq=lax.rem(s + i, S)).start()

    loop(1, S, gain_far)
    weight_hop(OUT, 1)

    arrived(r.table, r.local_sem.at[1])

    def tables(b):
        rows = rows_of(b * T, T)
        both = r.table[rows, :]
        other = pltpu.roll(both, HD // 2, 1)
        first = lax.broadcasted_iota(jnp.int32, (T, HD), 1) < HD // 2
        r.cosine[rows, :] = jnp.where(first, both, other)
        r.sine[rows, :] = jnp.where(first, -other, both)

    loop(0, L // T, tables)
    weight_hop(OUT, 2)
    arrived(plane(OUT, s), r.local_sem.at[3])
    deal(0, OUT)
    weight_hop(QKV, 0)
    arrived(block(X, c), r.local_sem.at[0])
    loop(1, CH, lambda i: gather_relay(X, i))
    local(r.g_in, block(G, c), r.local_sem.at[2]).start()
    gather_send(G, r.g_in)

    def gain_block(i):
        p = lax.rem(s + i, S)
        arrived(r.gains_all.at[pl.ds(p * C, C)], r.gain_recv.at[p])

    loop(1, S, gain_block)
    gains = jnp.sum(r.gains_all[...], axis=1).astype(BF)

    def gain_vector(offset, count):
        width = count * S * C
        shift = count.bit_length() - 1
        column = lax.broadcasted_iota(jnp.int32, (HD, width), 1)
        row = lax.broadcasted_iota(jnp.int32, (HD, width), 0)
        pick = jnp.where(row == offset + (column & (count - 1)), 1.0, 0.0).astype(BF)
        spread_out = nn(gains, pick)
        owner = lax.broadcasted_iota(jnp.int32, (S * C, width), 0)
        place = lax.broadcasted_iota(jnp.int32, (S * C, width), 1) >> shift
        return jnp.sum(jnp.where(owner == place, spread_out, 0.0), axis=0, keepdims=True)

    n1 = D // (S * C)
    n3 = HD // (S * C)
    r.gain1[...] = gain_vector(0, n1)
    r.gain2[...] = gain_vector(n1, n1)
    r.gainq[...] = gain_vector(2 * n1, n3)
    r.gaink[...] = gain_vector(2 * n1 + n3, n3)

    arrived(block(X, sibling), r.ag_recv.at[X, sibling])
    loop(1, CH, lambda i: gather_other(X, i))

    def first_norm(k):
        x = r.x_all[r.order[1, k]].astype(F32)
        r.h1[rows_of(k * RUN, RUN), :] = (x * inverse_root(x) * r.gain1[...]).astype(BF)

    loop(0, NR, first_norm)
    weight_hop(QKV, 1)
    spread_arrive(1, GU)
    weight_start(GATE)
    weight_hop(QKV, 2)

    def rotate(u, rows):
        return u * r.cosine[rows, :] + pltpu.roll(u, HD // 2, 1) * r.sine[rows, :]

    def rotate_back(u, rows):
        return u * r.cosine[rows, :] - pltpu.roll(u, HD // 2, 1) * r.sine[rows, :]

    def project(b):
        rows = rows_of(b * BLOCK, BLOCK)
        acc = nn(r.h1[rows, :], r.w_qkv[...])
        for h in range(H):
            u = acc[:, h * HD : (h + 1) * HD]
            r.q_lin[h, rows, :] = u
            r.q_rot[h, rows, :] = rotate(u * inverse_root(u) * r.gainq[...], rows).astype(BF)
        u = acc[:, H * HD : (H + 1) * HD]
        r.k_lin[rows, :] = u
        k = rotate(u * inverse_root(u) * r.gaink[...], rows)
        r.k_rot[rows, :] = k.astype(BF)
        r.k_t[:, rows] = k.T.astype(BF)
        v = acc[:, (H + 1) * HD :]
        r.v[rows, :] = v.astype(BF)
        r.v_t[:, rows] = v.T.astype(BF)

    loop(0, NB, project)
    loop(1, CH, lambda i: gather_relay(G, i))

    def attend(qb):
        @pl.when(qb == NB - 2)
        def _():
            weight_hop(GATE, 0)
            weight_start(UP)

        cols = rows_of(qb * BLOCK, BLOCK)

        def keys(kb, carry):
            rows = rows_of(kb * BLOCK, BLOCK)
            key = r.k_rot[rows, :]
            value_t = r.v_t[:, rows]
            ahead = lax.broadcasted_iota(jnp.int32, (BLOCK, BLOCK), 0) - lax.broadcasted_iota(
                jnp.int32, (BLOCK, BLOCK), 1
            )
            allowed = ahead <= (qb - kb) * BLOCK
            out = []
            for h in range(H):
                acc, total = carry[2 * h], carry[2 * h + 1]
                e = jnp.exp(nt(key, r.q_rot[h, cols, :]) * scale)
                e = jnp.where(allowed, e, 0.0)
                low = e.astype(BF)
                r.e[h, rows, cols] = low
                out += [acc + nn(value_t, low), total + jnp.sum(e, axis=0, keepdims=True)]
            return tuple(out)

        zero = (jnp.zeros((HD, BLOCK), F32), jnp.zeros((1, BLOCK), F32)) * H
        done = lax.fori_loop(0, qb + 1, keys, zero)
        for h in range(H):
            inverse = 1.0 / done[2 * h + 1]
            o = done[2 * h] * inverse
            r.l_inv[h, :, cols] = jnp.broadcast_to(inverse, (8, BLOCK))
            r.o_t[h, :, cols] = o
            r.o_sorted[runs_of(qb), :, h * HD : (h + 1) * HD] = o.T.astype(BF).reshape(-1, RUN, HD)

    loop(0, NB, attend)
    def unsort(i):
        r.o[rows_of(i * RUN, RUN), :] = r.o_sorted[r.order[0, i]]

    loop(0, NR, unsort)

    deal_arrive(0, OUT)
    scatter(0, lambda i: nn(r.o[rows_of(partner(i) * 2 * T, 2 * T), :], r.w_o[...]))
    weight_hop(GATE, 1)
    own_rows(1, DOWN, r.wd_in)
    weight_hop(UP, 0)
    weight_hop(GATE, 2)
    weight_hop(UP, 1)
    y1 = own_x() + scatter_sum(0)
    scatter_done(0)
    r.y1[...] = y1
    h2_own = (y1 * inverse_root(y1) * r.gain2[...]).astype(BF)
    r.h2_all[rows_of(c * T, T), :] = h2_own
    gather_send(H2, block(H2, c))

    weight_hop(UP, 2)
    arrived(block(G, c), r.local_sem.at[2])
    arrived(block(G, sibling), r.ag_recv.at[G, sibling])
    loop(1, CH, lambda i: gather_other(G, i))
    arrived(block(H2, sibling), r.ag_recv.at[H2, sibling])

    def feed(i):
        @pl.when(i > 0)
        def _():
            gather_relay(H2, i)
            gather_other(H2, i)

        @pl.when(i == 1)
        def _():
            weight_hop(DOWN, 0)

        @pl.when(i == 2)
        def _():
            weight_hop(DOWN, 1)

        rows = rows_of(partner(i) * 2 * T, 2 * T)
        h2 = r.h2_all[rows, :]
        gate = nn(h2, r.w_gu[:, :U])
        up = nn(h2, r.w_gu[:, U:])
        sig = 1.0 / (1.0 + jnp.exp(-gate))
        silu = gate * sig
        r.act[rows, :] = (silu * up).astype(BF)
        r.slope[rows, :] = up * sig * (1.0 + gate * (1.0 - sig))
        r.silu[rows, :] = silu

    loop(0, CH, feed)
    weight_hop(DOWN, 2)
    arrived(plane(DOWN, s), r.local_sem.at[4])
    deal(1, DOWN)
    deal_arrive(1, DOWN)

    def feed_back(i):
        rows = rows_of(partner(i) * 2 * T, 2 * T)
        d_act = nt(r.g_all[rows, :], r.w_d[...])
        r.d_gu[rows, :U] = (d_act * r.slope[rows, :]).astype(BF)
        r.d_gu[rows, U:] = (d_act * r.silu[rows, :]).astype(BF)
        return nt(r.d_gu[rows, :], r.w_gu[...])

    scatter(2, feed_back)

    def down_grad(m):
        cols = rows_of(m * HD, HD)
        r.g_d[cols, :] = tn(r.act[:, cols], r.g_all[...]).astype(BF)

    loop(0, U // HD, down_grad)
    loop(0, S, lambda i: grad_out(DOWN, grad_order(i)))

    def gu_grad(i):
        p = grad_order(i)
        cols = rows_of(p * PR, PR)
        r.g_gu[cols, :] = tn(r.h2_all[:, cols], r.d_gu[...]).astype(BF)
        grad_out(GU, p)

    loop(0, S, gu_grad)
    grad_combine(DOWN, 0)
    grad_combine(DOWN, 1)

    d_h2 = scatter_sum(2)
    scatter_done(2)
    y1 = r.y1[...]
    r2 = inverse_root(y1)
    normed = y1 * r2
    term2 = jnp.sum(d_h2 * normed, axis=0, keepdims=True)
    d_y1 = r.g_all[rows_of(c * T, T), :].astype(F32) + norm_backward(d_h2 * r.gain2[...], normed, r2)
    r.d_y1[...] = d_y1
    r.dy_all[rows_of(c * T, T), :] = d_y1.astype(BF)
    gather_send(DY, block(DY, c))
    WT = D // HD
    for k in range(WT):
        r.terms[WT + k : WT + k + 1, :] = term2[:, k * HD : (k + 1) * HD]

    scatter(1, lambda i: nn(r.act[rows_of(partner(i) * 2 * T, 2 * T), :], r.w_d[...]))
    arrived(block(DY, sibling), r.ag_recv.at[DY, sibling])

    def out_grad(i):
        @pl.when(i > 0)
        def _():
            gather_relay(DY, i)
            gather_other(DY, i)

        rows = rows_of(partner(i) * 2 * T, 2 * T)
        d_o = nt(r.dy_all[rows, :], r.w_o[...]).astype(BF)
        r.d_o[pl.ds(partner(i) * (2 * T // RUN), 2 * T // RUN)] = d_o.reshape(-1, RUN, H * HD)

    loop(0, CH, out_grad)

    def out_weight(m):
        cols = rows_of(m * HD, HD)
        r.g_o[cols, :] = tn(r.o[:, cols], r.dy_all[...]).astype(BF)

    loop(0, H * HD // HD, out_weight)
    loop(0, S, lambda i: grad_out(OUT, grad_order(i)))
    grad_combine(GU, 0)

    def sort(k):
        r.d_o_sorted[rows_of(k * RUN, RUN), :] = r.d_o[r.order[1, k]]

    loop(0, NR, sort)
    r.d_k[...] = jnp.zeros_like(r.d_k)
    r.d_v[...] = jnp.zeros_like(r.d_v)
    r.sums[...] = jnp.zeros_like(r.sums)

    def attend_back(qb):
        cols = rows_of(qb * BLOCK, BLOCK)
        d_o_t, d_o_low, row, factor = [], [], [], []
        for h in range(H):
            t = r.d_o_sorted[cols, h * HD : (h + 1) * HD].astype(F32).T
            inverse = r.l_inv[h, 0:1, cols]
            row.append(jnp.sum(t * r.o_t[h, :, cols], axis=0, keepdims=True))
            factor.append(inverse * scale)
            r.do_t[h] = t.astype(BF)
            r.do_l[h] = (t * inverse).T.astype(BF)

        def keys(kb, carry):
            rows = rows_of(kb * BLOCK, BLOCK)
            value = r.v[rows, :]
            key_t = r.k_t[:, rows]
            out = []
            d_k = r.d_k[rows, :]
            d_v = r.d_v[rows, :]
            for h in range(H):
                e = r.e[h, rows, cols]
                dp = nn(value, r.do_t[h])
                de = (e.astype(F32) * ((dp - row[h]) * factor[h])).astype(BF)
                out.append(carry[h] + nn(key_t, de))
                d_k = d_k + nn(de, r.q_rot[h, cols, :])
                d_v = d_v + nn(e, r.do_l[h])
            r.d_k[rows, :] = d_k
            r.d_v[rows, :] = d_v
            return tuple(out)

        done = lax.fori_loop(0, qb + 1, keys, (jnp.zeros((HD, BLOCK), F32),) * H)
        for h in range(H):
            d_g = rotate_back(done[h].T, cols)
            u = r.q_lin[h, cols, :]
            inverse = inverse_root(u)
            normed = u * inverse
            r.sums[0:1, :] += jnp.sum(d_g * normed, axis=0, keepdims=True)
            d_lin = norm_backward(d_g * r.gainq[...], normed, inverse).astype(BF)
            r.d_qkv[runs_of(qb), :, h * HD : (h + 1) * HD] = d_lin.reshape(-1, RUN, HD)

    loop(0, NB, attend_back)

    def key_back(b):
        rows = rows_of(b * BLOCK, BLOCK)
        d_g = rotate_back(r.d_k[rows, :], rows)
        u = r.k_lin[rows, :]
        inverse = inverse_root(u)
        normed = u * inverse
        r.sums[1:2, :] += jnp.sum(d_g * normed, axis=0, keepdims=True)
        d_lin = norm_backward(d_g * r.gaink[...], normed, inverse).astype(BF)
        r.d_qkv[runs_of(b), :, H * HD : (H + 1) * HD] = d_lin.reshape(-1, RUN, HD)
        r.d_qkv[runs_of(b), :, (H + 1) * HD :] = r.d_v[rows, :].astype(BF).reshape(-1, RUN, HD)

    loop(0, NB, key_back)

    def qkv_grad(i):
        p = grad_order(i)
        cols = rows_of(p * PR, PR)
        r.g_qkv[cols, :] = tn(r.h1[:, cols], r.d_qkv[...].reshape(L, AC)).astype(BF)
        grad_out(QKV, p)

    loop(0, S, qkv_grad)
    grad_combine(GU, 1)

    r.y_out[...] = (r.y1[...] + scatter_sum(1)).astype(BF)
    local(r.y_out, r.layer_out, r.out_sem.at[0]).start()
    scatter_done(1)

    def in_chip(i):
        j = partner(i) * 2
        parts = []
        for k in range(2 * T // RUN):
            parts.append(r.d_qkv[r.order[0, j * (T // RUN) + k]])
        return nt(jnp.concatenate(parts, axis=0), r.w_qkv[...])

    scatter(3, in_chip)
    grad_sum(DOWN)
    rows_send(1, DOWN)
    grad_combine(OUT, 0)
    grad_combine(OUT, 1)
    grad_sum(GU)
    columns_send(1, GU)
    grad_combine(QKV, 0)
    d_h1 = scatter_sum(3)
    x = own_x()
    r1 = inverse_root(x)
    normed = x * r1
    term1 = jnp.sum(d_h1 * normed, axis=0, keepdims=True)
    r.x_grad[...] = r.d_y1[...] + norm_backward(d_h1 * r.gain1[...], normed, r1)
    local(r.x_grad, r.hidden_grad, r.out_sem.at[1]).start()
    for k in range(WT):
        r.terms[k : k + 1, :] = term1[:, k * HD : (k + 1) * HD]
    r.terms[2 * WT : 2 * WT + 8, :] = r.sums[...]

    def terms_far(i):
        remote(r.terms, r.terms_z.at[s], r.t_send.at[i], r.t_recv.at[s],
               seq=lax.rem(s + i, S)).start()

    loop(1, S, terms_far)
    grad_combine(QKV, 1)
    grad_sum(OUT)
    rows_send(0, OUT)
    grad_sum(QKV)
    columns_send(0, QKV)
    total = r.terms[...]
    for i in range(1, S):
        p = lax.rem(s + i, S)
        arrived(r.terms_z.at[p], r.t_recv.at[p])
        total = total + r.terms_z[p]
    r.terms_sum[...] = total

    def terms_near(i):
        remote(r.terms_sum, r.terms_p.at[c], r.t_send.at[S + i], r.t_recv.at[S + c],
               ctx=lax.rem(c + i, C)).start()

    loop(1, C, terms_near)

    rows_arrive(1, DOWN)
    local(r.f_d, r.down_out, r.out_sem.at[2]).start()
    columns_arrive(1, GU)
    local(r.f_gu, r.gu_out, r.out_sem.at[3]).start()
    rows_arrive(0, OUT)
    local(r.f_o, r.o_out, r.out_sem.at[4]).start()
    columns_arrive(0, QKV)
    local(r.f_qkv, r.qkv_out, r.out_sem.at[5]).start()
    total = r.terms_sum[...]
    for i in range(1, C):
        j = lax.rem(c + i, C)
        arrived(r.terms_p.at[j], r.t_recv.at[S + j])
        total = total + r.terms_p[j]
    r.terms_all[...] = total
    local(r.terms_all, r.terms_out, r.out_sem.at[6]).start()

    loop(1, C, lambda i: arrived(gains_own, r.gain_send.at[i]))
    loop(1, S, lambda i: arrived(r.gains_all.at[pl.ds(0, C)], r.gain_send.at[C + i]))
    for kind in (X, G, H2, DY):
        gather_done(kind)
    spread_done(0, QKV)
    spread_done(1, GU)
    deal_done(0, OUT)
    deal_done(1, DOWN)
    for w in (QKV, GATE, UP, OUT, DOWN):
        weight_done(w)
    for w in (QKV, OUT, GU, DOWN):
        grad_done(w)
    columns_done(0, QKV)
    columns_done(1, GU)
    rows_done(0, OUT)
    rows_done(1, DOWN)
    scatter_done(3)
    loop(1, S, lambda i: arrived(r.terms, r.t_send.at[i]))
    loop(1, C, lambda i: arrived(r.terms, r.t_send.at[S + i]))
    pairs = (
        (r.y_out, r.layer_out), (r.x_grad, r.hidden_grad), (r.f_d, r.down_out), (r.f_gu, r.gu_out),
        (r.f_o, r.o_out), (r.f_qkv, r.qkv_out), (r.terms_all, r.terms_out),
    )
    for k, (src, dst) in enumerate(pairs):
        local(src, dst, r.out_sem.at[k]).wait()


def finish_kernel(dims, refs):
    S, C, D, H, U = dims.S, dims.C, dims.D, dims.H, dims.U
    HD = HEAD_DIMENSION
    r = refs
    me = lax.axis_index("seq") * C + lax.axis_index("ctx")
    r.layer_res[...] = r.layer_out[...]
    r.hidden_res[...] = r.hidden_grad[...]
    r.delta_down[...] = r.down_out[...].astype(F32)
    r.delta_out[...] = r.o_out[...].astype(F32)
    for j in range(C):
        r.delta_gate[:, j * U : (j + 1) * U] = r.gu_out[j, :, :U].astype(F32)
        r.delta_up[:, j * U : (j + 1) * U] = r.gu_out[j, :, U:].astype(F32)
        r.delta_query[:, j * H * HD : (j + 1) * H * HD] = r.qkv_out[j, :, : H * HD].astype(F32)
        r.delta_key[:, j * HD : (j + 1) * HD] = r.qkv_out[j, :, H * HD : (H + 1) * HD].astype(F32)
        r.delta_value[:, j * HD : (j + 1) * HD] = r.qkv_out[j, :, (H + 1) * HD :].astype(F32)

    def own(ref, first_row, count):
        start = me * count
        row = r.terms_out[pl.ds(first_row + lax.div(start, HD), 1), :]
        back = lax.rem(HD - lax.rem(start, HD), HD)
        ref[...] = pltpu.roll(jnp.broadcast_to(row, (8, HD)), back, 1)[0:1, :count]

    n1, n3 = D // (S * C), HD // (S * C)
    own(r.change1, 0, n1)
    own(r.change2, D // HD, n1)
    own(r.changeq, 2 * (D // HD), n3)
    own(r.changek, 2 * (D // HD) + 1, n3)


def fused_layer(mesh, args):
    (x, positions, gain1, wq, wk, wv, gainq, gaink, wo, gain2, wg, wu, wd, g) = args
    S, C = mesh.shape["seq"], mesh.shape["ctx"]
    T, D = x.shape[1:]
    L = positions.shape[1]
    HD = HEAD_DIMENSION
    H = QUERY_HEAD_COUNT // C
    RW, OR, DR = wq.shape[0], wo.shape[0], wd.shape[0]
    U = wg.shape[1] // C
    AC = (H + 2) * HD
    PR = C * RW
    CH = C // 2
    dims = types.SimpleNamespace(S=S, C=C, T=T, L=L, D=D, H=H, RW=RW, OR=OR, DR=DR, AC=AC, U=U)
    packed = jnp.concatenate([gain1, gain2, gainq, gaink]).astype(F32)
    packed = jnp.pad(packed[None, :], ((0, 7), (0, HD - packed.shape[0])))
    half = HD // 2
    frequency = np.power(THETA, -np.arange(half) * (2.0 / HD))
    phases = np.arange(L)[:, None] * frequency[None, :]
    table = jnp.asarray(np.concatenate([np.cos(phases), np.sin(phases)], axis=1), F32)
    TR = 2 * (D // HD) + 8
    run = positions[0, ::RUN] // RUN
    spot = jnp.arange(L // RUN, dtype=jnp.int32)
    place = jnp.sum(jnp.where(run[None, :] == spot[:, None], spot[None, :], 0), axis=1)
    order = jnp.stack([run, place]).astype(jnp.int32)
    inputs = dict(
        order=order, x_in=x.reshape(T // RUN, RUN, D), g_in=g[0], gains_in=packed, wq_in=wq, wk_in=wk, wv_in=wv, wo_in=wo,
        wg_in=wg, wu_in=wu, wd_in=wd, table_in=table,
    )
    TR_shape = ((TR, HD), F32)
    outputs = dict(
        layer_out=((T, D), BF), hidden_grad=((T, D), F32), qkv_out=((C, RW, AC), BF), o_out=((OR, D), BF),
        gu_out=((C, RW, 2 * U), BF), down_out=((DR, D), BF), terms_out=TR_shape,
    )
    n1, n3 = D // (S * C), HD // (S * C)
    final = dict(
        layer_res=((T, D), BF), hidden_res=((T, D), F32), change1=((1, n1), F32),
        delta_query=((RW, C * H * HD), F32), delta_key=((RW, C * HD), F32), delta_value=((RW, C * HD), F32),
        changeq=((1, n3), F32), changek=((1, n3), F32), delta_out=((OR, D), F32), change2=((1, n1), F32),
        delta_gate=((RW, C * U), F32), delta_up=((RW, C * U), F32), delta_down=((DR, D), F32),
    )
    V, DMA = pltpu.VMEM, pltpu.SemaphoreType.DMA
    scratch = dict(
        x_all=V((L // RUN, RUN, D), BF), g_all=V((L, D), BF), h2_all=V((L, D), BF), dy_all=V((L, D), BF),
        h1=V((L, D), BF), w_qkv=V((D, AC), BF), w_o=V((H * HD, D), BF), w_gu=V((D, 2 * U), BF),
        w_d=V((U, D), BF), gains_all=V((S * C, 8, HD), F32), table=V((L, HD), F32),
        cosine=V((L, HD), F32), sine=V((L, HD), F32), gain1=V((1, D), F32), gain2=V((1, D), F32),
        gainq=V((1, HD), F32), gaink=V((1, HD), F32), q_lin=V((H, L, HD), F32), k_lin=V((L, HD), F32),
        q_rot=V((H, L, HD), BF), k_rot=V((L, HD), BF), v=V((L, HD), BF), k_t=V((HD, L), BF),
        v_t=V((HD, L), BF), e=V((H, L, L), BF), l_inv=V((H, 8, L), F32), o_t=V((H, HD, L), F32),
        o_sorted=V((L // RUN, RUN, H * HD), BF), o=V((L, H * HD), BF), y1=V((T, D), F32), slope=V((L, U), F32), silu=V((L, U), F32),
        act=V((L, U), BF), d_gu=V((L, 2 * U), BF), d_y1=V((T, D), F32), d_o=V((L // RUN, RUN, H * HD), BF),
        d_o_sorted=V((L, H * HD), BF), do_t=V((H, HD, BLOCK), BF), do_l=V((H, BLOCK, HD), BF),
        d_k=V((L, HD), F32), d_v=V((L, HD), F32), d_qkv=V((L // RUN, RUN, AC), BF), sums=V((8, HD), F32),
        pair=V((CH, 2 * T, D), F32), s1=V((CH, T, D), BF), r1=V((2, CH, T, D), BF),
        s2=V((CH, T, D), BF), r2=V((2, CH, T, D), BF),
        g_qkv=V((D, AC), BF), g_o=V((H * HD, D), BF), g_gu=V((D, 2 * U), BF), g_d=V((U, D), BF),
        t_qkv=V((2, PR, AC), BF), t_o=V((2, OR, D), BF), t_gu=V((2, PR, 2 * U), BF), t_d=V((2, DR, D), BF),
        c_qkv=V((2, PR, AC), BF), c_o=V((2, OR, D), BF), c_gu=V((2, PR, 2 * U), BF), c_d=V((2, DR, D), BF),
        z_o=V((S, OR, D), BF), z_d=V((S, DR, D), BF), y_out=V((T, D), BF), x_grad=V((T, D), F32), terms_all=V(*TR_shape),
        u_qkv=V((PR, AC), BF), u_o=V((OR, D), BF), u_gu=V((PR, 2 * U), BF), u_d=V((DR, D), BF),
        f_qkv=V((C, RW, AC), BF), f_o=V((OR, D), BF), f_gu=V((C, RW, 2 * U), BF), f_d=V((DR, D), BF),
        terms=V((TR, HD), F32), terms_z=V((S, TR, HD), F32), terms_sum=V((TR, HD), F32),
        terms_p=V((C, TR, HD), F32),
        ag_send=DMA((4, 2 * CH)), ag_recv=DMA((4, C)), rs_send=DMA((4, 2 * CH)), r1_recv=DMA((4, CH)),
        r2_recv=DMA((4, CH)), z_send=DMA((5, 2, S)), z_recv=DMA((5, S)), gz_send=DMA((5, S)),
        gz_recv=DMA((5, 2)), gc_recv=DMA((5, 2)), gp_send=DMA((2, C)), gp_recv=DMA((2, C)), row_send=DMA((2,)),
        row_recv=DMA((2,)), w_send=DMA((2,)), w_recv=DMA((2,)), m_send=DMA((2, S)), m_recv=DMA((2,)),
        gain_send=DMA((C + S,)), gain_recv=DMA((S,)), t_send=DMA((S + C,)), t_recv=DMA((S + C,)),
        local_sem=DMA((5,)), out_sem=DMA((7,)),
    )
    names = list(inputs) + list(outputs) + list(scratch)

    def kernel(*refs):
        layer_kernel(dims, types.SimpleNamespace(**dict(zip(names, refs))))

    in_specs = [
        pl.BlockSpec(memory_space=pltpu.SMEM if name == "order" else pl.ANY) for name in inputs
    ]
    results = pl.pallas_call(
        kernel,
        out_shape=[jax.ShapeDtypeStruct(*v) for v in outputs.values()],
        in_specs=in_specs,
        out_specs=[pl.BlockSpec(memory_space=pl.ANY)] * len(outputs),
        scratch_shapes=list(scratch.values()),
        compiler_params=pltpu.CompilerParams(
            collective_id=0, has_side_effects=True, vmem_limit_bytes=67043328
        ),
        name="layer",
    )(*inputs.values())
    finish_names = list(outputs) + list(final)

    def finish(*refs):
        finish_kernel(dims, types.SimpleNamespace(**dict(zip(finish_names, refs))))

    out = pl.pallas_call(
        finish,
        out_shape=[jax.ShapeDtypeStruct(*v) for v in final.values()],
        in_specs=[pl.BlockSpec(memory_space=pltpu.VMEM)] * len(outputs),
        out_specs=[pl.BlockSpec(memory_space=pltpu.VMEM)] * len(final),
        name="finish",
    )(*results)
    one_axis = [k for k, v in enumerate(final.values()) if v[0][0] == 1]
    out = [o.reshape(-1) if k in one_axis else o for k, o in enumerate(out)]
    return (out[0][None], out[1][None], *out[2:])


def angles(places, head_size):
    half_size = head_size // 2
    frequency = jnp.power(THETA, -jnp.arange(half_size, dtype=F32) * (2.0 / head_size))
    phases = places.astype(F32)[:, None] * frequency[None, :]
    phases = jnp.concatenate([phases, phases], axis=-1)
    return (jnp.cos(phases), jnp.sin(phases))


def rotate(values, cosines, sines):
    half_size = values.shape[-1] // 2
    turned = jnp.concatenate([-values[..., half_size:], values[..., :half_size]], axis=-1)
    return values * cosines + turned * sines


def rotate_back(upstream, cosines, sines):
    half_size = upstream.shape[-1] // 2
    scaled = upstream * sines
    turned = jnp.concatenate([scaled[..., half_size:], -scaled[..., :half_size]], axis=-1)
    return upstream * cosines + turned


def dot(a, b):
    return jnp.dot(a, b, preferred_element_type=F32)


def local_of(mesh):
    seqs, ranks = mesh.shape["seq"], mesh.shape["ctx"]
    devices = seqs * ranks
    axes = ("seq", "ctx")

    def spread(shard, heads):
        rows, columns = shard.shape
        if heads and heads < ranks:
            blocks = shard.reshape(rows, heads, 1, columns // heads)
            blocks = jnp.broadcast_to(blocks, (rows, heads, ranks // heads, columns // heads))
            return blocks.reshape(rows, ranks, columns // heads)
        return shard.reshape(rows, ranks, columns // ranks)

    def fold(blocks, heads):
        rows, count, width = blocks.shape
        if heads and heads < ranks:
            return blocks.reshape(rows, heads, count // heads, width).sum(2).reshape(rows, heads * width)
        return blocks.reshape(rows, count * width)

    forth = [(seqs * r + j, j * ranks + r) for r in range(ranks) for j in range(seqs)]
    back = [(b, a) for a, b in forth]

    def local(
        hidden_states, positions, gain_first, weight_query, key_weight_matrix, value_weight_matrix,
        gain_query, gain_key, weight_output, gain_second, weight_gate, weight_up, weight_down,
        output_cotangent,
    ):
        tokens = hidden_states.shape[1]
        length = positions.shape[1]
        size = HEAD_DIMENSION
        group = QUERY_HEAD_COUNT // KEY_VALUE_HEADS
        my_q = QUERY_HEAD_COUNT // ranks
        my_k = max(1, KEY_VALUE_HEADS // ranks)
        scale = size ** (-0.5)
        places = positions[0]
        cosines, sines = angles(places, size)
        cosines, sines = cosines[:, None, :], sines[:, None, :]

        gains = jnp.concatenate([gain_first, gain_second, gain_query, gain_key])
        gains = lax.all_gather(gains, axes, axis=0).astype(F32)
        n1, n2, n3, n4 = (g.shape[0] for g in (gain_first, gain_second, gain_query, gain_key))
        first_scale = gains[:, :n1].reshape(-1)
        second_scale = gains[:, n1 : n1 + n2].reshape(-1)
        query_scale = gains[:, n1 + n2 : n1 + n2 + n3].reshape(-1)
        key_scale = gains[:, n1 + n2 + n3 :].reshape(-1)

        column_weights = jnp.concatenate(
            [
                spread(weight_query, 0),
                spread(key_weight_matrix, KEY_VALUE_HEADS),
                spread(value_weight_matrix, KEY_VALUE_HEADS),
                spread(weight_gate, 0),
                spread(weight_up, 0),
            ],
            axis=2,
        )
        column_weights = lax.all_to_all(column_weights, "ctx", split_axis=1, concat_axis=0, tiled=True)
        column_weights = lax.all_gather(column_weights[:, 0], "seq", axis=0, tiled=True)
        row_weights = jnp.concatenate([weight_output, weight_down], axis=0)
        row_weights = lax.all_gather(lax.ppermute(row_weights, axes, forth), "seq", axis=0)
        o_rows, d_rows = weight_output.shape[0], weight_down.shape[0]
        width = weight_output.shape[1]
        w_o = row_weights[:, :o_rows].reshape(-1, width)
        w_d = row_weights[:, o_rows:].reshape(-1, width)
        units = w_d.shape[0]
        attn_columns = (my_q + 2 * my_k) * size
        w_qkv = column_weights[:, :attn_columns]
        w_gu = column_weights[:, attn_columns:]

        x = lax.all_gather(hidden_states[0], "ctx", axis=0, tiled=True).astype(F32)
        g_low = lax.all_gather(output_cotangent[0], "ctx", axis=0, tiled=True)
        first_inverse = inverse_root(x)
        h1 = (x * first_inverse * first_scale).astype(BF)
        qkv = dot(h1, w_qkv)
        q_lin = qkv[:, : my_q * size].reshape(length, my_q, size)
        k_lin = qkv[:, my_q * size : (my_q + my_k) * size].reshape(length, my_k, size)
        v = qkv[:, (my_q + my_k) * size :].astype(BF).reshape(length, my_k, size)
        rq, rk = inverse_root(q_lin), inverse_root(k_lin)
        nq, nk = q_lin * rq, k_lin * rk
        qr = rotate(nq * query_scale, cosines, sines).astype(BF)
        kr = rotate(nk * key_scale, cosines, sines).astype(BF)
        mask = places[None, :] <= places[:, None]

        def scores(h):
            e = lax.dot_general(
                qr[:, h], kr[:, h // group], (((1,), (1,)), ((), ())), preferred_element_type=F32
            )
            return jnp.where(mask, e * scale, NEGATIVE)

        outs, probs = [], []
        for h in range(my_q):
            e = scores(h)
            p = jnp.exp(e - jnp.max(e, axis=-1, keepdims=True))
            p = p / jnp.sum(p, axis=-1, keepdims=True)
            probs.append(p)
            outs.append(dot(p.astype(BF), v[:, h // group]))
        o = jnp.concatenate(outs, axis=1).astype(BF)

        def scatter(part):
            return lax.psum_scatter(part.astype(BF), "ctx", scatter_dimension=0, tiled=True).astype(F32)

        x_own = hidden_states[0].astype(F32)
        y1 = x_own + scatter(dot(o, w_o))
        r2 = inverse_root(y1)
        second_normed = y1 * r2
        h2 = lax.all_gather((second_normed * second_scale).astype(BF), "ctx", axis=0, tiled=True)
        gu = dot(h2, w_gu)
        gate, up = gu[:, :units], gu[:, units:]
        sig = jax.nn.sigmoid(gate)
        silu = gate * sig
        act = (silu * up).astype(BF)
        layer_output = (y1 + scatter(dot(act, w_d))).astype(BF)

        d_act = dot(g_low, w_d.T)
        d_gate = (d_act * up * sig * (1.0 + gate * (1.0 - sig))).astype(BF)
        d_up = (d_act * silu).astype(BF)
        d_gu = jnp.concatenate([d_gate, d_up], axis=1)
        d_h2 = scatter(dot(d_gu, w_gu.T))
        second_term = jnp.sum(d_h2 * second_normed, axis=0)
        d_y1 = output_cotangent[0].astype(F32) + norm_backward(d_h2 * second_scale, second_normed, r2)
        d_y1_low = lax.all_gather(d_y1.astype(BF), "ctx", axis=0, tiled=True)
        d_o = dot(d_y1_low, w_o.T).astype(BF).reshape(length, my_q, size)

        d_q, d_k, d_v = [], [0.0] * my_k, [0.0] * my_k
        for h in range(my_q):
            p = probs[h]
            dp = lax.dot_general(
                d_o[:, h], v[:, h // group], (((1,), (1,)), ((), ())), preferred_element_type=F32
            )
            row = jnp.sum(p * dp, axis=-1, keepdims=True)
            de = (p * (dp - row) * scale).astype(BF)
            d_q.append(dot(de, kr[:, h // group]))
            d_k[h // group] += dot(de.T, qr[:, h])
            d_v[h // group] += dot(p.astype(BF).T, d_o[:, h])
        d_q, d_k, d_v = jnp.stack(d_q, 1), jnp.stack(d_k, 1), jnp.stack(d_v, 1)
        d_gq, d_gk = rotate_back(d_q, cosines, sines), rotate_back(d_k, cosines, sines)
        query_term = jnp.sum(d_gq * nq, axis=(0, 1))
        key_term = jnp.sum(d_gk * nk, axis=(0, 1))
        d_qlin = norm_backward(d_gq * query_scale, nq, rq).reshape(length, -1)
        d_klin = norm_backward(d_gk * key_scale, nk, rk).reshape(length, -1)
        d_qkv = jnp.concatenate([d_qlin, d_klin, d_v.reshape(length, -1)], axis=1).astype(BF)
        d_h1 = scatter(dot(d_qkv, w_qkv.T))
        r1 = inverse_root(x_own)
        first_normed = x_own * r1
        first_term = jnp.sum(d_h1 * first_normed, axis=0)
        hidden_gradient = d_y1 + norm_backward(d_h1 * first_scale, first_normed, r1)

        def rows_sum(part):
            part = lax.psum_scatter(part.astype(BF), "seq", scatter_dimension=0, tiled=True)
            return lax.ppermute(part, axes, back).astype(F32)

        delta_rows = jnp.concatenate(
            [dot(o.T, d_y1_low).reshape(seqs, o_rows, width), dot(act.T, g_low).reshape(seqs, d_rows, width)],
            axis=1,
        ).reshape(-1, width)
        delta_rows = rows_sum(delta_rows)
        delta_columns = jnp.concatenate([dot(h1.T, d_qkv), dot(h2.T, d_gu)], axis=1).astype(BF)
        delta_columns = lax.psum_scatter(delta_columns, "seq", scatter_dimension=0, tiled=True)
        own = delta_columns.shape[0] // ranks
        delta_columns = lax.all_to_all(
            delta_columns.reshape(ranks, own, -1), "ctx", split_axis=0, concat_axis=0, tiled=True
        )
        delta_columns = jnp.moveaxis(delta_columns, 0, 1).astype(F32)
        cuts = [my_q * size, (my_q + my_k) * size, (my_q + 2 * my_k) * size, attn_columns + units]
        parts = jnp.split(delta_columns, cuts, axis=2)
        delta_query = fold(parts[0], 0)
        delta_key = fold(parts[1], KEY_VALUE_HEADS)
        delta_value = fold(parts[2], KEY_VALUE_HEADS)
        delta_gate, delta_up = fold(parts[3], 0), fold(parts[4], 0)

        terms = lax.psum(jnp.concatenate([first_term, second_term, query_term, key_term]), axes)
        me = lax.axis_index("seq") * ranks + lax.axis_index("ctx")
        w = width

        def mine(start, n):
            return lax.dynamic_slice_in_dim(terms, start + me * n, n)

        return (
            layer_output[None],
            hidden_gradient[None],
            mine(0, n1),
            delta_query,
            delta_key,
            delta_value,
            mine(2 * w, n3),
            mine(2 * w + size, n4),
            delta_rows[:o_rows],
            mine(w, n2),
            delta_gate,
            delta_up,
            delta_rows[o_rows:],
        )

    return local


def solution(mesh):
    token = P("seq", "ctx", None)
    flat = P(("seq", "ctx"))
    rows = P(("seq", "ctx"), None)
    general = local_of(mesh)

    def body(*args):
        tokens, length = args[0].shape[1], args[1].shape[1]
        fits = (
            mesh.shape["ctx"] == KEY_VALUE_HEADS == 8
            and mesh.shape["seq"] == 4
            and length <= 1024
            and length % BLOCK == 0
            and tokens % RUN == 0
            and HEAD_DIMENSION % (mesh.shape["seq"] * mesh.shape["ctx"]) == 0
        )
        return fused_layer(mesh, args) if fits else general(*args)

    return jax.shard_map(
        body,
        mesh=mesh,
        in_specs=(token, P("seq", None), flat, rows, rows, rows, flat, flat, rows, flat, rows, rows, rows, token),
        out_specs=(token, token, flat, rows, rows, rows, flat, flat, rows, flat, rows, rows, rows),
        check_vma=False,
    )
```

```python
import types

import jax
import jax.numpy as jnp
import numpy as np
from jax import lax
from jax.experimental import pallas as pl
from jax.experimental.pallas import tpu as pltpu
from jax.sharding import PartitionSpec as P

QUERY_HEAD_COUNT = 16
KEY_VALUE_HEADS = 8
HEAD_DIMENSION = 128

EPS = 1e-06
THETA = 1000000.0
NEGATIVE = -1e30
BF = jnp.bfloat16
F32 = jnp.float32
MESH = pl.DeviceIdType.MESH
RUN = 64
BLOCK = 256


def nn(a, b):
    return jnp.dot(a, b, preferred_element_type=F32)


def nt(a, b):
    return lax.dot_general(a, b, (((1,), (1,)), ((), ())), preferred_element_type=F32)


def tn(a, b):
    return lax.dot_general(a, b, (((0,), (0,)), ((), ())), preferred_element_type=F32)


def loop(low, high, body):
    def step(i, carry):
        body(i)
        return carry

    lax.fori_loop(low, high, step, 0)


def rows_of(start, size):
    return pl.ds(pl.multiple_of(start, size), size)


def inverse_root(values):
    return lax.rsqrt(jnp.mean(values * values, axis=-1, keepdims=True) + EPS)


def norm_backward(normed_grad, normed, inverse):
    return inverse * (normed_grad - normed * jnp.mean(normed_grad * normed, axis=-1, keepdims=True))


def layer_kernel(dims, refs):
    S, C, T, L, D = dims.S, dims.C, dims.T, dims.L, dims.D
    H, RW, OR, DR, AC, U = dims.H, dims.RW, dims.OR, dims.DR, dims.AC, dims.U
    HD = HEAD_DIMENSION
    PR = C * RW
    NR = L // RUN
    NB = L // BLOCK
    CH = C // 2
    scale = HD ** (-0.5)
    r = refs
    s = lax.axis_index("seq")
    c = lax.axis_index("ctx")
    chip = lax.div(c, 2)
    core = lax.rem(c, 2)
    chip_y, chip_x = lax.div(chip, 2), lax.rem(chip, 2)
    sibling = chip * 2 + (1 - core)
    flat = s * C + c
    def partner(i):
        x = lax.rem(chip_x + lax.rem(i, 2), 2)
        y = lax.rem(chip_y + lax.div(i, 2), 2)
        return y * 2 + x

    def remote(src, dst, send, recv, **where):
        return pltpu.make_async_remote_copy(
            src_ref=src, dst_ref=dst, send_sem=send, recv_sem=recv, device_id=where, device_id_type=MESH
        )

    def local(src, dst, sem):
        return pltpu.make_async_copy(src, dst, sem)

    def arrived(dst, sem):
        pltpu.make_async_copy(dst, dst, sem).wait()

    barrier = pltpu.get_barrier_semaphore()

    def hello(**where):
        pl.semaphore_signal(barrier, inc=1, device_id=where, device_id_type=MESH)

    loop(1, C, lambda i: hello(ctx=lax.rem(c + i, C)))
    loop(1, S, lambda i: hello(seq=lax.rem(s + i, S)))

    pl.semaphore_wait(barrier, C - 1 + S - 1)

    def runs_of(b):
        return pl.ds(b * (BLOCK // RUN), BLOCK // RUN)

    def own_x():
        return r.x_all[pl.ds(c * (T // RUN), T // RUN)].reshape(T, D).astype(F32)

    X, G, H2, DY = 0, 1, 2, 3
    whole = {X: r.x_all, G: r.g_all, H2: r.h2_all, DY: r.dy_all}

    def block(kind, j):
        if kind == X:
            return whole[kind].at[pl.ds(j * (T // RUN), T // RUN)]
        return whole[kind].at[rows_of(j * T, T)]

    def half(ref, k):
        part = pl.ds(k * (D // 2), D // 2)
        return ref.at[:, :, part] if len(ref.shape) == 3 else ref.at[:, part]

    def gather_send(kind, src):
        for i in (1, 2):
            remote(src, block(kind, c), r.ag_send.at[kind, i], r.ag_recv.at[kind, c],
                   ctx=partner(i) * 2 + core).start()
        remote(src, block(kind, c), r.ag_send.at[kind, 0], r.ag_recv.at[kind, c], ctx=sibling).start()

    def gather_relay(kind, i):
        j = partner(i) * 2 + core
        arrived(block(kind, j), r.ag_recv.at[kind, j])

        @pl.when(i == 1)
        def _():
            part = half(block(kind, j), 0)
            remote(part, part, r.ag_send.at[kind, 3], r.ag_recv.at[kind, j], ctx=partner(2) * 2 + core).start()

        @pl.when(i == 2)
        def _():
            part = half(block(kind, j), 1)
            remote(part, part, r.ag_send.at[kind, 7], r.ag_recv.at[kind, j], ctx=partner(1) * 2 + core).start()

        remote(block(kind, j), block(kind, j), r.ag_send.at[kind, 3 + i], r.ag_recv.at[kind, j],
               ctx=sibling).start()

    def gather_other(kind, i):
        j = partner(i) * 2 + (1 - core)
        arrived(block(kind, j), r.ag_recv.at[kind, j])

    def gather_done(kind):
        for i in (0, 1, 2, 4, 5, 6):
            arrived(block(kind, c), r.ag_send.at[kind, i])
        for i in (3, 7):
            arrived(half(block(kind, c), 0), r.ag_send.at[kind, i])

    def scatter_pair(kind, i, partial):
        r.pair[i] = partial
        r.s1[i] = r.pair[i, rows_of((1 - core) * T, T), :].astype(BF)
        remote(r.s1.at[i], r.r1.at[1 if kind == 1 else 0, i], r.rs_send.at[kind, i],
               r.r1_recv.at[kind, i], ctx=sibling).start()

    def scatter_chip(kind, i):
        bank = 1 if kind == 1 else 0
        arrived(r.r1.at[bank, i], r.r1_recv.at[kind, i])
        mine = r.pair[i, rows_of(core * T, T), :] + r.r1[bank, i].astype(F32)
        r.s2[i] = mine.astype(BF)

        def to(k, slot, send, recv):
            remote(half(r.s2.at[i], k), half(r.r2.at[bank, slot], k), r.rs_send.at[kind, send],
                   r.r2_recv.at[kind, recv], ctx=partner(1 + k) * 2 + core).start()

        @pl.when(i == 1)
        def _():
            to(0, 0, CH, 0)

        @pl.when(i == 2)
        def _():
            to(1, 0, CH + 1, 1)

        @pl.when(i == 3)
        def _():
            to(0, 1, CH + 2, 2)
            to(1, 1, CH + 3, 3)

    def scatter(kind, partial):
        def go(k):
            i = jnp.where(k == 0, 3, jnp.where(k == 3, 0, k))
            scatter_pair(kind, i, partial(i))

            @pl.when(k > 0)
            def _():
                scatter_chip(kind, jnp.where(k == 1, 3, k - 1))

        loop(0, CH, go)

    def scatter_mid(kind):
        bank = 1 if kind == 1 else 0
        for k in (0, 1):
            i = 2 - k
            part = slice(k * (D // 2), (k + 1) * (D // 2))
            arrived(half(r.r2.at[bank, 1], k), r.r2_recv.at[kind, 2 + k])
            mine = r.pair[i, rows_of(core * T, T), part] + r.r1[bank, i, :, part].astype(F32)
            r.s3[:, part] = (mine + r.r2[bank, 1, :, part].astype(F32)).astype(BF)
            remote(half(r.s3, k), half(r.r2.at[bank, 2], k), r.rs_send.at[kind, CH + 4 + k],
                   r.r2_recv.at[kind, 4 + k], ctx=partner(i) * 2 + core).start()

    def scatter_sum(kind):
        bank = 1 if kind == 1 else 0
        arrived(r.r1.at[bank, 0], r.r1_recv.at[kind, 0])
        for k in (0, 1):
            arrived(half(r.r2.at[bank, 0], k), r.r2_recv.at[kind, k])
            arrived(half(r.r2.at[bank, 2], k), r.r2_recv.at[kind, 4 + k])
        total = r.pair[0, rows_of(core * T, T), :] + r.r1[bank, 0].astype(F32)
        return total + r.r2[bank, 0].astype(F32) + r.r2[bank, 2].astype(F32)

    def scatter_done(kind):
        loop(0, CH, lambda i: arrived(r.s1.at[0], r.rs_send.at[kind, i]))
        loop(CH, CH + 6, lambda i: arrived(half(r.s3, 0), r.rs_send.at[kind, i]))

    QKV, GATE, UP, OUT, DOWN, QKV2 = 0, 1, 2, 3, 4, 5
    PH = PR // 2

    def plane(w, b):
        if w == QKV:
            return r.w_qkv.at[rows_of(b * PR, PH)]
        if w == QKV2:
            return r.w_qkv.at[rows_of(b * PR + PH, PH)]
        if w == GATE:
            return r.w_gu.at[rows_of(b * PR, PR), pl.ds(0, U)]
        if w == UP:
            return r.w_gu.at[rows_of(b * PR, PR), pl.ds(U, U)]
        return (r.z_o if w == OUT else r.z_d).at[b]

    def weight_start(w, src=None):
        src = plane(w, s) if src is None else src

        @pl.when(s < S - 1)
        def _():
            remote(src, plane(w, s), r.z_send.at[w, 0, 0], r.z_recv.at[w, s], seq=s + 1).start()

        @pl.when(s > 0)
        def _():
            remote(src, plane(w, s), r.z_send.at[w, 1, 0], r.z_recv.at[w, s], seq=s - 1).start()

    rows_ref = {OUT: (0, r.w_o, OR), DOWN: (1, r.w_d, DR)}

    def deal(w, b, src=None):
        n, ref, size = rows_ref[w]
        src = plane(w, b) if src is None else src
        d = C * b + c
        rank, spot = lax.div(d, S), lax.rem(d, S)
        dst = ref.at[rows_of(spot * size, size)]

        @pl.when(rank != c)
        def _():
            remote(src, dst, r.m_send.at[n, b], r.m_recv.at[n], ctx=rank).start()

        @pl.when(rank == c)
        def _():
            local(src, dst, r.m_recv.at[n]).start()

    def deal_arrive(w):
        n, ref, size = rows_ref[w]
        arrived(ref, r.m_recv.at[n])

    def deal_done(w):
        n, ref, size = rows_ref[w]

        def go(b):
            @pl.when(lax.div(C * b + c, S) != c)
            def _():
                arrived(plane(w, 0), r.m_send.at[n, b])

        loop(0, S, go)

    def weight_hop(w, t):
        below, above = s - 1 - t, s + 1 + t

        @pl.when(below >= 0)
        def _():
            arrived(plane(w, below), r.z_recv.at[w, below])

            @pl.when(s < S - 1)
            def _():
                remote(plane(w, below), plane(w, below), r.z_send.at[w, 0, t + 1],
                       r.z_recv.at[w, below], seq=s + 1).start()

            if w in rows_ref:
                deal(w, below)

        @pl.when(above <= S - 1)
        def _():
            arrived(plane(w, above), r.z_recv.at[w, above])

            @pl.when(s > 0)
            def _():
                remote(plane(w, above), plane(w, above), r.z_send.at[w, 1, t + 1],
                       r.z_recv.at[w, above], seq=s - 1).start()

            if w in rows_ref:
                deal(w, above)

    def weight_done(w):
        for t in range(S - 1):
            @pl.when(jnp.logical_and(s - t >= 0, s < S - 1))
            def _():
                arrived(plane(w, s), r.z_send.at[w, 0, t])

            @pl.when(jnp.logical_and(s + t <= S - 1, s > 0))
            def _():
                arrived(plane(w, s), r.z_send.at[w, 1, t])

    GU = GATE
    sent = {QKV: (r.g_qkv, PR), OUT: (r.h_o, OR), GU: (r.g_gu, PR), DOWN: (r.h_d, DR)}
    got = {QKV: r.t_qkv, OUT: r.t_o, GU: r.t_gu, DOWN: r.t_d}
    halfway = {QKV: r.c_qkv, OUT: r.c_o, GU: r.c_gu, DOWN: r.c_d}
    summed = {QKV: r.u_qkv, OUT: r.u_o, GU: r.u_gu, DOWN: r.u_d}
    side = jnp.where(s >= 2, 1, 0)

    def grad_rows(w, p):
        ref, size = sent[w]
        return ref.at[rows_of(p * size, size)]

    def grad_order(i):
        return jnp.where(s < 2, lax.rem(3 - i + s, S), lax.rem(i + (3 - s) * 3, S))

    def grad_direct(w, p):
        remote(grad_rows(w, p), got[w].at[side], r.gz_send.at[w, p], r.gz_recv.at[w, side], seq=p).start()

    def grad_out(w, p):
        far_up = jnp.logical_and(s == 0, p >= 2)
        far_down = jnp.logical_and(s == S - 1, p <= 1)
        later = jnp.logical_or(
            jnp.logical_and(s == 1, p >= 2), jnp.logical_and(s == 2, p <= 1)
        )

        @pl.when(far_up)
        def _():
            remote(grad_rows(w, p), halfway[w].at[p - 2], r.gz_send.at[w, p], r.gc_recv.at[w, p - 2],
                   seq=1).start()

        @pl.when(far_down)
        def _():
            remote(grad_rows(w, p), halfway[w].at[p], r.gz_send.at[w, p], r.gc_recv.at[w, p], seq=2).start()

        others = jnp.logical_or(jnp.logical_or(far_up, far_down), jnp.logical_or(later, p == s))

        @pl.when(jnp.logical_not(others))
        def _():
            grad_direct(w, p)

    def grad_combine(w, k):
        @pl.when(jnp.logical_or(s == 1, s == 2))
        def _():
            p = jnp.where(s == 1, 3 - k, k)
            slot = jnp.where(s == 1, 1 - k, k)
            ref, size = sent[w]
            rows = rows_of(p * size, size)
            arrived(halfway[w].at[slot], r.gc_recv.at[w, slot])
            ref[rows, :] = (ref[rows, :].astype(F32) + halfway[w][slot].astype(F32)).astype(BF)
            grad_direct(w, p)

    def grad_sum(w):
        ref, size = sent[w]
        total = ref[rows_of(s * size, size), :].astype(F32)
        for i in range(2):
            arrived(got[w].at[i], r.gz_recv.at[w, i])
            total = total + got[w][i].astype(F32)
        summed[w][...] = total.astype(BF)

    def grad_done(w):
        loop(1, S, lambda i: arrived(got[w].at[0], r.gz_send.at[w, lax.rem(s + i, S)]))

    final = {QKV: r.f_qkv, GU: r.f_gu}

    def columns_send(n, w):
        def go(i):
            j = lax.rem(c + i, C)
            remote(summed[w].at[rows_of(j * RW, RW)], final[w].at[c], r.gp_send.at[n, i],
                   r.gp_recv.at[n, c], ctx=j).start()

        loop(1, C, go)
        final[w][c] = summed[w][rows_of(c * RW, RW), :]

    def columns_arrive(n, w):
        loop(1, C, lambda i: arrived(final[w].at[lax.rem(c + i, C)], r.gp_recv.at[n, lax.rem(c + i, C)]))

    def columns_done(n, w):
        loop(1, C, lambda i: arrived(final[w].at[0], r.gp_send.at[n, i]))

    undealt = {OUT: (0, r.g_o, r.h_o, OR), DOWN: (1, r.g_d, r.h_d, DR)}

    def undeal(w):
        n, src, dst, size = undealt[w]

        def go(j):
            d = S * c + j
            b, place = lax.div(d, C), lax.rem(d, C)
            here, there = src.at[rows_of(j * size, size)], dst.at[rows_of(b * size, size)]

            @pl.when(place != c)
            def _():
                remote(here, there, r.u_send.at[n, j], r.u_recv.at[n], ctx=place).start()

            @pl.when(place == c)
            def _():
                local(here, there, r.u_recv.at[n]).start()

        loop(0, S, go)

    def undeal_arrive(w):
        n, src, dst, size = undealt[w]
        arrived(dst, r.u_recv.at[n])

    def undeal_done(w):
        n, src, dst, size = undealt[w]

        def go(j):
            @pl.when(lax.rem(S * c + j, C) != c)
            def _():
                arrived(src.at[pl.ds(0, size)], r.u_send.at[n, j])

        loop(0, S, go)

    gains_own = r.gains_all.at[flat]
    gain_copy = local(r.gains_in, gains_own, r.gain_recv.at[s])
    gain_copy.start()

    def gain_go(i):
        remote(r.gains_in, gains_own, r.gain_send.at[i], r.gain_recv.at[s],
               ctx=lax.rem(c + i, C)).start()

    loop(1, C, gain_go)

    def qkv_piece(j):
        return (
            (r.wq_in.at[:, rows_of(j * H * HD, H * HD)], slice(0, H * HD)),
            (r.wk_in.at[:, rows_of(j * HD, HD)], slice(H * HD, (H + 1) * HD)),
            (r.wv_in.at[:, rows_of(j * HD, HD)], slice((H + 1) * HD, (H + 2) * HD)),
        )

    def gu_piece(j):
        return (
            (r.wg_in.at[:, rows_of(j * U, U)], slice(0, U)),
            (r.wu_in.at[:, rows_of(j * U, U)], slice(U, 2 * U)),
        )

    columns_of = {QKV: r.w_qkv, GU: r.w_gu}

    def spread(n, w, piece):
        ref = columns_of[w]
        own = rows_of(s * PR + c * RW, RW)

        def go(i):
            j = lax.rem(c + i, C)
            for src, columns in piece(j):
                remote(src, ref.at[own, columns], r.w_send.at[n], r.w_recv.at[n], ctx=j).start()

        loop(1, C, go)
        for src, columns in piece(c):
            local(src, ref.at[own, columns], r.w_recv.at[n]).start()

    def spread_arrive(n, w):
        arrived(columns_of[w].at[rows_of(s * PR, PR)], r.w_recv.at[n])

    def spread_done(n, w):
        arrived(columns_of[w].at[pl.ds(0, (C - 1) * RW)], r.w_send.at[n])

    weight_start(OUT, r.wo_in)
    spread(0, QKV, qkv_piece)
    local(r.x_in, block(X, c), r.local_sem.at[0]).start()
    local(r.table_in, r.table, r.local_sem.at[1]).start()
    gather_send(X, r.x_in)
    deal(OUT, s, r.wo_in)
    spread(1, GU, gu_piece)
    weight_hop(OUT, 0)
    spread_arrive(0, QKV)
    weight_start(QKV)
    weight_start(QKV2)
    arrived(r.gains_all.at[pl.ds(s * C, C)], r.gain_recv.at[s])

    def gain_far(i):
        mine = r.gains_all.at[pl.ds(s * C, C)]
        remote(mine, mine, r.gain_send.at[C + i], r.gain_recv.at[s], seq=lax.rem(s + i, S)).start()

    loop(1, S, gain_far)

    arrived(r.table, r.local_sem.at[1])

    def tables(b):
        rows = rows_of(b * T, T)
        both = r.table[rows, :]
        other = pltpu.roll(both, HD // 2, 1)
        first = lax.broadcasted_iota(jnp.int32, (T, HD), 1) < HD // 2
        r.cosine[rows, :] = jnp.where(first, both, other)
        r.sine[rows, :] = jnp.where(first, -other, both)

    loop(0, L // T, tables)
    arrived(block(X, c), r.local_sem.at[0])
    weight_hop(QKV, 0)
    gather_relay(X, 1)
    gather_relay(X, 2)
    weight_hop(QKV2, 0)
    gather_relay(X, 3)
    local(r.g_in, block(G, c), r.local_sem.at[2]).start()
    gather_send(G, r.g_in)

    def gain_block(i):
        p = lax.rem(s + i, S)
        arrived(r.gains_all.at[pl.ds(p * C, C)], r.gain_recv.at[p])

    loop(1, S, gain_block)
    gains = jnp.sum(r.gains_all[...], axis=1).astype(BF)

    def gain_vector(offset, count):
        width = count * S * C
        shift = count.bit_length() - 1
        column = lax.broadcasted_iota(jnp.int32, (HD, width), 1)
        row = lax.broadcasted_iota(jnp.int32, (HD, width), 0)
        pick = jnp.where(row == offset + (column & (count - 1)), 1.0, 0.0).astype(BF)
        spread_out = nn(gains, pick)
        owner = lax.broadcasted_iota(jnp.int32, (S * C, width), 0)
        place = lax.broadcasted_iota(jnp.int32, (S * C, width), 1) >> shift
        return jnp.sum(jnp.where(owner == place, spread_out, 0.0), axis=0, keepdims=True)

    n1 = D // (S * C)
    n3 = HD // (S * C)
    r.gain1[...] = gain_vector(0, n1)
    r.gain2[...] = gain_vector(n1, n1)
    r.gainq[...] = gain_vector(2 * n1, n3)
    r.gaink[...] = gain_vector(2 * n1 + n3, n3)

    arrived(block(X, sibling), r.ag_recv.at[X, sibling])
    loop(1, CH, lambda i: gather_other(X, i))

    def first_norm(k):
        x = r.x_all[r.order[1, k]].astype(F32)
        r.h1[rows_of(k * RUN, RUN), :] = (x * inverse_root(x) * r.gain1[...]).astype(BF)

    loop(0, NR, first_norm)
    weight_hop(QKV, 1)
    weight_hop(QKV2, 1)
    weight_hop(OUT, 1)
    weight_start(DOWN, r.wd_in)
    deal(DOWN, s, r.wd_in)
    spread_arrive(1, GU)
    weight_hop(QKV, 2)
    weight_hop(QKV2, 2)

    def rotate(u, rows):
        return u * r.cosine[rows, :] + pltpu.roll(u, HD // 2, 1) * r.sine[rows, :]

    def rotate_back(u, rows):
        return u * r.cosine[rows, :] - pltpu.roll(u, HD // 2, 1) * r.sine[rows, :]

    def project(b):
        rows = rows_of(b * BLOCK, BLOCK)
        acc = nn(r.h1[rows, :], r.w_qkv[...])
        for h in range(H):
            u = acc[:, h * HD : (h + 1) * HD]
            r.q_lin[h, rows, :] = u
            r.q_rot[h, rows, :] = rotate(u * inverse_root(u) * r.gainq[...], rows).astype(BF)
        u = acc[:, H * HD : (H + 1) * HD]
        r.k_lin[rows, :] = u
        k = rotate(u * inverse_root(u) * r.gaink[...], rows)
        r.k_rot[rows, :] = k.astype(BF)
        r.k_t[:, rows] = k.T.astype(BF)
        v = acc[:, (H + 1) * HD :]
        r.v[rows, :] = v.astype(BF)
        r.v_t[:, rows] = v.T.astype(BF)

    loop(0, NB, project)

    def attend(qb):
        @pl.when(qb == NB - 2)
        def _():
            gather_relay(G, 1)
            gather_relay(G, 2)
            weight_hop(OUT, 2)

        @pl.when(qb == NB - 1)
        def _():
            weight_hop(DOWN, 0)
            weight_start(GATE)

        cols = rows_of(qb * BLOCK, BLOCK)

        def keys(kb, carry):
            rows = rows_of(kb * BLOCK, BLOCK)
            key = r.k_rot[rows, :]
            value_t = r.v_t[:, rows]
            ahead = lax.broadcasted_iota(jnp.int32, (BLOCK, BLOCK), 0) - lax.broadcasted_iota(
                jnp.int32, (BLOCK, BLOCK), 1
            )
            allowed = ahead <= (qb - kb) * BLOCK
            out = []
            for h in range(H):
                acc, total = carry[2 * h], carry[2 * h + 1]
                e = jnp.exp(nt(key, r.q_rot[h, cols, :]) * scale)
                e = jnp.where(allowed, e, 0.0)
                low = e.astype(BF)
                r.e[h, rows, cols] = low
                out += [acc + nn(value_t, low), total + jnp.sum(e, axis=0, keepdims=True)]
            return tuple(out)

        zero = (jnp.zeros((HD, BLOCK), F32), jnp.zeros((1, BLOCK), F32)) * H
        done = lax.fori_loop(0, qb + 1, keys, zero)
        for h in range(H):
            inverse = 1.0 / done[2 * h + 1]
            o = done[2 * h] * inverse
            r.l_inv[h, :, cols] = jnp.broadcast_to(inverse, (8, BLOCK))
            r.o_t[h, :, cols] = o
            r.o_sorted[runs_of(qb), :, h * HD : (h + 1) * HD] = o.T.astype(BF).reshape(-1, RUN, HD)

    loop(0, NB, attend)
    def unsort(i):
        r.o[rows_of(i * RUN, RUN), :] = r.o_sorted[r.order[0, i]]

    loop(0, NR, unsort)

    gather_relay(G, 3)
    deal_arrive(OUT)
    scatter(0, lambda i: nn(r.o[rows_of(partner(i) * 2 * T, 2 * T), :], r.w_o[...]))
    weight_hop(DOWN, 1)
    weight_start(UP)
    weight_hop(GATE, 0)
    scatter_mid(0)
    weight_hop(DOWN, 2)
    y1 = own_x() + scatter_sum(0)
    scatter_done(0)
    r.y1[...] = y1
    h2_own = (y1 * inverse_root(y1) * r.gain2[...]).astype(BF)
    r.h2_all[rows_of(c * T, T), :] = h2_own
    gather_send(H2, block(H2, c))

    weight_hop(GATE, 1)
    arrived(block(G, c), r.local_sem.at[2])
    arrived(block(G, sibling), r.ag_recv.at[G, sibling])
    loop(1, CH, lambda i: gather_other(G, i))
    deal_arrive(DOWN)

    def act_grad(b):
        rows = rows_of(b * BLOCK, BLOCK)
        r.d_act[rows, :] = nt(r.g_all[rows, :], r.w_d[...])

    loop(0, NB, act_grad)
    weight_hop(UP, 0)
    gather_relay(H2, 1)
    gather_relay(H2, 2)
    weight_hop(GATE, 2)
    weight_hop(UP, 1)
    gather_relay(H2, 3)
    arrived(block(H2, sibling), r.ag_recv.at[H2, sibling])
    loop(1, CH, lambda i: gather_other(H2, i))

    def feed_gate(b):
        rows = rows_of(b * BLOCK, BLOCK)
        r.gate[rows, :] = nn(r.h2_all[rows, :], r.w_gu[:, :U])

    loop(0, NB, feed_gate)
    weight_hop(UP, 2)

    def feed(i):
        rows = rows_of(partner(i) * 2 * T, 2 * T)
        up = nn(r.h2_all[rows, :], r.w_gu[:, U:])
        gate = r.gate[rows, :]
        sig = 1.0 / (1.0 + jnp.exp(-gate))
        silu = gate * sig
        r.act[rows, :] = (silu * up).astype(BF)
        d_act = r.d_act[rows, :]
        r.d_gu[rows, :U] = (d_act * up * sig * (1.0 + gate * (1.0 - sig))).astype(BF)
        r.d_gu[rows, U:] = (d_act * silu).astype(BF)
        return nt(r.d_gu[rows, :], r.w_gu[...])

    scatter(2, feed)

    def gu_grad(i):
        p = grad_order(i)
        cols = rows_of(p * PR, PR)
        r.g_gu[cols, :] = tn(r.h2_all[:, cols], r.d_gu[...]).astype(BF)
        grad_out(GU, p)

    loop(0, S, gu_grad)
    scatter_mid(2)

    def down_grad(m):
        cols = rows_of(m * HD, HD)
        r.g_d[cols, :] = tn(r.act[:, cols], r.g_all[...]).astype(BF)

    loop(0, U // HD, down_grad)
    d_h2 = scatter_sum(2)
    scatter_done(2)
    y1 = r.y1[...]
    r2 = inverse_root(y1)
    normed = y1 * r2
    term2 = jnp.sum(d_h2 * normed, axis=0, keepdims=True)
    d_y1 = r.g_all[rows_of(c * T, T), :].astype(F32) + norm_backward(d_h2 * r.gain2[...], normed, r2)
    r.d_y1[...] = d_y1
    r.dy_all[rows_of(c * T, T), :] = d_y1.astype(BF)
    gather_send(DY, block(DY, c))
    WT = D // HD
    for k in range(WT):
        r.terms[WT + k : WT + k + 1, :] = term2[:, k * HD : (k + 1) * HD]

    arrived(block(DY, sibling), r.ag_recv.at[DY, sibling])

    def out_grad(i):
        @pl.when(i == 1)
        def _():
            gather_relay(DY, 1)
            gather_relay(DY, 2)

        @pl.when(i == 3)
        def _():
            gather_relay(DY, 3)

        @pl.when(i > 0)
        def _():
            gather_other(DY, i)

        rows = rows_of(partner(i) * 2 * T, 2 * T)
        d_o = nt(r.dy_all[rows, :], r.w_o[...]).astype(BF)
        r.d_o[pl.ds(partner(i) * (2 * T // RUN), 2 * T // RUN)] = d_o.reshape(-1, RUN, H * HD)

    loop(0, CH, out_grad)

    def out_weight(m):
        cols = rows_of(m * HD, HD)
        r.g_o[cols, :] = tn(r.o[:, cols], r.dy_all[...]).astype(BF)

    loop(0, H * HD // HD, out_weight)
    undeal(DOWN)
    undeal(OUT)
    grad_combine(GU, 0)

    def sort(k):
        r.d_o_sorted[rows_of(k * RUN, RUN), :] = r.d_o[r.order[1, k]]

    loop(0, NR, sort)
    r.d_k[...] = jnp.zeros_like(r.d_k)
    r.d_v[...] = jnp.zeros_like(r.d_v)
    r.sums[...] = jnp.zeros_like(r.sums)

    def attend_back(qb):
        @pl.when(qb == NB - 1)
        def _():
            undeal_arrive(DOWN)
            loop(0, S, lambda i: grad_out(DOWN, grad_order(i)))
            grad_combine(GU, 1)

        cols = rows_of(qb * BLOCK, BLOCK)
        d_o_t, d_o_low, row, factor = [], [], [], []
        for h in range(H):
            t = r.d_o_sorted[cols, h * HD : (h + 1) * HD].astype(F32).T
            inverse = r.l_inv[h, 0:1, cols]
            row.append(jnp.sum(t * r.o_t[h, :, cols], axis=0, keepdims=True))
            factor.append(inverse * scale)
            r.do_t[h] = t.astype(BF)
            r.do_l[h] = (t * inverse).T.astype(BF)

        def keys(kb, carry):
            rows = rows_of(kb * BLOCK, BLOCK)
            value = r.v[rows, :]
            key_t = r.k_t[:, rows]
            out = []
            d_k = r.d_k[rows, :]
            d_v = r.d_v[rows, :]
            for h in range(H):
                e = r.e[h, rows, cols]
                dp = nn(value, r.do_t[h])
                de = (e.astype(F32) * ((dp - row[h]) * factor[h])).astype(BF)
                out.append(carry[h] + nn(key_t, de))
                d_k = d_k + nn(de, r.q_rot[h, cols, :])
                d_v = d_v + nn(e, r.do_l[h])
            r.d_k[rows, :] = d_k
            r.d_v[rows, :] = d_v
            return tuple(out)

        done = lax.fori_loop(0, qb + 1, keys, (jnp.zeros((HD, BLOCK), F32),) * H)
        for h in range(H):
            d_g = rotate_back(done[h].T, cols)
            u = r.q_lin[h, cols, :]
            inverse = inverse_root(u)
            normed = u * inverse
            r.sums[0:1, :] += jnp.sum(d_g * normed, axis=0, keepdims=True)
            d_lin = norm_backward(d_g * r.gainq[...], normed, inverse).astype(BF)
            r.d_qkv[runs_of(qb), :, h * HD : (h + 1) * HD] = d_lin.reshape(-1, RUN, HD)

    loop(0, NB, attend_back)

    def key_back(b):
        rows = rows_of(b * BLOCK, BLOCK)
        d_g = rotate_back(r.d_k[rows, :], rows)
        u = r.k_lin[rows, :]
        inverse = inverse_root(u)
        normed = u * inverse
        r.sums[1:2, :] += jnp.sum(d_g * normed, axis=0, keepdims=True)
        d_lin = norm_backward(d_g * r.gaink[...], normed, inverse).astype(BF)
        r.d_qkv[runs_of(b), :, H * HD : (H + 1) * HD] = d_lin.reshape(-1, RUN, HD)
        r.d_qkv[runs_of(b), :, (H + 1) * HD :] = r.d_v[rows, :].astype(BF).reshape(-1, RUN, HD)

    loop(0, NB, key_back)
    undeal_arrive(OUT)
    loop(0, S, lambda i: grad_out(OUT, grad_order(i)))

    def qkv_grad(i):
        p = grad_order(i)
        cols = rows_of(p * PR, PR)
        r.g_qkv[cols, :] = tn(r.h1[:, cols], r.d_qkv[...].reshape(L, AC)).astype(BF)
        grad_out(QKV, p)

    loop(0, S, qkv_grad)

    def in_chip(i):
        j = partner(i) * 2
        parts = []
        for k in range(2 * T // RUN):
            parts.append(r.d_qkv[r.order[0, j * (T // RUN) + k]])
        return nt(jnp.concatenate(parts, axis=0), r.w_qkv[...])

    scatter(3, in_chip)
    grad_combine(DOWN, 0)
    scatter_mid(3)
    grad_sum(GU)
    columns_send(1, GU)
    grad_combine(DOWN, 1)
    d_h1 = scatter_sum(3)
    x = own_x()
    r1 = inverse_root(x)
    normed = x * r1
    term1 = jnp.sum(d_h1 * normed, axis=0, keepdims=True)
    r.x_grad[...] = r.d_y1[...] + norm_backward(d_h1 * r.gain1[...], normed, r1)
    local(r.x_grad, r.hidden_grad, r.out_sem.at[1]).start()
    for k in range(WT):
        r.terms[k : k + 1, :] = term1[:, k * HD : (k + 1) * HD]
    r.terms[2 * WT : 2 * WT + 8, :] = r.sums[...]

    def terms_far(i):
        remote(r.terms, r.terms_z.at[s], r.t_send.at[i], r.t_recv.at[s],
               seq=lax.rem(s + i, S)).start()

    loop(1, S, terms_far)
    scatter_done(3)
    grad_combine(OUT, 0)
    scatter(1, lambda i: nn(r.act[rows_of(partner(i) * 2 * T, 2 * T), :], r.w_d[...]))
    grad_combine(OUT, 1)
    scatter_mid(1)
    columns_arrive(1, GU)
    local(r.f_gu, r.gu_out, r.out_sem.at[3]).start()
    grad_sum(DOWN)
    local(r.u_d, r.down_out, r.out_sem.at[2]).start()
    grad_combine(QKV, 0)
    r.y_out[...] = (r.y1[...] + scatter_sum(1)).astype(BF)
    local(r.y_out, r.layer_out, r.out_sem.at[0]).start()
    grad_combine(QKV, 1)
    grad_sum(OUT)
    local(r.u_o, r.o_out, r.out_sem.at[4]).start()
    grad_sum(QKV)
    columns_send(0, QKV)
    total = r.terms[...]
    for i in range(1, S):
        p = lax.rem(s + i, S)
        arrived(r.terms_z.at[p], r.t_recv.at[p])
        total = total + r.terms_z[p]
    r.terms_sum[...] = total

    def terms_near(i):
        remote(r.terms_sum, r.terms_p.at[c], r.t_send.at[S + i], r.t_recv.at[S + c],
               ctx=lax.rem(c + i, C)).start()

    loop(1, C, terms_near)

    columns_arrive(0, QKV)
    local(r.f_qkv, r.qkv_out, r.out_sem.at[5]).start()
    total = r.terms_sum[...]
    for i in range(1, C):
        j = lax.rem(c + i, C)
        arrived(r.terms_p.at[j], r.t_recv.at[S + j])
        total = total + r.terms_p[j]
    r.terms_all[...] = total
    local(r.terms_all, r.terms_out, r.out_sem.at[6]).start()

    loop(1, C, lambda i: arrived(gains_own, r.gain_send.at[i]))
    loop(1, S, lambda i: arrived(r.gains_all.at[pl.ds(0, C)], r.gain_send.at[C + i]))
    for kind in (X, G, H2, DY):
        gather_done(kind)
    spread_done(0, QKV)
    spread_done(1, GU)
    deal_done(OUT)
    deal_done(DOWN)
    undeal_done(OUT)
    undeal_done(DOWN)
    for w in (QKV, QKV2, GATE, UP, OUT, DOWN):
        weight_done(w)
    for w in (QKV, OUT, GU, DOWN):
        grad_done(w)
    columns_done(0, QKV)
    columns_done(1, GU)
    scatter_done(1)
    loop(1, S, lambda i: arrived(r.terms, r.t_send.at[i]))
    loop(1, C, lambda i: arrived(r.terms, r.t_send.at[S + i]))
    pairs = (
        (r.y_out, r.layer_out), (r.x_grad, r.hidden_grad), (r.u_d, r.down_out), (r.f_gu, r.gu_out),
        (r.u_o, r.o_out), (r.f_qkv, r.qkv_out), (r.terms_all, r.terms_out),
    )
    for k, (src, dst) in enumerate(pairs):
        local(src, dst, r.out_sem.at[k]).wait()


def finish_kernel(dims, refs):
    S, C, D, H, U = dims.S, dims.C, dims.D, dims.H, dims.U
    HD = HEAD_DIMENSION
    r = refs
    me = lax.axis_index("seq") * C + lax.axis_index("ctx")
    r.layer_res[...] = r.layer_out[...]
    r.hidden_res[...] = r.hidden_grad[...]
    r.delta_down[...] = r.down_out[...].astype(F32)
    r.delta_out[...] = r.o_out[...].astype(F32)
    for j in range(C):
        r.delta_gate[:, j * U : (j + 1) * U] = r.gu_out[j, :, :U].astype(F32)
        r.delta_up[:, j * U : (j + 1) * U] = r.gu_out[j, :, U:].astype(F32)
        r.delta_query[:, j * H * HD : (j + 1) * H * HD] = r.qkv_out[j, :, : H * HD].astype(F32)
        r.delta_key[:, j * HD : (j + 1) * HD] = r.qkv_out[j, :, H * HD : (H + 1) * HD].astype(F32)
        r.delta_value[:, j * HD : (j + 1) * HD] = r.qkv_out[j, :, (H + 1) * HD :].astype(F32)

    def own(ref, first_row, count):
        start = me * count
        row = r.terms_out[pl.ds(first_row + lax.div(start, HD), 1), :]
        back = lax.rem(HD - lax.rem(start, HD), HD)
        ref[...] = pltpu.roll(jnp.broadcast_to(row, (8, HD)), back, 1)[0:1, :count]

    n1, n3 = D // (S * C), HD // (S * C)
    own(r.change1, 0, n1)
    own(r.change2, D // HD, n1)
    own(r.changeq, 2 * (D // HD), n3)
    own(r.changek, 2 * (D // HD) + 1, n3)


def fused_layer(mesh, args):
    (x, positions, gain1, wq, wk, wv, gainq, gaink, wo, gain2, wg, wu, wd, g) = args
    S, C = mesh.shape["seq"], mesh.shape["ctx"]
    T, D = x.shape[1:]
    L = positions.shape[1]
    HD = HEAD_DIMENSION
    H = QUERY_HEAD_COUNT // C
    RW, OR, DR = wq.shape[0], wo.shape[0], wd.shape[0]
    U = wg.shape[1] // C
    AC = (H + 2) * HD
    PR = C * RW
    CH = C // 2
    dims = types.SimpleNamespace(S=S, C=C, T=T, L=L, D=D, H=H, RW=RW, OR=OR, DR=DR, AC=AC, U=U)
    packed = jnp.concatenate([gain1, gain2, gainq, gaink]).astype(F32)
    packed = jnp.pad(packed[None, :], ((0, 7), (0, HD - packed.shape[0])))
    half = HD // 2
    frequency = np.power(THETA, -np.arange(half) * (2.0 / HD))
    phases = np.arange(L)[:, None] * frequency[None, :]
    table = jnp.asarray(np.concatenate([np.cos(phases), np.sin(phases)], axis=1), F32)
    TR = 2 * (D // HD) + 8
    run = positions[0, ::RUN] // RUN
    spot = jnp.arange(L // RUN, dtype=jnp.int32)
    place = jnp.sum(jnp.where(run[None, :] == spot[:, None], spot[None, :], 0), axis=1)
    order = jnp.stack([run, place]).astype(jnp.int32)
    inputs = dict(
        order=order, x_in=x.reshape(T // RUN, RUN, D), g_in=g[0], gains_in=packed, wq_in=wq, wk_in=wk, wv_in=wv, wo_in=wo,
        wg_in=wg, wu_in=wu, wd_in=wd, table_in=table,
    )
    TR_shape = ((TR, HD), F32)
    outputs = dict(
        layer_out=((T, D), BF), hidden_grad=((T, D), F32), qkv_out=((C, RW, AC), BF), o_out=((OR, D), BF),
        gu_out=((C, RW, 2 * U), BF), down_out=((DR, D), BF), terms_out=TR_shape,
    )
    n1, n3 = D // (S * C), HD // (S * C)
    final = dict(
        layer_res=((T, D), BF), hidden_res=((T, D), F32), change1=((1, n1), F32),
        delta_query=((RW, C * H * HD), F32), delta_key=((RW, C * HD), F32), delta_value=((RW, C * HD), F32),
        changeq=((1, n3), F32), changek=((1, n3), F32), delta_out=((OR, D), F32), change2=((1, n1), F32),
        delta_gate=((RW, C * U), F32), delta_up=((RW, C * U), F32), delta_down=((DR, D), F32),
    )
    V, DMA = pltpu.VMEM, pltpu.SemaphoreType.DMA
    scratch = dict(
        x_all=V((L // RUN, RUN, D), BF), g_all=V((L, D), BF), h2_all=V((L, D), BF), dy_all=V((L, D), BF),
        h1=V((L, D), BF), w_qkv=V((D, AC), BF), w_o=V((H * HD, D), BF), w_gu=V((D, 2 * U), BF),
        w_d=V((U, D), BF), gains_all=V((S * C, 8, HD), F32), table=V((L, HD), F32),
        cosine=V((L, HD), F32), sine=V((L, HD), F32), gain1=V((1, D), F32), gain2=V((1, D), F32),
        gainq=V((1, HD), F32), gaink=V((1, HD), F32), q_lin=V((H, L, HD), F32), k_lin=V((L, HD), F32),
        q_rot=V((H, L, HD), BF), k_rot=V((L, HD), BF), v=V((L, HD), BF), k_t=V((HD, L), BF),
        v_t=V((HD, L), BF), e=V((H, L, L), BF), l_inv=V((H, 8, L), F32), o_t=V((H, HD, L), F32),
        o_sorted=V((L // RUN, RUN, H * HD), BF), o=V((L, H * HD), BF), y1=V((T, D), F32), gate=V((L, U), F32), d_act=V((L, U), F32),
        act=V((L, U), BF), d_gu=V((L, 2 * U), BF), d_y1=V((T, D), F32), d_o=V((L // RUN, RUN, H * HD), BF),
        d_o_sorted=V((L, H * HD), BF), do_t=V((H, HD, BLOCK), BF), do_l=V((H, BLOCK, HD), BF),
        d_k=V((L, HD), F32), d_v=V((L, HD), F32), d_qkv=V((L // RUN, RUN, AC), BF), sums=V((8, HD), F32),
        pair=V((CH, 2 * T, D), F32), s1=V((CH, T, D), BF), r1=V((2, CH, T, D), BF),
        s2=V((CH, T, D), BF), r2=V((2, 3, T, D), BF), s3=V((T, D), BF),
        g_qkv=V((D, AC), BF), g_o=V((H * HD, D), BF), g_gu=V((D, 2 * U), BF), g_d=V((U, D), BF),
        t_qkv=V((2, PR, AC), BF), t_o=V((2, OR, D), BF), t_gu=V((2, PR, 2 * U), BF), t_d=V((2, DR, D), BF),
        c_qkv=V((2, PR, AC), BF), c_o=V((2, OR, D), BF), c_gu=V((2, PR, 2 * U), BF), c_d=V((2, DR, D), BF),
        z_o=V((S, OR, D), BF), z_d=V((S, DR, D), BF), y_out=V((T, D), BF), x_grad=V((T, D), F32), terms_all=V(*TR_shape),
        u_qkv=V((PR, AC), BF), u_o=V((OR, D), BF), u_gu=V((PR, 2 * U), BF), u_d=V((DR, D), BF),
        f_qkv=V((C, RW, AC), BF), h_o=V((S * OR, D), BF), f_gu=V((C, RW, 2 * U), BF), h_d=V((S * DR, D), BF),
        terms=V((TR, HD), F32), terms_z=V((S, TR, HD), F32), terms_sum=V((TR, HD), F32),
        terms_p=V((C, TR, HD), F32),
        ag_send=DMA((4, 2 * CH)), ag_recv=DMA((4, C)), rs_send=DMA((4, CH + 6)), r1_recv=DMA((4, CH)),
        r2_recv=DMA((4, 6)), z_send=DMA((6, 2, S)), z_recv=DMA((6, S)), gz_send=DMA((5, S)),
        gz_recv=DMA((5, 2)), gc_recv=DMA((5, 2)), gp_send=DMA((2, C)), gp_recv=DMA((2, C)), u_send=DMA((2, S)),
        u_recv=DMA((2,)), w_send=DMA((2,)), w_recv=DMA((2,)), m_send=DMA((2, S)), m_recv=DMA((2,)),
        gain_send=DMA((C + S,)), gain_recv=DMA((S,)), t_send=DMA((S + C,)), t_recv=DMA((S + C,)),
        local_sem=DMA((3,)), out_sem=DMA((7,)),
    )
    names = list(inputs) + list(outputs) + list(scratch)

    def kernel(*refs):
        layer_kernel(dims, types.SimpleNamespace(**dict(zip(names, refs))))

    in_specs = [
        pl.BlockSpec(memory_space=pltpu.SMEM if name == "order" else pl.ANY) for name in inputs
    ]
    results = pl.pallas_call(
        kernel,
        out_shape=[jax.ShapeDtypeStruct(*v) for v in outputs.values()],
        in_specs=in_specs,
        out_specs=[pl.BlockSpec(memory_space=pl.ANY)] * len(outputs),
        scratch_shapes=list(scratch.values()),
        compiler_params=pltpu.CompilerParams(
            collective_id=0, has_side_effects=True, vmem_limit_bytes=67043328
        ),
        name="layer",
    )(*inputs.values())
    finish_names = list(outputs) + list(final)

    def finish(*refs):
        finish_kernel(dims, types.SimpleNamespace(**dict(zip(finish_names, refs))))

    out = pl.pallas_call(
        finish,
        out_shape=[jax.ShapeDtypeStruct(*v) for v in final.values()],
        in_specs=[pl.BlockSpec(memory_space=pltpu.VMEM)] * len(outputs),
        out_specs=[pl.BlockSpec(memory_space=pltpu.VMEM)] * len(final),
        name="finish",
    )(*results)
    one_axis = [k for k, v in enumerate(final.values()) if v[0][0] == 1]
    out = [o.reshape(-1) if k in one_axis else o for k, o in enumerate(out)]
    return (out[0][None], out[1][None], *out[2:])


def angles(places, head_size):
    half_size = head_size // 2
    frequency = jnp.power(THETA, -jnp.arange(half_size, dtype=F32) * (2.0 / head_size))
    phases = places.astype(F32)[:, None] * frequency[None, :]
    phases = jnp.concatenate([phases, phases], axis=-1)
    return (jnp.cos(phases), jnp.sin(phases))


def rotate(values, cosines, sines):
    half_size = values.shape[-1] // 2
    turned = jnp.concatenate([-values[..., half_size:], values[..., :half_size]], axis=-1)
    return values * cosines + turned * sines


def rotate_back(upstream, cosines, sines):
    half_size = upstream.shape[-1] // 2
    scaled = upstream * sines
    turned = jnp.concatenate([scaled[..., half_size:], -scaled[..., :half_size]], axis=-1)
    return upstream * cosines + turned


def dot(a, b):
    return jnp.dot(a, b, preferred_element_type=F32)


def local_of(mesh):
    seqs, ranks = mesh.shape["seq"], mesh.shape["ctx"]
    devices = seqs * ranks
    axes = ("seq", "ctx")

    def spread(shard, heads):
        rows, columns = shard.shape
        if heads and heads < ranks:
            blocks = shard.reshape(rows, heads, 1, columns // heads)
            blocks = jnp.broadcast_to(blocks, (rows, heads, ranks // heads, columns // heads))
            return blocks.reshape(rows, ranks, columns // heads)
        return shard.reshape(rows, ranks, columns // ranks)

    def fold(blocks, heads):
        rows, count, width = blocks.shape
        if heads and heads < ranks:
            return blocks.reshape(rows, heads, count // heads, width).sum(2).reshape(rows, heads * width)
        return blocks.reshape(rows, count * width)

    forth = [(seqs * r + j, j * ranks + r) for r in range(ranks) for j in range(seqs)]
    back = [(b, a) for a, b in forth]

    def local(
        hidden_states, positions, gain_first, weight_query, key_weight_matrix, value_weight_matrix,
        gain_query, gain_key, weight_output, gain_second, weight_gate, weight_up, weight_down,
        output_cotangent,
    ):
        tokens = hidden_states.shape[1]
        length = positions.shape[1]
        size = HEAD_DIMENSION
        group = QUERY_HEAD_COUNT // KEY_VALUE_HEADS
        my_q = QUERY_HEAD_COUNT // ranks
        my_k = max(1, KEY_VALUE_HEADS // ranks)
        scale = size ** (-0.5)
        places = positions[0]
        cosines, sines = angles(places, size)
        cosines, sines = cosines[:, None, :], sines[:, None, :]

        gains = jnp.concatenate([gain_first, gain_second, gain_query, gain_key])
        gains = lax.all_gather(gains, axes, axis=0).astype(F32)
        n1, n2, n3, n4 = (g.shape[0] for g in (gain_first, gain_second, gain_query, gain_key))
        first_scale = gains[:, :n1].reshape(-1)
        second_scale = gains[:, n1 : n1 + n2].reshape(-1)
        query_scale = gains[:, n1 + n2 : n1 + n2 + n3].reshape(-1)
        key_scale = gains[:, n1 + n2 + n3 :].reshape(-1)

        column_weights = jnp.concatenate(
            [
                spread(weight_query, 0),
                spread(key_weight_matrix, KEY_VALUE_HEADS),
                spread(value_weight_matrix, KEY_VALUE_HEADS),
                spread(weight_gate, 0),
                spread(weight_up, 0),
            ],
            axis=2,
        )
        column_weights = lax.all_to_all(column_weights, "ctx", split_axis=1, concat_axis=0, tiled=True)
        column_weights = lax.all_gather(column_weights[:, 0], "seq", axis=0, tiled=True)
        row_weights = jnp.concatenate([weight_output, weight_down], axis=0)
        row_weights = lax.all_gather(lax.ppermute(row_weights, axes, forth), "seq", axis=0)
        o_rows, d_rows = weight_output.shape[0], weight_down.shape[0]
        width = weight_output.shape[1]
        w_o = row_weights[:, :o_rows].reshape(-1, width)
        w_d = row_weights[:, o_rows:].reshape(-1, width)
        units = w_d.shape[0]
        attn_columns = (my_q + 2 * my_k) * size
        w_qkv = column_weights[:, :attn_columns]
        w_gu = column_weights[:, attn_columns:]

        x = lax.all_gather(hidden_states[0], "ctx", axis=0, tiled=True).astype(F32)
        g_low = lax.all_gather(output_cotangent[0], "ctx", axis=0, tiled=True)
        first_inverse = inverse_root(x)
        h1 = (x * first_inverse * first_scale).astype(BF)
        qkv = dot(h1, w_qkv)
        q_lin = qkv[:, : my_q * size].reshape(length, my_q, size)
        k_lin = qkv[:, my_q * size : (my_q + my_k) * size].reshape(length, my_k, size)
        v = qkv[:, (my_q + my_k) * size :].astype(BF).reshape(length, my_k, size)
        rq, rk = inverse_root(q_lin), inverse_root(k_lin)
        nq, nk = q_lin * rq, k_lin * rk
        qr = rotate(nq * query_scale, cosines, sines).astype(BF)
        kr = rotate(nk * key_scale, cosines, sines).astype(BF)
        mask = places[None, :] <= places[:, None]

        def scores(h):
            e = lax.dot_general(
                qr[:, h], kr[:, h // group], (((1,), (1,)), ((), ())), preferred_element_type=F32
            )
            return jnp.where(mask, e * scale, NEGATIVE)

        outs, probs = [], []
        for h in range(my_q):
            e = scores(h)
            p = jnp.exp(e - jnp.max(e, axis=-1, keepdims=True))
            p = p / jnp.sum(p, axis=-1, keepdims=True)
            probs.append(p)
            outs.append(dot(p.astype(BF), v[:, h // group]))
        o = jnp.concatenate(outs, axis=1).astype(BF)

        def scatter(part):
            return lax.psum_scatter(part.astype(BF), "ctx", scatter_dimension=0, tiled=True).astype(F32)

        x_own = hidden_states[0].astype(F32)
        y1 = x_own + scatter(dot(o, w_o))
        r2 = inverse_root(y1)
        second_normed = y1 * r2
        h2 = lax.all_gather((second_normed * second_scale).astype(BF), "ctx", axis=0, tiled=True)
        gu = dot(h2, w_gu)
        gate, up = gu[:, :units], gu[:, units:]
        sig = jax.nn.sigmoid(gate)
        silu = gate * sig
        act = (silu * up).astype(BF)
        layer_output = (y1 + scatter(dot(act, w_d))).astype(BF)

        d_act = dot(g_low, w_d.T)
        d_gate = (d_act * up * sig * (1.0 + gate * (1.0 - sig))).astype(BF)
        d_up = (d_act * silu).astype(BF)
        d_gu = jnp.concatenate([d_gate, d_up], axis=1)
        d_h2 = scatter(dot(d_gu, w_gu.T))
        second_term = jnp.sum(d_h2 * second_normed, axis=0)
        d_y1 = output_cotangent[0].astype(F32) + norm_backward(d_h2 * second_scale, second_normed, r2)
        d_y1_low = lax.all_gather(d_y1.astype(BF), "ctx", axis=0, tiled=True)
        d_o = dot(d_y1_low, w_o.T).astype(BF).reshape(length, my_q, size)

        d_q, d_k, d_v = [], [0.0] * my_k, [0.0] * my_k
        for h in range(my_q):
            p = probs[h]
            dp = lax.dot_general(
                d_o[:, h], v[:, h // group], (((1,), (1,)), ((), ())), preferred_element_type=F32
            )
            row = jnp.sum(p * dp, axis=-1, keepdims=True)
            de = (p * (dp - row) * scale).astype(BF)
            d_q.append(dot(de, kr[:, h // group]))
            d_k[h // group] += dot(de.T, qr[:, h])
            d_v[h // group] += dot(p.astype(BF).T, d_o[:, h])
        d_q, d_k, d_v = jnp.stack(d_q, 1), jnp.stack(d_k, 1), jnp.stack(d_v, 1)
        d_gq, d_gk = rotate_back(d_q, cosines, sines), rotate_back(d_k, cosines, sines)
        query_term = jnp.sum(d_gq * nq, axis=(0, 1))
        key_term = jnp.sum(d_gk * nk, axis=(0, 1))
        d_qlin = norm_backward(d_gq * query_scale, nq, rq).reshape(length, -1)
        d_klin = norm_backward(d_gk * key_scale, nk, rk).reshape(length, -1)
        d_qkv = jnp.concatenate([d_qlin, d_klin, d_v.reshape(length, -1)], axis=1).astype(BF)
        d_h1 = scatter(dot(d_qkv, w_qkv.T))
        r1 = inverse_root(x_own)
        first_normed = x_own * r1
        first_term = jnp.sum(d_h1 * first_normed, axis=0)
        hidden_gradient = d_y1 + norm_backward(d_h1 * first_scale, first_normed, r1)

        def rows_sum(part):
            part = lax.psum_scatter(part.astype(BF), "seq", scatter_dimension=0, tiled=True)
            return lax.ppermute(part, axes, back).astype(F32)

        delta_rows = jnp.concatenate(
            [dot(o.T, d_y1_low).reshape(seqs, o_rows, width), dot(act.T, g_low).reshape(seqs, d_rows, width)],
            axis=1,
        ).reshape(-1, width)
        delta_rows = rows_sum(delta_rows)
        delta_columns = jnp.concatenate([dot(h1.T, d_qkv), dot(h2.T, d_gu)], axis=1).astype(BF)
        delta_columns = lax.psum_scatter(delta_columns, "seq", scatter_dimension=0, tiled=True)
        own = delta_columns.shape[0] // ranks
        delta_columns = lax.all_to_all(
            delta_columns.reshape(ranks, own, -1), "ctx", split_axis=0, concat_axis=0, tiled=True
        )
        delta_columns = jnp.moveaxis(delta_columns, 0, 1).astype(F32)
        cuts = [my_q * size, (my_q + my_k) * size, (my_q + 2 * my_k) * size, attn_columns + units]
        parts = jnp.split(delta_columns, cuts, axis=2)
        delta_query = fold(parts[0], 0)
        delta_key = fold(parts[1], KEY_VALUE_HEADS)
        delta_value = fold(parts[2], KEY_VALUE_HEADS)
        delta_gate, delta_up = fold(parts[3], 0), fold(parts[4], 0)

        terms = lax.psum(jnp.concatenate([first_term, second_term, query_term, key_term]), axes)
        me = lax.axis_index("seq") * ranks + lax.axis_index("ctx")
        w = width

        def mine(start, n):
            return lax.dynamic_slice_in_dim(terms, start + me * n, n)

        return (
            layer_output[None],
            hidden_gradient[None],
            mine(0, n1),
            delta_query,
            delta_key,
            delta_value,
            mine(2 * w, n3),
            mine(2 * w + size, n4),
            delta_rows[:o_rows],
            mine(w, n2),
            delta_gate,
            delta_up,
            delta_rows[o_rows:],
        )

    return local


def solution(mesh):
    token = P("seq", "ctx", None)
    flat = P(("seq", "ctx"))
    rows = P(("seq", "ctx"), None)
    general = local_of(mesh)

    def body(*args):
        tokens, length = args[0].shape[1], args[1].shape[1]
        fits = (
            mesh.shape["ctx"] == KEY_VALUE_HEADS == 8
            and mesh.shape["seq"] == 4
            and length <= 1024
            and length % BLOCK == 0
            and tokens % RUN == 0
            and HEAD_DIMENSION % (mesh.shape["seq"] * mesh.shape["ctx"]) == 0
        )
        return fused_layer(mesh, args) if fits else general(*args)

    return jax.shard_map(
        body,
        mesh=mesh,
        in_specs=(token, P("seq", None), flat, rows, rows, rows, flat, flat, rows, flat, rows, rows, rows, token),
        out_specs=(token, token, flat, rows, rows, rows, flat, flat, rows, flat, rows, rows, rows),
        check_vma=False,
    )
```

```python
import types

import jax
import jax.numpy as jnp
import numpy as np
from jax import lax
from jax.experimental import pallas as pl
from jax.experimental.pallas import tpu as pltpu
from jax.sharding import PartitionSpec as P

QUERY_HEAD_COUNT = 16
KEY_VALUE_HEADS = 8
HEAD_DIMENSION = 128

EPS = 1e-06
THETA = 1000000.0
NEGATIVE = -1e30
BF = jnp.bfloat16
F32 = jnp.float32
MESH = pl.DeviceIdType.MESH
RUN = 64
BLOCK = 256


def nn(a, b):
    return jnp.dot(a, b, preferred_element_type=F32)


def nt(a, b):
    return lax.dot_general(a, b, (((1,), (1,)), ((), ())), preferred_element_type=F32)


def tn(a, b):
    return lax.dot_general(a, b, (((0,), (0,)), ((), ())), preferred_element_type=F32)


def loop(low, high, body):
    def step(i, carry):
        body(i)
        return carry

    lax.fori_loop(low, high, step, 0)


def rows_of(start, size):
    return pl.ds(pl.multiple_of(start, size), size)


def inverse_root(values):
    return lax.rsqrt(jnp.mean(values * values, axis=-1, keepdims=True) + EPS)


def norm_backward(normed_grad, normed, inverse):
    return inverse * (normed_grad - normed * jnp.mean(normed_grad * normed, axis=-1, keepdims=True))


def layer_kernel(dims, refs):
    S, C, T, L, D = dims.S, dims.C, dims.T, dims.L, dims.D
    H, RW, OR, DR, AC, U = dims.H, dims.RW, dims.OR, dims.DR, dims.AC, dims.U
    HD = HEAD_DIMENSION
    PR = C * RW
    NR = L // RUN
    NB = L // BLOCK
    CH = C // 2
    scale = HD ** (-0.5)
    r = refs
    s = lax.axis_index("seq")
    c = lax.axis_index("ctx")
    chip = lax.div(c, 2)
    core = lax.rem(c, 2)
    chip_y, chip_x = lax.div(chip, 2), lax.rem(chip, 2)
    sibling = chip * 2 + (1 - core)
    flat = s * C + c
    def partner(i):
        x = lax.rem(chip_x + lax.rem(i, 2), 2)
        y = lax.rem(chip_y + lax.div(i, 2), 2)
        return y * 2 + x

    def remote(src, dst, send, recv, **where):
        return pltpu.make_async_remote_copy(
            src_ref=src, dst_ref=dst, send_sem=send, recv_sem=recv, device_id=where, device_id_type=MESH
        )

    def local(src, dst, sem):
        return pltpu.make_async_copy(src, dst, sem)

    def arrived(dst, sem):
        pltpu.make_async_copy(dst, dst, sem).wait()

    barrier = pltpu.get_barrier_semaphore()

    def hello(**where):
        pl.semaphore_signal(barrier, inc=1, device_id=where, device_id_type=MESH)

    loop(1, C, lambda i: hello(ctx=lax.rem(c + i, C)))
    loop(1, S, lambda i: hello(seq=lax.rem(s + i, S)))

    pl.semaphore_wait(barrier, C - 1 + S - 1)

    def runs_of(b):
        return pl.ds(b * (BLOCK // RUN), BLOCK // RUN)

    def own_x():
        return r.x_all[pl.ds(c * (T // RUN), T // RUN)].reshape(T, D).astype(F32)

    X, G, H2, DY = 0, 1, 2, 3
    whole = {X: r.x_all, G: r.g_all, H2: r.h2_all, DY: r.dy_all}

    def block(kind, j):
        if kind == X:
            return whole[kind].at[pl.ds(j * (T // RUN), T // RUN)]
        return whole[kind].at[rows_of(j * T, T)]

    def half(ref, k):
        part = pl.ds(k * (D // 2), D // 2)
        return ref.at[:, :, part] if len(ref.shape) == 3 else ref.at[:, part]

    def gather_send(kind, src):
        for i in (1, 2):
            remote(src, block(kind, c), r.ag_send.at[kind, i], r.ag_recv.at[kind, c],
                   ctx=partner(i) * 2 + core).start()
        remote(src, block(kind, c), r.ag_send.at[kind, 0], r.ag_recv.at[kind, c], ctx=sibling).start()

    def gather_relay(kind, i):
        j = partner(i) * 2 + core
        arrived(block(kind, j), r.ag_recv.at[kind, j])

        @pl.when(i == 1)
        def _():
            part = half(block(kind, j), 0)
            remote(part, part, r.ag_send.at[kind, 3], r.ag_recv.at[kind, j], ctx=partner(2) * 2 + core).start()

        @pl.when(i == 2)
        def _():
            part = half(block(kind, j), 1)
            remote(part, part, r.ag_send.at[kind, 7], r.ag_recv.at[kind, j], ctx=partner(1) * 2 + core).start()

        remote(block(kind, j), block(kind, j), r.ag_send.at[kind, 3 + i], r.ag_recv.at[kind, j],
               ctx=sibling).start()

    def gather_other(kind, i):
        j = partner(i) * 2 + (1 - core)
        arrived(block(kind, j), r.ag_recv.at[kind, j])

    def gather_done(kind):
        for i in (0, 1, 2, 4, 5, 6):
            arrived(block(kind, c), r.ag_send.at[kind, i])
        for i in (3, 7):
            arrived(half(block(kind, c), 0), r.ag_send.at[kind, i])

    def scatter_pair(kind, i, partial):
        r.pair[i] = partial
        r.s1[i] = r.pair[i, rows_of((1 - core) * T, T), :].astype(BF)
        remote(r.s1.at[i], r.r1.at[1 if kind == 1 else 0, i], r.rs_send.at[kind, i],
               r.r1_recv.at[kind, i], ctx=sibling).start()

    def scatter_chip(kind, i):
        bank = 1 if kind == 1 else 0
        arrived(r.r1.at[bank, i], r.r1_recv.at[kind, i])
        mine = r.pair[i, rows_of(core * T, T), :] + r.r1[bank, i].astype(F32)
        r.s2[i] = mine.astype(BF)

        def to(k, slot, send, recv):
            remote(half(r.s2.at[i], k), half(r.r2.at[bank, slot], k), r.rs_send.at[kind, send],
                   r.r2_recv.at[kind, recv], ctx=partner(1 + k) * 2 + core).start()

        @pl.when(i == 1)
        def _():
            to(0, 0, CH, 0)

        @pl.when(i == 2)
        def _():
            to(1, 0, CH + 1, 1)

        @pl.when(i == 3)
        def _():
            to(0, 1, CH + 2, 2)
            to(1, 1, CH + 3, 3)

    def scatter(kind, partial):
        def go(k):
            i = jnp.where(k == 0, 3, jnp.where(k == 3, 0, k))
            scatter_pair(kind, i, partial(i))

            @pl.when(k > 0)
            def _():
                scatter_chip(kind, jnp.where(k == 1, 3, k - 1))

        loop(0, CH, go)

    def scatter_pairs(kind, partial):
        loop(0, CH, lambda i: scatter_pair(kind, i, partial(i)))

    def scatter_mid(kind):
        bank = 1 if kind == 1 else 0
        for k in (0, 1):
            i = 2 - k
            part = slice(k * (D // 2), (k + 1) * (D // 2))
            arrived(half(r.r2.at[bank, 1], k), r.r2_recv.at[kind, 2 + k])
            mine = r.pair[i, rows_of(core * T, T), part] + r.r1[bank, i, :, part].astype(F32)
            r.s3[:, part] = (mine + r.r2[bank, 1, :, part].astype(F32)).astype(BF)
            remote(half(r.s3, k), half(r.r2.at[bank, 2], k), r.rs_send.at[kind, CH + 4 + k],
                   r.r2_recv.at[kind, 4 + k], ctx=partner(i) * 2 + core).start()

    def scatter_sum(kind):
        bank = 1 if kind == 1 else 0
        arrived(r.r1.at[bank, 0], r.r1_recv.at[kind, 0])
        for k in (0, 1):
            arrived(half(r.r2.at[bank, 0], k), r.r2_recv.at[kind, k])
            arrived(half(r.r2.at[bank, 2], k), r.r2_recv.at[kind, 4 + k])
        total = r.pair[0, rows_of(core * T, T), :] + r.r1[bank, 0].astype(F32)
        return total + r.r2[bank, 0].astype(F32) + r.r2[bank, 2].astype(F32)

    def scatter_done(kind):
        loop(0, CH, lambda i: arrived(r.s1.at[0], r.rs_send.at[kind, i]))
        loop(CH, CH + 6, lambda i: arrived(half(r.s3, 0), r.rs_send.at[kind, i]))

    QKV, GATE, UP, OUT, DOWN, QKV2 = 0, 1, 2, 3, 4, 5
    PH = PR // 2

    def plane(w, b):
        if w == QKV:
            return r.w_qkv.at[rows_of(b * PR, PH)]
        if w == QKV2:
            return r.w_qkv.at[rows_of(b * PR + PH, PH)]
        if w == GATE:
            return r.w_gu.at[rows_of(b * PR, PR), pl.ds(0, U)]
        if w == UP:
            return r.w_gu.at[rows_of(b * PR, PR), pl.ds(U, U)]
        if w == DOWN:
            return r.w_d.at[rows_of(b * DR, DR)]
        return r.z_o.at[b]

    def weight_start(w, src=None):
        src = plane(w, s) if src is None else src

        @pl.when(s < S - 1)
        def _():
            remote(src, plane(w, s), r.z_send.at[w, 0, 0], r.z_recv.at[w, s], seq=s + 1).start()

        @pl.when(s > 0)
        def _():
            remote(src, plane(w, s), r.z_send.at[w, 1, 0], r.z_recv.at[w, s], seq=s - 1).start()

    rows_ref = {OUT: (0, r.w_o, OR)}

    def deal(w, b, src=None):
        n, ref, size = rows_ref[w]
        src = plane(w, b) if src is None else src
        d = C * b + c
        rank, spot = lax.div(d, S), lax.rem(d, S)
        dst = ref.at[rows_of(spot * size, size)]

        @pl.when(rank != c)
        def _():
            remote(src, dst, r.m_send.at[n, b], r.m_recv.at[n], ctx=rank).start()

        @pl.when(rank == c)
        def _():
            local(src, dst, r.m_recv.at[n]).start()

    def deal_arrive(w):
        n, ref, size = rows_ref[w]
        arrived(ref, r.m_recv.at[n])

    def deal_done(w):
        n, ref, size = rows_ref[w]

        def go(b):
            @pl.when(lax.div(C * b + c, S) != c)
            def _():
                arrived(plane(w, 0), r.m_send.at[n, b])

        loop(0, S, go)

    def weight_hop(w, t):
        below, above = s - 1 - t, s + 1 + t

        @pl.when(below >= 0)
        def _():
            arrived(plane(w, below), r.z_recv.at[w, below])

            @pl.when(s < S - 1)
            def _():
                remote(plane(w, below), plane(w, below), r.z_send.at[w, 0, t + 1],
                       r.z_recv.at[w, below], seq=s + 1).start()

        @pl.when(above <= S - 1)
        def _():
            arrived(plane(w, above), r.z_recv.at[w, above])

            @pl.when(s > 0)
            def _():
                remote(plane(w, above), plane(w, above), r.z_send.at[w, 1, t + 1],
                       r.z_recv.at[w, above], seq=s - 1).start()

    def deal_hop(w, t):
        below, above = s - 1 - t, s + 1 + t

        @pl.when(below >= 0)
        def _():
            deal(w, below)

        @pl.when(above <= S - 1)
        def _():
            deal(w, above)

    def weight_done(w):
        for t in range(S - 1):
            @pl.when(jnp.logical_and(s - t >= 0, s < S - 1))
            def _():
                arrived(plane(w, s), r.z_send.at[w, 0, t])

            @pl.when(jnp.logical_and(s + t <= S - 1, s > 0))
            def _():
                arrived(plane(w, s), r.z_send.at[w, 1, t])

    GU = GATE
    sent = {QKV: (r.g_qkv, PR), OUT: (r.h_o, OR), GU: (r.g_gu, PR), DOWN: (r.g_d, DR)}
    got = {QKV: r.t_qkv, OUT: r.t_o, GU: r.t_gu, DOWN: r.t_d}
    halfway = {QKV: r.c_qkv, OUT: r.c_o, GU: r.c_gu, DOWN: r.c_d}
    summed = {QKV: r.u_qkv, OUT: r.u_o, GU: r.u_gu, DOWN: r.u_d}
    side = jnp.where(s >= 2, 1, 0)

    def grad_rows(w, p):
        ref, size = sent[w]
        return ref.at[rows_of(p * size, size)]

    def grad_order(i):
        return jnp.where(s < 2, lax.rem(3 - i + s, S), lax.rem(i + (3 - s) * 3, S))

    def grad_direct(w, p):
        remote(grad_rows(w, p), got[w].at[side], r.gz_send.at[w, p], r.gz_recv.at[w, side], seq=p).start()

    def grad_out(w, p):
        far_up = jnp.logical_and(s == 0, p >= 2)
        far_down = jnp.logical_and(s == S - 1, p <= 1)
        later = jnp.logical_or(
            jnp.logical_and(s == 1, p >= 2), jnp.logical_and(s == 2, p <= 1)
        )

        @pl.when(far_up)
        def _():
            remote(grad_rows(w, p), halfway[w].at[p - 2], r.gz_send.at[w, p], r.gc_recv.at[w, p - 2],
                   seq=1).start()

        @pl.when(far_down)
        def _():
            remote(grad_rows(w, p), halfway[w].at[p], r.gz_send.at[w, p], r.gc_recv.at[w, p], seq=2).start()

        others = jnp.logical_or(jnp.logical_or(far_up, far_down), jnp.logical_or(later, p == s))

        @pl.when(jnp.logical_not(others))
        def _():
            grad_direct(w, p)

    def grad_combine(w, k):
        @pl.when(jnp.logical_or(s == 1, s == 2))
        def _():
            p = jnp.where(s == 1, 3 - k, k)
            slot = jnp.where(s == 1, 1 - k, k)
            ref, size = sent[w]
            rows = rows_of(p * size, size)
            arrived(halfway[w].at[slot], r.gc_recv.at[w, slot])
            ref[rows, :] = (ref[rows, :].astype(F32) + halfway[w][slot].astype(F32)).astype(BF)
            grad_direct(w, p)

    def grad_sum(w):
        ref, size = sent[w]
        total = ref[rows_of(s * size, size), :].astype(F32)
        for i in range(2):
            arrived(got[w].at[i], r.gz_recv.at[w, i])
            total = total + got[w][i].astype(F32)
        summed[w][...] = total.astype(BF)

    def grad_done(w):
        loop(1, S, lambda i: arrived(got[w].at[0], r.gz_send.at[w, lax.rem(s + i, S)]))

    final = {QKV: r.f_qkv, GU: r.f_gu}

    def columns_send(n, w):
        def go(i):
            j = lax.rem(c + i, C)
            remote(summed[w].at[rows_of(j * RW, RW)], final[w].at[c], r.gp_send.at[n, i],
                   r.gp_recv.at[n, c], ctx=j).start()

        loop(1, C, go)
        final[w][c] = summed[w][rows_of(c * RW, RW), :]

    def columns_arrive(n, w):
        loop(1, C, lambda i: arrived(final[w].at[lax.rem(c + i, C)], r.gp_recv.at[n, lax.rem(c + i, C)]))

    def columns_done(n, w):
        loop(1, C, lambda i: arrived(final[w].at[0], r.gp_send.at[n, i]))

    undealt = {OUT: (0, r.g_o, r.h_o, OR)}

    def undeal(w):
        n, src, dst, size = undealt[w]

        def go(j):
            d = S * c + j
            b, place = lax.div(d, C), lax.rem(d, C)
            here, there = src.at[rows_of(j * size, size)], dst.at[rows_of(b * size, size)]

            @pl.when(place != c)
            def _():
                remote(here, there, r.u_send.at[n, j], r.u_recv.at[n], ctx=place).start()

            @pl.when(place == c)
            def _():
                local(here, there, r.u_recv.at[n]).start()

        loop(0, S, go)

    def undeal_arrive(w):
        n, src, dst, size = undealt[w]
        arrived(dst, r.u_recv.at[n])

    def undeal_done(w):
        n, src, dst, size = undealt[w]

        def go(j):
            @pl.when(lax.rem(S * c + j, C) != c)
            def _():
                arrived(src.at[pl.ds(0, size)], r.u_send.at[n, j])

        loop(0, S, go)

    gains_own = r.gains_all.at[flat]
    gain_copy = local(r.gains_in, gains_own, r.gain_recv.at[s])
    gain_copy.start()

    def gain_go(i):
        remote(r.gains_in, gains_own, r.gain_send.at[i], r.gain_recv.at[s],
               ctx=lax.rem(c + i, C)).start()

    loop(1, C, gain_go)

    def qkv_piece(j):
        return (
            (r.wq_in.at[:, rows_of(j * H * HD, H * HD)], slice(0, H * HD)),
            (r.wk_in.at[:, rows_of(j * HD, HD)], slice(H * HD, (H + 1) * HD)),
            (r.wv_in.at[:, rows_of(j * HD, HD)], slice((H + 1) * HD, (H + 2) * HD)),
        )

    def gu_piece(j):
        return ((r.gu_own.at[j], slice(0, 2 * U)),)

    def gu_order(k, ref):
        for j in range(C):
            parts = [ref[:, (C * b + j) * DR : (C * b + j + 1) * DR] for b in range(S)]
            r.gu_own[j, :, k * U : (k + 1) * U] = jnp.concatenate(parts, axis=1)

    columns_of = {QKV: r.w_qkv, GU: r.w_gu}

    def spread(n, w, piece):
        ref = columns_of[w]
        own = rows_of(s * PR + c * RW, RW)

        def go(i):
            j = lax.rem(c + i, C)
            for src, columns in piece(j):
                remote(src, ref.at[own, columns], r.w_send.at[n], r.w_recv.at[n], ctx=j).start()

        loop(1, C, go)
        for src, columns in piece(c):
            local(src, ref.at[own, columns], r.w_recv.at[n]).start()

    def spread_arrive(n, w):
        arrived(columns_of[w].at[rows_of(s * PR, PR)], r.w_recv.at[n])

    def spread_done(n, w):
        arrived(columns_of[w].at[pl.ds(0, (C - 1) * RW)], r.w_send.at[n])

    weight_start(OUT, r.wo_in)
    spread(0, QKV, qkv_piece)
    local(r.x_in, block(X, c), r.local_sem.at[0]).start()
    local(r.table_in, r.table, r.local_sem.at[1]).start()
    local(r.wg_in, r.wg_own, r.local_sem.at[4]).start()
    local(r.wu_in, r.wu_own, r.local_sem.at[5]).start()
    gather_send(X, r.x_in)
    arrived(r.wg_own, r.local_sem.at[4])
    gu_order(0, r.wg_own)
    arrived(r.wu_own, r.local_sem.at[5])
    gu_order(1, r.wu_own)
    weight_hop(OUT, 0)
    spread_arrive(0, QKV)
    weight_start(QKV)
    weight_start(QKV2)
    arrived(r.gains_all.at[pl.ds(s * C, C)], r.gain_recv.at[s])

    def gain_far(i):
        mine = r.gains_all.at[pl.ds(s * C, C)]
        remote(mine, mine, r.gain_send.at[C + i], r.gain_recv.at[s], seq=lax.rem(s + i, S)).start()

    loop(1, S, gain_far)

    arrived(r.table, r.local_sem.at[1])

    def tables(b):
        rows = rows_of(b * T, T)
        both = r.table[rows, :]
        other = pltpu.roll(both, HD // 2, 1)
        first = lax.broadcasted_iota(jnp.int32, (T, HD), 1) < HD // 2
        r.cosine[rows, :] = jnp.where(first, both, other)
        r.sine[rows, :] = jnp.where(first, -other, both)

    loop(0, L // T, tables)
    arrived(block(X, c), r.local_sem.at[0])
    gather_relay(X, 1)
    gather_relay(X, 2)
    weight_hop(QKV, 0)
    weight_hop(QKV2, 0)
    gather_relay(X, 3)
    spread(1, GU, gu_piece)
    deal(OUT, s, r.wo_in)
    deal_hop(OUT, 0)
    local(r.g_in, block(G, c), r.local_sem.at[2]).start()
    gather_send(G, r.g_in)

    def gain_block(i):
        p = lax.rem(s + i, S)
        arrived(r.gains_all.at[pl.ds(p * C, C)], r.gain_recv.at[p])

    loop(1, S, gain_block)
    gains = jnp.sum(r.gains_all[...], axis=1).astype(BF)

    def gain_vector(offset, count):
        width = count * S * C
        shift = count.bit_length() - 1
        column = lax.broadcasted_iota(jnp.int32, (HD, width), 1)
        row = lax.broadcasted_iota(jnp.int32, (HD, width), 0)
        pick = jnp.where(row == offset + (column & (count - 1)), 1.0, 0.0).astype(BF)
        spread_out = nn(gains, pick)
        owner = lax.broadcasted_iota(jnp.int32, (S * C, width), 0)
        place = lax.broadcasted_iota(jnp.int32, (S * C, width), 1) >> shift
        return jnp.sum(jnp.where(owner == place, spread_out, 0.0), axis=0, keepdims=True)

    n1 = D // (S * C)
    n3 = HD // (S * C)
    r.gain1[...] = gain_vector(0, n1)
    r.gain2[...] = gain_vector(n1, n1)
    r.gainq[...] = gain_vector(2 * n1, n3)
    r.gaink[...] = gain_vector(2 * n1 + n3, n3)

    arrived(block(X, sibling), r.ag_recv.at[X, sibling])
    loop(1, CH, lambda i: gather_other(X, i))

    def first_norm(k):
        x = r.x_all[r.order[1, k]].astype(F32)
        r.h1[rows_of(k * RUN, RUN), :] = (x * inverse_root(x) * r.gain1[...]).astype(BF)

    loop(0, NR, first_norm)
    weight_hop(QKV, 1)
    weight_hop(QKV2, 1)
    weight_hop(OUT, 1)
    weight_start(DOWN, r.wd_in)
    local(r.wd_in, plane(DOWN, s), r.local_sem.at[3]).start()
    deal_hop(OUT, 1)
    weight_hop(QKV, 2)
    gather_relay(G, 1)
    gather_relay(G, 2)
    weight_hop(QKV2, 2)

    def rotate(u, rows):
        return u * r.cosine[rows, :] + pltpu.roll(u, HD // 2, 1) * r.sine[rows, :]

    def rotate_back(u, rows):
        return u * r.cosine[rows, :] - pltpu.roll(u, HD // 2, 1) * r.sine[rows, :]

    def project(b):
        rows = rows_of(b * BLOCK, BLOCK)
        acc = nn(r.h1[rows, :], r.w_qkv[...])
        for h in range(H):
            u = acc[:, h * HD : (h + 1) * HD]
            r.q_lin[h, rows, :] = u
            r.q_rot[h, rows, :] = rotate(u * inverse_root(u) * r.gainq[...], rows).astype(BF)
        u = acc[:, H * HD : (H + 1) * HD]
        r.k_lin[rows, :] = u
        k = rotate(u * inverse_root(u) * r.gaink[...], rows)
        r.k_rot[rows, :] = k.astype(BF)
        r.k_t[:, rows] = k.T.astype(BF)
        v = acc[:, (H + 1) * HD :]
        r.v[rows, :] = v.astype(BF)
        r.v_t[:, rows] = v.T.astype(BF)

    loop(0, NB, project)
    weight_hop(OUT, 2)
    deal_hop(OUT, 2)
    spread_arrive(1, GU)

    def attend(qb):
        @pl.when(qb == NB - 2)
        def _():
            gather_relay(G, 3)

        @pl.when(qb == NB - 1)
        def _():
            weight_hop(DOWN, 0)
            weight_start(GATE)

        cols = rows_of(qb * BLOCK, BLOCK)

        def keys(kb, carry):
            rows = rows_of(kb * BLOCK, BLOCK)
            key = r.k_rot[rows, :]
            value_t = r.v_t[:, rows]
            ahead = lax.broadcasted_iota(jnp.int32, (BLOCK, BLOCK), 0) - lax.broadcasted_iota(
                jnp.int32, (BLOCK, BLOCK), 1
            )
            allowed = ahead <= (qb - kb) * BLOCK
            out = []
            for h in range(H):
                acc, total = carry[2 * h], carry[2 * h + 1]
                e = jnp.exp(nt(key, r.q_rot[h, cols, :]) * scale)
                e = jnp.where(allowed, e, 0.0)
                low = e.astype(BF)
                r.e[h, rows, cols] = low
                out += [acc + nn(value_t, low), total + jnp.sum(e, axis=0, keepdims=True)]
            return tuple(out)

        zero = (jnp.zeros((HD, BLOCK), F32), jnp.zeros((1, BLOCK), F32)) * H
        done = lax.fori_loop(0, qb + 1, keys, zero)
        for h in range(H):
            inverse = 1.0 / done[2 * h + 1]
            o = done[2 * h] * inverse
            r.l_inv[h, :, cols] = jnp.broadcast_to(inverse, (8, BLOCK))
            r.o_t[h, :, cols] = o
            r.o_sorted[runs_of(qb), :, h * HD : (h + 1) * HD] = o.T.astype(BF).reshape(-1, RUN, HD)

    loop(0, NB, attend)
    def unsort(i):
        r.o[rows_of(i * RUN, RUN), :] = r.o_sorted[r.order[0, i]]

    loop(0, NR, unsort)

    deal_arrive(OUT)
    scatter(0, lambda i: nn(r.o[rows_of(partner(i) * 2 * T, 2 * T), :], r.w_o[...]))
    weight_hop(DOWN, 1)
    weight_start(UP)
    weight_hop(GATE, 0)
    scatter_mid(0)
    weight_hop(DOWN, 2)
    y1 = own_x() + scatter_sum(0)
    r.y1[...] = y1
    h2_own = (y1 * inverse_root(y1) * r.gain2[...]).astype(BF)
    r.h2_all[rows_of(c * T, T), :] = h2_own
    gather_send(H2, block(H2, c))

    weight_hop(GATE, 1)
    arrived(block(G, c), r.local_sem.at[2])
    arrived(block(G, sibling), r.ag_recv.at[G, sibling])
    loop(1, CH, lambda i: gather_other(G, i))
    arrived(plane(DOWN, s), r.local_sem.at[3])

    def act_grad(b):
        rows = rows_of(b * BLOCK, BLOCK)
        r.d_act[rows, :] = nt(r.g_all[rows, :], r.w_d[...])

    loop(0, NB, act_grad)
    weight_hop(UP, 0)
    gather_relay(H2, 1)
    gather_relay(H2, 2)
    weight_hop(GATE, 2)
    weight_hop(UP, 1)
    arrived(block(H2, sibling), r.ag_recv.at[H2, sibling])

    def feed_gate(i):
        @pl.when(i == 3)
        def _():
            gather_relay(H2, 3)

        @pl.when(i > 0)
        def _():
            gather_other(H2, i)

        rows = rows_of(partner(i) * 2 * T, 2 * T)
        r.gate[rows, :] = nn(r.h2_all[rows, :], r.w_gu[:, :U])

    loop(0, CH, feed_gate)
    weight_hop(UP, 2)
    scatter_done(0)

    def feed(i):
        rows = rows_of(partner(i) * 2 * T, 2 * T)
        up = nn(r.h2_all[rows, :], r.w_gu[:, U:])
        gate = r.gate[rows, :]
        sig = 1.0 / (1.0 + jnp.exp(-gate))
        silu = gate * sig
        r.act[rows, :] = (silu * up).astype(BF)
        d_act = r.d_act[rows, :]
        r.d_gu[rows, :U] = (d_act * up * sig * (1.0 + gate * (1.0 - sig))).astype(BF)
        r.d_gu[rows, U:] = (d_act * silu).astype(BF)
        return nt(r.d_gu[rows, :], r.w_gu[...])

    scatter(2, feed)

    def gu_grad(i):
        p = grad_order(i)
        cols = rows_of(p * PR, PR)
        r.g_gu[cols, :] = tn(r.h2_all[:, cols], r.d_gu[...]).astype(BF)
        grad_out(GU, p)

    loop(0, S, gu_grad)
    scatter_mid(2)

    def down_grad(m):
        cols = rows_of(m * HD, HD)
        r.g_d[cols, :] = tn(r.act[:, cols], r.g_all[...]).astype(BF)

    loop(0, U // HD, down_grad)
    loop(0, S, lambda i: grad_out(DOWN, grad_order(i)))
    d_h2 = scatter_sum(2)
    y1 = r.y1[...]
    r2 = inverse_root(y1)
    normed = y1 * r2
    term2 = jnp.sum(d_h2 * normed, axis=0, keepdims=True)
    d_y1 = r.g_all[rows_of(c * T, T), :].astype(F32) + norm_backward(d_h2 * r.gain2[...], normed, r2)
    r.d_y1[...] = d_y1
    r.dy_all[rows_of(c * T, T), :] = d_y1.astype(BF)
    gather_send(DY, block(DY, c))
    scatter_done(2)
    scatter_pairs(1, lambda i: nn(r.act[rows_of(partner(i) * 2 * T, 2 * T), :], r.w_d[...]))
    WT = D // HD
    for k in range(WT):
        r.terms[WT + k : WT + k + 1, :] = term2[:, k * HD : (k + 1) * HD]

    arrived(block(DY, sibling), r.ag_recv.at[DY, sibling])

    def out_grad(i):
        @pl.when(i == 1)
        def _():
            gather_relay(DY, 1)
            gather_relay(DY, 2)

        @pl.when(i == 3)
        def _():
            gather_relay(DY, 3)

        @pl.when(i > 0)
        def _():
            gather_other(DY, i)

        rows = rows_of(partner(i) * 2 * T, 2 * T)
        d_o = nt(r.dy_all[rows, :], r.w_o[...]).astype(BF)
        r.d_o[pl.ds(partner(i) * (2 * T // RUN), 2 * T // RUN)] = d_o.reshape(-1, RUN, H * HD)

    loop(0, CH, out_grad)

    def out_weight(m):
        cols = rows_of(m * HD, HD)
        r.g_o[cols, :] = tn(r.o[:, cols], r.dy_all[...]).astype(BF)

    loop(0, H * HD // HD, out_weight)
    undeal(OUT)
    for i in (3, 1, 2):
        scatter_chip(1, i)
    grad_combine(GU, 0)

    def sort(k):
        r.d_o_sorted[rows_of(k * RUN, RUN), :] = r.d_o[r.order[1, k]]

    loop(0, NR, sort)
    r.d_k[...] = jnp.zeros_like(r.d_k)
    r.d_v[...] = jnp.zeros_like(r.d_v)
    r.sums[...] = jnp.zeros_like(r.sums)

    def attend_back(qb):
        @pl.when(qb == NB - 1)
        def _():
            undeal_arrive(OUT)
            loop(0, S, lambda i: grad_out(OUT, grad_order(i)))
            scatter_mid(1)

        cols = rows_of(qb * BLOCK, BLOCK)
        d_o_t, d_o_low, row, factor = [], [], [], []
        for h in range(H):
            t = r.d_o_sorted[cols, h * HD : (h + 1) * HD].astype(F32).T
            inverse = r.l_inv[h, 0:1, cols]
            row.append(jnp.sum(t * r.o_t[h, :, cols], axis=0, keepdims=True))
            factor.append(inverse * scale)
            r.do_t[h] = t.astype(BF)
            r.do_l[h] = (t * inverse).T.astype(BF)

        def keys(kb, carry):
            rows = rows_of(kb * BLOCK, BLOCK)
            value = r.v[rows, :]
            key_t = r.k_t[:, rows]
            out = []
            d_k = r.d_k[rows, :]
            d_v = r.d_v[rows, :]
            for h in range(H):
                e = r.e[h, rows, cols]
                dp = nn(value, r.do_t[h])
                de = (e.astype(F32) * ((dp - row[h]) * factor[h])).astype(BF)
                out.append(carry[h] + nn(key_t, de))
                d_k = d_k + nn(de, r.q_rot[h, cols, :])
                d_v = d_v + nn(e, r.do_l[h])
            r.d_k[rows, :] = d_k
            r.d_v[rows, :] = d_v
            return tuple(out)

        done = lax.fori_loop(0, qb + 1, keys, (jnp.zeros((HD, BLOCK), F32),) * H)
        for h in range(H):
            d_g = rotate_back(done[h].T, cols)
            u = r.q_lin[h, cols, :]
            inverse = inverse_root(u)
            normed = u * inverse
            r.sums[0:1, :] += jnp.sum(d_g * normed, axis=0, keepdims=True)
            d_lin = norm_backward(d_g * r.gainq[...], normed, inverse).astype(BF)
            r.d_qkv[runs_of(qb), :, h * HD : (h + 1) * HD] = d_lin.reshape(-1, RUN, HD)

    loop(0, NB, attend_back)

    def key_back(b):
        rows = rows_of(b * BLOCK, BLOCK)
        d_g = rotate_back(r.d_k[rows, :], rows)
        u = r.k_lin[rows, :]
        inverse = inverse_root(u)
        normed = u * inverse
        r.sums[1:2, :] += jnp.sum(d_g * normed, axis=0, keepdims=True)
        d_lin = norm_backward(d_g * r.gaink[...], normed, inverse).astype(BF)
        r.d_qkv[runs_of(b), :, H * HD : (H + 1) * HD] = d_lin.reshape(-1, RUN, HD)
        r.d_qkv[runs_of(b), :, (H + 1) * HD :] = r.d_v[rows, :].astype(BF).reshape(-1, RUN, HD)

    loop(0, NB, key_back)
    r.y_out[...] = (r.y1[...] + scatter_sum(1)).astype(BF)
    local(r.y_out, r.layer_out, r.out_sem.at[0]).start()

    def qkv_grad(i):
        p = grad_order(i)
        cols = rows_of(p * PR, PR)
        r.g_qkv[cols, :] = tn(r.h1[:, cols], r.d_qkv[...].reshape(L, AC)).astype(BF)
        grad_out(QKV, p)

    loop(0, S, qkv_grad)
    grad_combine(GU, 1)
    scatter_done(1)

    def in_chip(i):
        j = partner(i) * 2
        parts = []
        for k in range(2 * T // RUN):
            parts.append(r.d_qkv[r.order[0, j * (T // RUN) + k]])
        return nt(jnp.concatenate(parts, axis=0), r.w_qkv[...])

    scatter(3, in_chip)
    grad_combine(DOWN, 0)
    scatter_mid(3)
    grad_sum(GU)
    columns_send(1, GU)
    grad_combine(DOWN, 1)
    d_h1 = scatter_sum(3)
    x = own_x()
    r1 = inverse_root(x)
    normed = x * r1
    term1 = jnp.sum(d_h1 * normed, axis=0, keepdims=True)
    r.x_grad[...] = r.d_y1[...] + norm_backward(d_h1 * r.gain1[...], normed, r1)
    local(r.x_grad, r.hidden_grad, r.out_sem.at[1]).start()
    for k in range(WT):
        r.terms[k : k + 1, :] = term1[:, k * HD : (k + 1) * HD]
    r.terms[2 * WT : 2 * WT + 8, :] = r.sums[...]

    def terms_far(i):
        remote(r.terms, r.terms_z.at[s], r.t_send.at[i], r.t_recv.at[s],
               seq=lax.rem(s + i, S)).start()

    loop(1, S, terms_far)
    scatter_done(3)
    grad_combine(OUT, 0)
    grad_combine(OUT, 1)
    columns_arrive(1, GU)
    local(r.f_gu, r.gu_out, r.out_sem.at[3]).start()
    grad_sum(DOWN)
    local(r.u_d, r.down_out, r.out_sem.at[2]).start()
    grad_combine(QKV, 0)
    grad_combine(QKV, 1)
    grad_sum(OUT)
    local(r.u_o, r.o_out, r.out_sem.at[4]).start()
    grad_sum(QKV)
    columns_send(0, QKV)
    total = r.terms[...]
    for i in range(1, S):
        p = lax.rem(s + i, S)
        arrived(r.terms_z.at[p], r.t_recv.at[p])
        total = total + r.terms_z[p]
    r.terms_sum[...] = total

    def terms_near(i):
        remote(r.terms_sum, r.terms_p.at[c], r.t_send.at[S + i], r.t_recv.at[S + c],
               ctx=lax.rem(c + i, C)).start()

    loop(1, C, terms_near)

    columns_arrive(0, QKV)
    local(r.f_qkv, r.qkv_out, r.out_sem.at[5]).start()
    total = r.terms_sum[...]
    for i in range(1, C):
        j = lax.rem(c + i, C)
        arrived(r.terms_p.at[j], r.t_recv.at[S + j])
        total = total + r.terms_p[j]
    r.terms_all[...] = total
    local(r.terms_all, r.terms_out, r.out_sem.at[6]).start()

    loop(1, C, lambda i: arrived(gains_own, r.gain_send.at[i]))
    loop(1, S, lambda i: arrived(r.gains_all.at[pl.ds(0, C)], r.gain_send.at[C + i]))
    for kind in (X, G, H2, DY):
        gather_done(kind)
    spread_done(0, QKV)
    spread_done(1, GU)
    deal_done(OUT)
    undeal_done(OUT)
    for w in (QKV, QKV2, GATE, UP, OUT, DOWN):
        weight_done(w)
    for w in (QKV, OUT, GU, DOWN):
        grad_done(w)
    columns_done(0, QKV)
    columns_done(1, GU)
    loop(1, S, lambda i: arrived(r.terms, r.t_send.at[i]))
    loop(1, C, lambda i: arrived(r.terms, r.t_send.at[S + i]))
    pairs = (
        (r.y_out, r.layer_out), (r.x_grad, r.hidden_grad), (r.u_d, r.down_out), (r.f_gu, r.gu_out),
        (r.u_o, r.o_out), (r.f_qkv, r.qkv_out), (r.terms_all, r.terms_out),
    )
    for k, (src, dst) in enumerate(pairs):
        local(src, dst, r.out_sem.at[k]).wait()


def finish_kernel(dims, refs):
    S, C, D, H, U = dims.S, dims.C, dims.D, dims.H, dims.U
    HD = HEAD_DIMENSION
    r = refs
    me = lax.axis_index("seq") * C + lax.axis_index("ctx")
    r.layer_res[...] = r.layer_out[...]
    r.hidden_res[...] = r.hidden_grad[...]
    r.delta_down[...] = r.down_out[...].astype(F32)
    r.delta_out[...] = r.o_out[...].astype(F32)
    for j in range(C):
        r.delta_query[:, j * H * HD : (j + 1) * H * HD] = r.qkv_out[j, :, : H * HD].astype(F32)
        r.delta_key[:, j * HD : (j + 1) * HD] = r.qkv_out[j, :, H * HD : (H + 1) * HD].astype(F32)
        r.delta_value[:, j * HD : (j + 1) * HD] = r.qkv_out[j, :, (H + 1) * HD :].astype(F32)

    for k, ref in ((0, r.delta_gate), (1, r.delta_up)):
        for d in range(0, S * C, 4):
            parts = []
            for e in range(d, d + 4):
                first = k * U + (e // C) * dims.DR
                parts.append(r.gu_out[e % C, :, first : first + dims.DR].astype(F32))
            ref[:, d * dims.DR : (d + 4) * dims.DR] = jnp.concatenate(parts, axis=1)

    def own(ref, first_row, count):
        start = me * count
        row = r.terms_out[pl.ds(first_row + lax.div(start, HD), 1), :]
        back = lax.rem(HD - lax.rem(start, HD), HD)
        ref[...] = pltpu.roll(jnp.broadcast_to(row, (8, HD)), back, 1)[0:1, :count]

    n1, n3 = D // (S * C), HD // (S * C)
    own(r.change1, 0, n1)
    own(r.change2, D // HD, n1)
    own(r.changeq, 2 * (D // HD), n3)
    own(r.changek, 2 * (D // HD) + 1, n3)


def fused_layer(mesh, args):
    (x, positions, gain1, wq, wk, wv, gainq, gaink, wo, gain2, wg, wu, wd, g) = args
    S, C = mesh.shape["seq"], mesh.shape["ctx"]
    T, D = x.shape[1:]
    L = positions.shape[1]
    HD = HEAD_DIMENSION
    H = QUERY_HEAD_COUNT // C
    RW, OR, DR = wq.shape[0], wo.shape[0], wd.shape[0]
    U = wg.shape[1] // C
    AC = (H + 2) * HD
    PR = C * RW
    CH = C // 2
    dims = types.SimpleNamespace(S=S, C=C, T=T, L=L, D=D, H=H, RW=RW, OR=OR, DR=DR, AC=AC, U=U)
    packed = jnp.concatenate([gain1, gain2, gainq, gaink]).astype(F32)
    packed = jnp.pad(packed[None, :], ((0, 7), (0, HD - packed.shape[0])))
    half = HD // 2
    frequency = np.power(THETA, -np.arange(half) * (2.0 / HD))
    phases = np.arange(L)[:, None] * frequency[None, :]
    table = jnp.asarray(np.concatenate([np.cos(phases), np.sin(phases)], axis=1), F32)
    TR = 2 * (D // HD) + 8
    run = positions[0, ::RUN] // RUN
    spot = jnp.arange(L // RUN, dtype=jnp.int32)
    place = jnp.sum(jnp.where(run[None, :] == spot[:, None], spot[None, :], 0), axis=1)
    order = jnp.stack([run, place]).astype(jnp.int32)
    inputs = dict(
        order=order, x_in=x.reshape(T // RUN, RUN, D), g_in=g[0], gains_in=packed, wq_in=wq, wk_in=wk, wv_in=wv, wo_in=wo,
        wg_in=wg, wu_in=wu, wd_in=wd, table_in=table,
    )
    TR_shape = ((TR, HD), F32)
    outputs = dict(
        layer_out=((T, D), BF), hidden_grad=((T, D), F32), qkv_out=((C, RW, AC), BF), o_out=((OR, D), BF),
        gu_out=((C, RW, 2 * U), BF), down_out=((DR, D), BF), terms_out=TR_shape,
    )
    n1, n3 = D // (S * C), HD // (S * C)
    final = dict(
        layer_res=((T, D), BF), hidden_res=((T, D), F32), change1=((1, n1), F32),
        delta_query=((RW, C * H * HD), F32), delta_key=((RW, C * HD), F32), delta_value=((RW, C * HD), F32),
        changeq=((1, n3), F32), changek=((1, n3), F32), delta_out=((OR, D), F32), change2=((1, n1), F32),
        delta_gate=((RW, C * U), F32), delta_up=((RW, C * U), F32), delta_down=((DR, D), F32),
    )
    V, DMA = pltpu.VMEM, pltpu.SemaphoreType.DMA
    scratch = dict(
        x_all=V((L // RUN, RUN, D), BF), g_all=V((L, D), BF), h2_all=V((L, D), BF), dy_all=V((L, D), BF),
        h1=V((L, D), BF), w_qkv=V((D, AC), BF), w_o=V((H * HD, D), BF), w_gu=V((D, 2 * U), BF),
        w_d=V((U, D), BF), gains_all=V((S * C, 8, HD), F32), table=V((L, HD), F32),
        cosine=V((L, HD), F32), sine=V((L, HD), F32), gain1=V((1, D), F32), gain2=V((1, D), F32),
        gainq=V((1, HD), F32), gaink=V((1, HD), F32), q_lin=V((H, L, HD), F32), k_lin=V((L, HD), F32),
        q_rot=V((H, L, HD), BF), k_rot=V((L, HD), BF), v=V((L, HD), BF), k_t=V((HD, L), BF),
        v_t=V((HD, L), BF), e=V((H, L, L), BF), l_inv=V((H, 8, L), F32), o_t=V((H, HD, L), F32),
        o_sorted=V((L // RUN, RUN, H * HD), BF), o=V((L, H * HD), BF), y1=V((T, D), F32), gate=V((L, U), F32), d_act=V((L, U), F32),
        act=V((L, U), BF), d_gu=V((L, 2 * U), BF), d_y1=V((T, D), F32), d_o=V((L // RUN, RUN, H * HD), BF),
        d_o_sorted=V((L, H * HD), BF), do_t=V((H, HD, BLOCK), BF), do_l=V((H, BLOCK, HD), BF),
        d_k=V((L, HD), F32), d_v=V((L, HD), F32), d_qkv=V((L // RUN, RUN, AC), BF), sums=V((8, HD), F32),
        pair=V((CH, 2 * T, D), F32), s1=V((CH, T, D), BF), r1=V((2, CH, T, D), BF),
        s2=V((CH, T, D), BF), r2=V((2, 3, T, D), BF), s3=V((T, D), BF),
        g_qkv=V((D, AC), BF), g_o=V((H * HD, D), BF), g_gu=V((D, 2 * U), BF), g_d=V((U, D), BF),
        t_qkv=V((2, PR, AC), BF), t_o=V((2, OR, D), BF), t_gu=V((2, PR, 2 * U), BF), t_d=V((2, DR, D), BF),
        c_qkv=V((2, PR, AC), BF), c_o=V((2, OR, D), BF), c_gu=V((2, PR, 2 * U), BF), c_d=V((2, DR, D), BF),
        z_o=V((S, OR, D), BF), y_out=V((T, D), BF), x_grad=V((T, D), F32), terms_all=V(*TR_shape),
        u_qkv=V((PR, AC), BF), u_o=V((OR, D), BF), u_gu=V((PR, 2 * U), BF), u_d=V((DR, D), BF),
        f_qkv=V((C, RW, AC), BF), h_o=V((S * OR, D), BF), f_gu=V((C, RW, 2 * U), BF), gu_own=V((C, RW, 2 * U), BF),
        wg_own=V((RW, C * U), BF), wu_own=V((RW, C * U), BF),
        terms=V((TR, HD), F32), terms_z=V((S, TR, HD), F32), terms_sum=V((TR, HD), F32),
        terms_p=V((C, TR, HD), F32),
        ag_send=DMA((4, 2 * CH)), ag_recv=DMA((4, C)), rs_send=DMA((4, CH + 6)), r1_recv=DMA((4, CH)),
        r2_recv=DMA((4, 6)), z_send=DMA((6, 2, S)), z_recv=DMA((6, S)), gz_send=DMA((5, S)),
        gz_recv=DMA((5, 2)), gc_recv=DMA((5, 2)), gp_send=DMA((2, C)), gp_recv=DMA((2, C)), u_send=DMA((1, S)),
        u_recv=DMA((1,)), w_send=DMA((2,)), w_recv=DMA((2,)), m_send=DMA((1, S)), m_recv=DMA((1,)),
        gain_send=DMA((C + S,)), gain_recv=DMA((S,)), t_send=DMA((S + C,)), t_recv=DMA((S + C,)),
        local_sem=DMA((6,)), out_sem=DMA((7,)),
    )
    names = list(inputs) + list(outputs) + list(scratch)

    def kernel(*refs):
        layer_kernel(dims, types.SimpleNamespace(**dict(zip(names, refs))))

    in_specs = [
        pl.BlockSpec(memory_space=pltpu.SMEM if name == "order" else pl.ANY) for name in inputs
    ]
    results = pl.pallas_call(
        kernel,
        out_shape=[jax.ShapeDtypeStruct(*v) for v in outputs.values()],
        in_specs=in_specs,
        out_specs=[pl.BlockSpec(memory_space=pl.ANY)] * len(outputs),
        scratch_shapes=list(scratch.values()),
        compiler_params=pltpu.CompilerParams(
            collective_id=0, has_side_effects=True, vmem_limit_bytes=67043328
        ),
        name="layer",
    )(*inputs.values())
    finish_names = list(outputs) + list(final)

    def finish(*refs):
        finish_kernel(dims, types.SimpleNamespace(**dict(zip(finish_names, refs))))

    out = pl.pallas_call(
        finish,
        out_shape=[jax.ShapeDtypeStruct(*v) for v in final.values()],
        in_specs=[pl.BlockSpec(memory_space=pltpu.VMEM)] * len(outputs),
        out_specs=[pl.BlockSpec(memory_space=pltpu.VMEM)] * len(final),
        name="finish",
    )(*results)
    one_axis = [k for k, v in enumerate(final.values()) if v[0][0] == 1]
    out = [o.reshape(-1) if k in one_axis else o for k, o in enumerate(out)]
    return (out[0][None], out[1][None], *out[2:])


def angles(places, head_size):
    half_size = head_size // 2
    frequency = jnp.power(THETA, -jnp.arange(half_size, dtype=F32) * (2.0 / head_size))
    phases = places.astype(F32)[:, None] * frequency[None, :]
    phases = jnp.concatenate([phases, phases], axis=-1)
    return (jnp.cos(phases), jnp.sin(phases))


def rotate(values, cosines, sines):
    half_size = values.shape[-1] // 2
    turned = jnp.concatenate([-values[..., half_size:], values[..., :half_size]], axis=-1)
    return values * cosines + turned * sines


def rotate_back(upstream, cosines, sines):
    half_size = upstream.shape[-1] // 2
    scaled = upstream * sines
    turned = jnp.concatenate([scaled[..., half_size:], -scaled[..., :half_size]], axis=-1)
    return upstream * cosines + turned


def dot(a, b):
    return jnp.dot(a, b, preferred_element_type=F32)


def local_of(mesh):
    seqs, ranks = mesh.shape["seq"], mesh.shape["ctx"]
    devices = seqs * ranks
    axes = ("seq", "ctx")

    def spread(shard, heads):
        rows, columns = shard.shape
        if heads and heads < ranks:
            blocks = shard.reshape(rows, heads, 1, columns // heads)
            blocks = jnp.broadcast_to(blocks, (rows, heads, ranks // heads, columns // heads))
            return blocks.reshape(rows, ranks, columns // heads)
        return shard.reshape(rows, ranks, columns // ranks)

    def fold(blocks, heads):
        rows, count, width = blocks.shape
        if heads and heads < ranks:
            return blocks.reshape(rows, heads, count // heads, width).sum(2).reshape(rows, heads * width)
        return blocks.reshape(rows, count * width)

    forth = [(seqs * r + j, j * ranks + r) for r in range(ranks) for j in range(seqs)]
    back = [(b, a) for a, b in forth]

    def local(
        hidden_states, positions, gain_first, weight_query, key_weight_matrix, value_weight_matrix,
        gain_query, gain_key, weight_output, gain_second, weight_gate, weight_up, weight_down,
        output_cotangent,
    ):
        tokens = hidden_states.shape[1]
        length = positions.shape[1]
        size = HEAD_DIMENSION
        group = QUERY_HEAD_COUNT // KEY_VALUE_HEADS
        my_q = QUERY_HEAD_COUNT // ranks
        my_k = max(1, KEY_VALUE_HEADS // ranks)
        scale = size ** (-0.5)
        places = positions[0]
        cosines, sines = angles(places, size)
        cosines, sines = cosines[:, None, :], sines[:, None, :]

        gains = jnp.concatenate([gain_first, gain_second, gain_query, gain_key])
        gains = lax.all_gather(gains, axes, axis=0).astype(F32)
        n1, n2, n3, n4 = (g.shape[0] for g in (gain_first, gain_second, gain_query, gain_key))
        first_scale = gains[:, :n1].reshape(-1)
        second_scale = gains[:, n1 : n1 + n2].reshape(-1)
        query_scale = gains[:, n1 + n2 : n1 + n2 + n3].reshape(-1)
        key_scale = gains[:, n1 + n2 + n3 :].reshape(-1)

        column_weights = jnp.concatenate(
            [
                spread(weight_query, 0),
                spread(key_weight_matrix, KEY_VALUE_HEADS),
                spread(value_weight_matrix, KEY_VALUE_HEADS),
                spread(weight_gate, 0),
                spread(weight_up, 0),
            ],
            axis=2,
        )
        column_weights = lax.all_to_all(column_weights, "ctx", split_axis=1, concat_axis=0, tiled=True)
        column_weights = lax.all_gather(column_weights[:, 0], "seq", axis=0, tiled=True)
        row_weights = jnp.concatenate([weight_output, weight_down], axis=0)
        row_weights = lax.all_gather(lax.ppermute(row_weights, axes, forth), "seq", axis=0)
        o_rows, d_rows = weight_output.shape[0], weight_down.shape[0]
        width = weight_output.shape[1]
        w_o = row_weights[:, :o_rows].reshape(-1, width)
        w_d = row_weights[:, o_rows:].reshape(-1, width)
        units = w_d.shape[0]
        attn_columns = (my_q + 2 * my_k) * size
        w_qkv = column_weights[:, :attn_columns]
        w_gu = column_weights[:, attn_columns:]

        x = lax.all_gather(hidden_states[0], "ctx", axis=0, tiled=True).astype(F32)
        g_low = lax.all_gather(output_cotangent[0], "ctx", axis=0, tiled=True)
        first_inverse = inverse_root(x)
        h1 = (x * first_inverse * first_scale).astype(BF)
        qkv = dot(h1, w_qkv)
        q_lin = qkv[:, : my_q * size].reshape(length, my_q, size)
        k_lin = qkv[:, my_q * size : (my_q + my_k) * size].reshape(length, my_k, size)
        v = qkv[:, (my_q + my_k) * size :].astype(BF).reshape(length, my_k, size)
        rq, rk = inverse_root(q_lin), inverse_root(k_lin)
        nq, nk = q_lin * rq, k_lin * rk
        qr = rotate(nq * query_scale, cosines, sines).astype(BF)
        kr = rotate(nk * key_scale, cosines, sines).astype(BF)
        mask = places[None, :] <= places[:, None]

        def scores(h):
            e = lax.dot_general(
                qr[:, h], kr[:, h // group], (((1,), (1,)), ((), ())), preferred_element_type=F32
            )
            return jnp.where(mask, e * scale, NEGATIVE)

        outs, probs = [], []
        for h in range(my_q):
            e = scores(h)
            p = jnp.exp(e - jnp.max(e, axis=-1, keepdims=True))
            p = p / jnp.sum(p, axis=-1, keepdims=True)
            probs.append(p)
            outs.append(dot(p.astype(BF), v[:, h // group]))
        o = jnp.concatenate(outs, axis=1).astype(BF)

        def scatter(part):
            return lax.psum_scatter(part.astype(BF), "ctx", scatter_dimension=0, tiled=True).astype(F32)

        x_own = hidden_states[0].astype(F32)
        y1 = x_own + scatter(dot(o, w_o))
        r2 = inverse_root(y1)
        second_normed = y1 * r2
        h2 = lax.all_gather((second_normed * second_scale).astype(BF), "ctx", axis=0, tiled=True)
        gu = dot(h2, w_gu)
        gate, up = gu[:, :units], gu[:, units:]
        sig = jax.nn.sigmoid(gate)
        silu = gate * sig
        act = (silu * up).astype(BF)
        layer_output = (y1 + scatter(dot(act, w_d))).astype(BF)

        d_act = dot(g_low, w_d.T)
        d_gate = (d_act * up * sig * (1.0 + gate * (1.0 - sig))).astype(BF)
        d_up = (d_act * silu).astype(BF)
        d_gu = jnp.concatenate([d_gate, d_up], axis=1)
        d_h2 = scatter(dot(d_gu, w_gu.T))
        second_term = jnp.sum(d_h2 * second_normed, axis=0)
        d_y1 = output_cotangent[0].astype(F32) + norm_backward(d_h2 * second_scale, second_normed, r2)
        d_y1_low = lax.all_gather(d_y1.astype(BF), "ctx", axis=0, tiled=True)
        d_o = dot(d_y1_low, w_o.T).astype(BF).reshape(length, my_q, size)

        d_q, d_k, d_v = [], [0.0] * my_k, [0.0] * my_k
        for h in range(my_q):
            p = probs[h]
            dp = lax.dot_general(
                d_o[:, h], v[:, h // group], (((1,), (1,)), ((), ())), preferred_element_type=F32
            )
            row = jnp.sum(p * dp, axis=-1, keepdims=True)
            de = (p * (dp - row) * scale).astype(BF)
            d_q.append(dot(de, kr[:, h // group]))
            d_k[h // group] += dot(de.T, qr[:, h])
            d_v[h // group] += dot(p.astype(BF).T, d_o[:, h])
        d_q, d_k, d_v = jnp.stack(d_q, 1), jnp.stack(d_k, 1), jnp.stack(d_v, 1)
        d_gq, d_gk = rotate_back(d_q, cosines, sines), rotate_back(d_k, cosines, sines)
        query_term = jnp.sum(d_gq * nq, axis=(0, 1))
        key_term = jnp.sum(d_gk * nk, axis=(0, 1))
        d_qlin = norm_backward(d_gq * query_scale, nq, rq).reshape(length, -1)
        d_klin = norm_backward(d_gk * key_scale, nk, rk).reshape(length, -1)
        d_qkv = jnp.concatenate([d_qlin, d_klin, d_v.reshape(length, -1)], axis=1).astype(BF)
        d_h1 = scatter(dot(d_qkv, w_qkv.T))
        r1 = inverse_root(x_own)
        first_normed = x_own * r1
        first_term = jnp.sum(d_h1 * first_normed, axis=0)
        hidden_gradient = d_y1 + norm_backward(d_h1 * first_scale, first_normed, r1)

        def rows_sum(part):
            part = lax.psum_scatter(part.astype(BF), "seq", scatter_dimension=0, tiled=True)
            return lax.ppermute(part, axes, back).astype(F32)

        delta_rows = jnp.concatenate(
            [dot(o.T, d_y1_low).reshape(seqs, o_rows, width), dot(act.T, g_low).reshape(seqs, d_rows, width)],
            axis=1,
        ).reshape(-1, width)
        delta_rows = rows_sum(delta_rows)
        delta_columns = jnp.concatenate([dot(h1.T, d_qkv), dot(h2.T, d_gu)], axis=1).astype(BF)
        delta_columns = lax.psum_scatter(delta_columns, "seq", scatter_dimension=0, tiled=True)
        own = delta_columns.shape[0] // ranks
        delta_columns = lax.all_to_all(
            delta_columns.reshape(ranks, own, -1), "ctx", split_axis=0, concat_axis=0, tiled=True
        )
        delta_columns = jnp.moveaxis(delta_columns, 0, 1).astype(F32)
        cuts = [my_q * size, (my_q + my_k) * size, (my_q + 2 * my_k) * size, attn_columns + units]
        parts = jnp.split(delta_columns, cuts, axis=2)
        delta_query = fold(parts[0], 0)
        delta_key = fold(parts[1], KEY_VALUE_HEADS)
        delta_value = fold(parts[2], KEY_VALUE_HEADS)
        delta_gate, delta_up = fold(parts[3], 0), fold(parts[4], 0)

        terms = lax.psum(jnp.concatenate([first_term, second_term, query_term, key_term]), axes)
        me = lax.axis_index("seq") * ranks + lax.axis_index("ctx")
        w = width

        def mine(start, n):
            return lax.dynamic_slice_in_dim(terms, start + me * n, n)

        return (
            layer_output[None],
            hidden_gradient[None],
            mine(0, n1),
            delta_query,
            delta_key,
            delta_value,
            mine(2 * w, n3),
            mine(2 * w + size, n4),
            delta_rows[:o_rows],
            mine(w, n2),
            delta_gate,
            delta_up,
            delta_rows[o_rows:],
        )

    return local


def solution(mesh):
    token = P("seq", "ctx", None)
    flat = P(("seq", "ctx"))
    rows = P(("seq", "ctx"), None)
    general = local_of(mesh)

    def body(*args):
        tokens, length = args[0].shape[1], args[1].shape[1]
        fits = (
            mesh.shape["ctx"] == KEY_VALUE_HEADS == 8
            and mesh.shape["seq"] == 4
            and length <= 1024
            and length % BLOCK == 0
            and tokens % RUN == 0
            and HEAD_DIMENSION % (mesh.shape["seq"] * mesh.shape["ctx"]) == 0
        )
        return fused_layer(mesh, args) if fits else general(*args)

    return jax.shard_map(
        body,
        mesh=mesh,
        in_specs=(token, P("seq", None), flat, rows, rows, rows, flat, flat, rows, flat, rows, rows, rows, token),
        out_specs=(token, token, flat, rows, rows, rows, flat, flat, rows, flat, rows, rows, rows),
        check_vma=False,
    )
```

```python
import types

import jax
import jax.numpy as jnp
import numpy as np
from jax import lax
from jax.experimental import pallas as pl
from jax.experimental.pallas import tpu as pltpu
from jax.sharding import PartitionSpec as P

QUERY_HEAD_COUNT = 16
KEY_VALUE_HEADS = 8
HEAD_DIMENSION = 128

EPS = 1e-06
THETA = 1000000.0
NEGATIVE = -1e30
BF = jnp.bfloat16
F32 = jnp.float32
MESH = pl.DeviceIdType.MESH
RUN = 64
BLOCK = 256


def nn(a, b):
    return jnp.dot(a, b, preferred_element_type=F32)


def nt(a, b):
    return lax.dot_general(a, b, (((1,), (1,)), ((), ())), preferred_element_type=F32)


def tn(a, b):
    return lax.dot_general(a, b, (((0,), (0,)), ((), ())), preferred_element_type=F32)


def loop(low, high, body):
    def step(i, carry):
        body(i)
        return carry

    lax.fori_loop(low, high, step, 0)


def rows_of(start, size):
    return pl.ds(pl.multiple_of(start, size), size)


def inverse_root(values):
    return lax.rsqrt(jnp.mean(values * values, axis=-1, keepdims=True) + EPS)


def norm_backward(normed_grad, normed, inverse):
    return inverse * (normed_grad - normed * jnp.mean(normed_grad * normed, axis=-1, keepdims=True))


def layer_kernel(dims, refs):
    S, C, T, L, D = dims.S, dims.C, dims.T, dims.L, dims.D
    H, RW, OR, DR, AC, U = dims.H, dims.RW, dims.OR, dims.DR, dims.AC, dims.U
    HD = HEAD_DIMENSION
    PR = C * RW
    NR = L // RUN
    NB = L // BLOCK
    CH = C // 2
    scale = HD ** (-0.5)
    r = refs
    s = lax.axis_index("seq")
    c = lax.axis_index("ctx")
    chip = lax.div(c, 2)
    core = lax.rem(c, 2)
    chip_y, chip_x = lax.div(chip, 2), lax.rem(chip, 2)
    sibling = chip * 2 + (1 - core)
    flat = s * C + c
    def partner(i):
        x = lax.rem(chip_x + lax.rem(i, 2), 2)
        y = lax.rem(chip_y + lax.div(i, 2), 2)
        return y * 2 + x

    def remote(src, dst, send, recv, **where):
        return pltpu.make_async_remote_copy(
            src_ref=src, dst_ref=dst, send_sem=send, recv_sem=recv, device_id=where, device_id_type=MESH
        )

    def local(src, dst, sem):
        return pltpu.make_async_copy(src, dst, sem)

    def arrived(dst, sem):
        pltpu.make_async_copy(dst, dst, sem).wait()

    barrier = pltpu.get_barrier_semaphore()

    def hello(**where):
        pl.semaphore_signal(barrier, inc=1, device_id=where, device_id_type=MESH)

    loop(1, C, lambda i: hello(ctx=lax.rem(c + i, C)))
    loop(1, S, lambda i: hello(seq=lax.rem(s + i, S)))

    pl.semaphore_wait(barrier, C - 1 + S - 1)

    def runs_of(b):
        return pl.ds(b * (BLOCK // RUN), BLOCK // RUN)

    def own_x():
        return r.x_all[pl.ds(c * (T // RUN), T // RUN)].reshape(T, D).astype(F32)

    X, G, H2, DY = 0, 1, 2, 3
    whole = {X: r.x_all, G: r.g_all, H2: r.h2_all, DY: r.dy_all}

    def block(kind, j):
        if kind == X:
            return whole[kind].at[pl.ds(j * (T // RUN), T // RUN)]
        return whole[kind].at[rows_of(j * T, T)]

    def half(ref, k):
        part = pl.ds(k * (D // 2), D // 2)
        return ref.at[:, :, part] if len(ref.shape) == 3 else ref.at[:, part]

    def gather_send(kind, src):
        for i in (1, 2):
            remote(src, block(kind, c), r.ag_send.at[kind, i], r.ag_recv.at[kind, c],
                   ctx=partner(i) * 2 + core).start()
        remote(src, block(kind, c), r.ag_send.at[kind, 0], r.ag_recv.at[kind, c], ctx=sibling).start()

    def gather_relay(kind, i):
        j = partner(i) * 2 + core
        arrived(block(kind, j), r.ag_recv.at[kind, j])

        @pl.when(i == 1)
        def _():
            part = half(block(kind, j), 0)
            remote(part, part, r.ag_send.at[kind, 3], r.ag_recv.at[kind, j], ctx=partner(2) * 2 + core).start()

        @pl.when(i == 2)
        def _():
            part = half(block(kind, j), 1)
            remote(part, part, r.ag_send.at[kind, 7], r.ag_recv.at[kind, j], ctx=partner(1) * 2 + core).start()

        remote(block(kind, j), block(kind, j), r.ag_send.at[kind, 3 + i], r.ag_recv.at[kind, j],
               ctx=sibling).start()

    def gather_other(kind, i):
        j = partner(i) * 2 + (1 - core)
        arrived(block(kind, j), r.ag_recv.at[kind, j])

    def gather_done(kind):
        for i in (0, 1, 2, 4, 5, 6):
            arrived(block(kind, c), r.ag_send.at[kind, i])
        for i in (3, 7):
            arrived(half(block(kind, c), 0), r.ag_send.at[kind, i])

    def scatter_pair(kind, i, partial):
        r.pair[i] = partial
        r.s1[i] = r.pair[i, rows_of((1 - core) * T, T), :].astype(BF)
        remote(r.s1.at[i], r.r1.at[1 if kind == 1 else 0, i], r.rs_send.at[kind, i],
               r.r1_recv.at[kind, i], ctx=sibling).start()

    def scatter_chip(kind, i):
        bank = 1 if kind == 1 else 0
        arrived(r.r1.at[bank, i], r.r1_recv.at[kind, i])
        mine = r.pair[i, rows_of(core * T, T), :] + r.r1[bank, i].astype(F32)
        r.s2[i] = mine.astype(BF)

        def to(k, slot, send, recv):
            remote(half(r.s2.at[i], k), half(r.r2.at[bank, slot], k), r.rs_send.at[kind, send],
                   r.r2_recv.at[kind, recv], ctx=partner(1 + k) * 2 + core).start()

        @pl.when(i == 1)
        def _():
            to(0, 0, CH, 0)

        @pl.when(i == 2)
        def _():
            to(1, 0, CH + 1, 1)

        @pl.when(i == 3)
        def _():
            to(0, 1, CH + 2, 2)
            to(1, 1, CH + 3, 3)

    def scatter(kind, partial):
        def go(k):
            i = jnp.where(k == 0, 3, jnp.where(k == 3, 0, k))
            scatter_pair(kind, i, partial(i))

            @pl.when(k > 0)
            def _():
                scatter_chip(kind, jnp.where(k == 1, 3, k - 1))

        loop(0, CH, go)

    def scatter_pairs(kind, partial):
        loop(0, CH, lambda i: scatter_pair(kind, i, partial(i)))

    def scatter_mid(kind):
        bank = 1 if kind == 1 else 0
        for k in (0, 1):
            i = 2 - k
            part = slice(k * (D // 2), (k + 1) * (D // 2))
            arrived(half(r.r2.at[bank, 1], k), r.r2_recv.at[kind, 2 + k])
            mine = r.pair[i, rows_of(core * T, T), part] + r.r1[bank, i, :, part].astype(F32)
            r.s3[:, part] = (mine + r.r2[bank, 1, :, part].astype(F32)).astype(BF)
            remote(half(r.s3, k), half(r.r2.at[bank, 2], k), r.rs_send.at[kind, CH + 4 + k],
                   r.r2_recv.at[kind, 4 + k], ctx=partner(i) * 2 + core).start()

    def scatter_sum(kind):
        bank = 1 if kind == 1 else 0
        arrived(r.r1.at[bank, 0], r.r1_recv.at[kind, 0])
        for k in (0, 1):
            arrived(half(r.r2.at[bank, 0], k), r.r2_recv.at[kind, k])
            arrived(half(r.r2.at[bank, 2], k), r.r2_recv.at[kind, 4 + k])
        total = r.pair[0, rows_of(core * T, T), :] + r.r1[bank, 0].astype(F32)
        return total + r.r2[bank, 0].astype(F32) + r.r2[bank, 2].astype(F32)

    def scatter_done(kind):
        loop(0, CH, lambda i: arrived(r.s1.at[0], r.rs_send.at[kind, i]))
        loop(CH, CH + 6, lambda i: arrived(half(r.s3, 0), r.rs_send.at[kind, i]))

    QKV, GATE, UP, OUT, DOWN, QKV2 = 0, 1, 2, 3, 4, 5
    PH = PR // 2

    def plane(w, b):
        if w == QKV:
            return r.w_qkv.at[rows_of(b * PR, PH)]
        if w == QKV2:
            return r.w_qkv.at[rows_of(b * PR + PH, PH)]
        if w == GATE:
            return r.w_gu.at[rows_of(b * PR, PR), pl.ds(0, U)]
        if w == UP:
            return r.w_gu.at[rows_of(b * PR, PR), pl.ds(U, U)]
        if w == DOWN:
            return r.w_d.at[rows_of(b * DR, DR)]
        return r.z_o.at[b]

    def weight_start(w, src=None):
        src = plane(w, s) if src is None else src

        @pl.when(s < S - 1)
        def _():
            remote(src, plane(w, s), r.z_send.at[w, 0, 0], r.z_recv.at[w, s], seq=s + 1).start()

        @pl.when(s > 0)
        def _():
            remote(src, plane(w, s), r.z_send.at[w, 1, 0], r.z_recv.at[w, s], seq=s - 1).start()

    rows_ref = {OUT: (0, r.w_o, OR)}

    def deal(w, b, src=None):
        n, ref, size = rows_ref[w]
        src = plane(w, b) if src is None else src
        d = C * b + c
        rank, spot = lax.div(d, S), lax.rem(d, S)
        dst = ref.at[rows_of(spot * size, size)]

        @pl.when(rank != c)
        def _():
            remote(src, dst, r.m_send.at[n, b], r.m_recv.at[n], ctx=rank).start()

        @pl.when(rank == c)
        def _():
            local(src, dst, r.m_recv.at[n]).start()

    def deal_arrive(w):
        n, ref, size = rows_ref[w]
        arrived(ref, r.m_recv.at[n])

    def deal_done(w):
        n, ref, size = rows_ref[w]

        def go(b):
            @pl.when(lax.div(C * b + c, S) != c)
            def _():
                arrived(plane(w, 0), r.m_send.at[n, b])

        loop(0, S, go)

    def weight_hop(w, t):
        below, above = s - 1 - t, s + 1 + t

        @pl.when(below >= 0)
        def _():
            arrived(plane(w, below), r.z_recv.at[w, below])

            @pl.when(s < S - 1)
            def _():
                remote(plane(w, below), plane(w, below), r.z_send.at[w, 0, t + 1],
                       r.z_recv.at[w, below], seq=s + 1).start()

        @pl.when(above <= S - 1)
        def _():
            arrived(plane(w, above), r.z_recv.at[w, above])

            @pl.when(s > 0)
            def _():
                remote(plane(w, above), plane(w, above), r.z_send.at[w, 1, t + 1],
                       r.z_recv.at[w, above], seq=s - 1).start()

    inner = jnp.logical_and(s > 0, s < S - 1)

    def hop_inner(w, t):
        @pl.when(inner)
        def _():
            weight_hop(w, t)

    def hop_outer(w, t):
        @pl.when(jnp.logical_not(inner))
        def _():
            weight_hop(w, t)

    def deal_hop(w, t):
        below, above = s - 1 - t, s + 1 + t

        @pl.when(below >= 0)
        def _():
            deal(w, below)

        @pl.when(above <= S - 1)
        def _():
            deal(w, above)

    def weight_done(w):
        for t in range(S - 1):
            @pl.when(jnp.logical_and(s - t >= 0, s < S - 1))
            def _():
                arrived(plane(w, s), r.z_send.at[w, 0, t])

            @pl.when(jnp.logical_and(s + t <= S - 1, s > 0))
            def _():
                arrived(plane(w, s), r.z_send.at[w, 1, t])

    GU = GATE
    sent = {QKV: (r.g_q, PR), QKV2: (r.g_kv, PR), OUT: (r.h_o, OR), GU: (r.g_gu, PR), DOWN: (r.g_d, DR)}
    got = {QKV: r.t_q, QKV2: r.t_kv, OUT: r.t_o, GU: r.t_gu, DOWN: r.t_d}
    halfway = {QKV: r.c_q, QKV2: r.c_kv, OUT: r.c_o, GU: r.c_gu, DOWN: r.c_d}
    summed = {QKV: r.u_q, QKV2: r.u_kv, OUT: r.u_o, GU: r.u_gu, DOWN: r.u_d}
    side = jnp.where(s >= 2, 1, 0)

    def grad_rows(w, p):
        ref, size = sent[w]
        return ref.at[rows_of(p * size, size)]

    def grad_order(i):
        return jnp.where(s < 2, lax.rem(3 - i + s, S), lax.rem(i + (3 - s) * 3, S))

    def grad_direct(w, p):
        remote(grad_rows(w, p), got[w].at[side], r.gz_send.at[w, p], r.gz_recv.at[w, side], seq=p).start()

    def grad_out(w, p):
        far_up = jnp.logical_and(s == 0, p >= 2)
        far_down = jnp.logical_and(s == S - 1, p <= 1)
        later = jnp.logical_or(
            jnp.logical_and(s == 1, p >= 2), jnp.logical_and(s == 2, p <= 1)
        )

        @pl.when(far_up)
        def _():
            remote(grad_rows(w, p), halfway[w].at[p - 2], r.gz_send.at[w, p], r.gc_recv.at[w, p - 2],
                   seq=1).start()

        @pl.when(far_down)
        def _():
            remote(grad_rows(w, p), halfway[w].at[p], r.gz_send.at[w, p], r.gc_recv.at[w, p], seq=2).start()

        others = jnp.logical_or(jnp.logical_or(far_up, far_down), jnp.logical_or(later, p == s))

        @pl.when(jnp.logical_not(others))
        def _():
            grad_direct(w, p)

    def grad_combine(w, k):
        @pl.when(jnp.logical_or(s == 1, s == 2))
        def _():
            p = jnp.where(s == 1, 3 - k, k)
            slot = jnp.where(s == 1, 1 - k, k)
            ref, size = sent[w]
            rows = rows_of(p * size, size)
            arrived(halfway[w].at[slot], r.gc_recv.at[w, slot])
            ref[rows, :] = (ref[rows, :].astype(F32) + halfway[w][slot].astype(F32)).astype(BF)
            grad_direct(w, p)

    def grad_sum(w):
        ref, size = sent[w]
        total = ref[rows_of(s * size, size), :].astype(F32)
        for i in range(2):
            arrived(got[w].at[i], r.gz_recv.at[w, i])
            total = total + got[w][i].astype(F32)
        summed[w][...] = total.astype(BF)

    def grad_done(w):
        loop(1, S, lambda i: arrived(got[w].at[0], r.gz_send.at[w, lax.rem(s + i, S)]))

    final = {QKV: r.f_q, QKV2: r.f_kv, GU: r.f_gu}

    def columns_send(n, w):
        def go(i):
            j = lax.rem(c + i, C)
            remote(summed[w].at[rows_of(j * RW, RW)], final[w].at[c], r.gp_send.at[n, i],
                   r.gp_recv.at[n, c], ctx=j).start()

        loop(1, C, go)
        final[w][c] = summed[w][rows_of(c * RW, RW), :]

    def columns_arrive(n, w):
        loop(1, C, lambda i: arrived(final[w].at[lax.rem(c + i, C)], r.gp_recv.at[n, lax.rem(c + i, C)]))

    def columns_done(n, w):
        loop(1, C, lambda i: arrived(final[w].at[0], r.gp_send.at[n, i]))

    undealt = {OUT: (0, r.g_o, r.h_o, OR)}

    def undeal(w):
        n, src, dst, size = undealt[w]

        def go(j):
            d = S * c + j
            b, place = lax.div(d, C), lax.rem(d, C)
            here, there = src.at[rows_of(j * size, size)], dst.at[rows_of(b * size, size)]

            @pl.when(place != c)
            def _():
                remote(here, there, r.u_send.at[n, j], r.u_recv.at[n], ctx=place).start()

            @pl.when(place == c)
            def _():
                local(here, there, r.u_recv.at[n]).start()

        loop(0, S, go)

    def undeal_arrive(w):
        n, src, dst, size = undealt[w]
        arrived(dst, r.u_recv.at[n])

    def undeal_done(w):
        n, src, dst, size = undealt[w]

        def go(j):
            @pl.when(lax.rem(S * c + j, C) != c)
            def _():
                arrived(src.at[pl.ds(0, size)], r.u_send.at[n, j])

        loop(0, S, go)

    gains_own = r.gains_all.at[flat]
    gain_copy = local(r.gains_in, gains_own, r.gain_recv.at[s])
    gain_copy.start()

    def gain_go(i):
        remote(r.gains_in, gains_own, r.gain_send.at[i], r.gain_recv.at[s],
               ctx=lax.rem(c + i, C)).start()

    loop(1, C, gain_go)

    def qkv_piece(j):
        return (
            (r.wq_in.at[:, rows_of(j * H * HD, H * HD)], slice(0, H * HD)),
            (r.wk_in.at[:, rows_of(j * HD, HD)], slice(H * HD, (H + 1) * HD)),
            (r.wv_in.at[:, rows_of(j * HD, HD)], slice((H + 1) * HD, (H + 2) * HD)),
        )

    def gu_piece(j):
        return ((r.gu_own.at[j], slice(0, 2 * U)),)

    def gu_order(k, ref):
        for j in range(C):
            parts = [ref[:, (C * b + j) * DR : (C * b + j + 1) * DR] for b in range(S)]
            r.gu_own[j, :, k * U : (k + 1) * U] = jnp.concatenate(parts, axis=1)

    columns_of = {QKV: r.w_qkv, GU: r.w_gu}

    def spread(n, w, piece):
        ref = columns_of[w]
        own = rows_of(s * PR + c * RW, RW)

        def go(i):
            j = lax.rem(c + i, C)
            for src, columns in piece(j):
                remote(src, ref.at[own, columns], r.w_send.at[n], r.w_recv.at[n], ctx=j).start()

        loop(1, C, go)
        for src, columns in piece(c):
            local(src, ref.at[own, columns], r.w_recv.at[n]).start()

    def spread_arrive(n, w):
        arrived(columns_of[w].at[rows_of(s * PR, PR)], r.w_recv.at[n])

    def spread_done(n, w):
        arrived(columns_of[w].at[pl.ds(0, (C - 1) * RW)], r.w_send.at[n])

    weight_start(OUT, r.wo_in)
    spread(0, QKV, qkv_piece)
    local(r.x_in, block(X, c), r.local_sem.at[0]).start()
    local(r.table_in, r.table, r.local_sem.at[1]).start()
    local(r.wg_in, r.wg_own, r.local_sem.at[4]).start()
    local(r.wu_in, r.wu_own, r.local_sem.at[5]).start()
    gather_send(X, r.x_in)
    arrived(r.wg_own, r.local_sem.at[4])
    gu_order(0, r.wg_own)
    arrived(r.wu_own, r.local_sem.at[5])
    gu_order(1, r.wu_own)
    weight_hop(OUT, 0)
    spread_arrive(0, QKV)
    weight_start(QKV)
    weight_start(QKV2)
    arrived(r.gains_all.at[pl.ds(s * C, C)], r.gain_recv.at[s])

    def gain_far(i):
        mine = r.gains_all.at[pl.ds(s * C, C)]
        remote(mine, mine, r.gain_send.at[C + i], r.gain_recv.at[s], seq=lax.rem(s + i, S)).start()

    loop(1, S, gain_far)

    arrived(r.table, r.local_sem.at[1])

    def tables(b):
        rows = rows_of(b * T, T)
        both = r.table[rows, :]
        other = pltpu.roll(both, HD // 2, 1)
        first = lax.broadcasted_iota(jnp.int32, (T, HD), 1) < HD // 2
        r.cosine[rows, :] = jnp.where(first, both, other)
        r.sine[rows, :] = jnp.where(first, -other, both)

    loop(0, L // T, tables)
    arrived(block(X, c), r.local_sem.at[0])
    gather_relay(X, 1)
    gather_relay(X, 2)
    weight_hop(QKV, 0)
    weight_hop(QKV2, 0)
    gather_relay(X, 3)
    spread(1, GU, gu_piece)
    deal(OUT, s, r.wo_in)
    deal_hop(OUT, 0)
    local(r.g_in, block(G, c), r.local_sem.at[2]).start()
    gather_send(G, r.g_in)

    def gain_block(i):
        p = lax.rem(s + i, S)
        arrived(r.gains_all.at[pl.ds(p * C, C)], r.gain_recv.at[p])

    loop(1, S, gain_block)
    gains = jnp.sum(r.gains_all[...], axis=1).astype(BF)

    def gain_vector(offset, count):
        width = count * S * C
        shift = count.bit_length() - 1
        column = lax.broadcasted_iota(jnp.int32, (HD, width), 1)
        row = lax.broadcasted_iota(jnp.int32, (HD, width), 0)
        pick = jnp.where(row == offset + (column & (count - 1)), 1.0, 0.0).astype(BF)
        spread_out = nn(gains, pick)
        owner = lax.broadcasted_iota(jnp.int32, (S * C, width), 0)
        place = lax.broadcasted_iota(jnp.int32, (S * C, width), 1) >> shift
        return jnp.sum(jnp.where(owner == place, spread_out, 0.0), axis=0, keepdims=True)

    n1 = D // (S * C)
    n3 = HD // (S * C)
    r.gain1[...] = gain_vector(0, n1)
    r.gain2[...] = gain_vector(n1, n1)
    r.gainq[...] = gain_vector(2 * n1, n3)
    r.gaink[...] = gain_vector(2 * n1 + n3, n3)

    arrived(block(X, sibling), r.ag_recv.at[X, sibling])
    loop(1, CH, lambda i: gather_other(X, i))

    def first_norm(k):
        x = r.x_all[r.order[1, k]].astype(F32)
        r.h1[rows_of(k * RUN, RUN), :] = (x * inverse_root(x) * r.gain1[...]).astype(BF)

    loop(0, NR, first_norm)
    weight_hop(QKV, 1)
    weight_hop(QKV2, 1)
    weight_hop(OUT, 1)
    spread_arrive(1, GU)
    weight_start(GATE)
    local(r.wd_in, plane(DOWN, s), r.local_sem.at[3]).start()
    deal_hop(OUT, 1)
    weight_hop(QKV, 2)
    weight_hop(QKV2, 2)

    def rotate(u, rows):
        return u * r.cosine[rows, :] + pltpu.roll(u, HD // 2, 1) * r.sine[rows, :]

    def rotate_back(u, rows):
        return u * r.cosine[rows, :] - pltpu.roll(u, HD // 2, 1) * r.sine[rows, :]

    def project(b):
        rows = rows_of(b * BLOCK, BLOCK)
        acc = nn(r.h1[rows, :], r.w_qkv[...])
        for h in range(H):
            u = acc[:, h * HD : (h + 1) * HD]
            r.q_lin[h, rows, :] = u
            r.q_rot[h, rows, :] = rotate(u * inverse_root(u) * r.gainq[...], rows).astype(BF)
        u = acc[:, H * HD : (H + 1) * HD]
        r.k_lin[rows, :] = u
        k = rotate(u * inverse_root(u) * r.gaink[...], rows)
        r.k_rot[rows, :] = k.astype(BF)
        r.k_t[:, rows] = k.T.astype(BF)
        v = acc[:, (H + 1) * HD :]
        r.v[rows, :] = v.astype(BF)
        r.v_t[:, rows] = v.T.astype(BF)

    loop(0, NB, project)
    weight_hop(OUT, 2)
    deal_hop(OUT, 2)

    def attend(qb):
        @pl.when(qb == NB - 2)
        def _():
            gather_relay(G, 1)
            gather_relay(G, 2)

        @pl.when(qb == NB - 1)
        def _():
            hop_inner(GATE, 0)
            weight_start(UP)

        cols = rows_of(qb * BLOCK, BLOCK)

        def keys(kb, carry):
            rows = rows_of(kb * BLOCK, BLOCK)
            key = r.k_rot[rows, :]
            value_t = r.v_t[:, rows]
            ahead = lax.broadcasted_iota(jnp.int32, (BLOCK, BLOCK), 0) - lax.broadcasted_iota(
                jnp.int32, (BLOCK, BLOCK), 1
            )
            allowed = ahead <= (qb - kb) * BLOCK
            out = []
            for h in range(H):
                acc, total = carry[2 * h], carry[2 * h + 1]
                e = jnp.exp(nt(key, r.q_rot[h, cols, :]) * scale)
                e = jnp.where(allowed, e, 0.0)
                low = e.astype(BF)
                r.e[h, rows, cols] = low
                out += [acc + nn(value_t, low), total + jnp.sum(e, axis=0, keepdims=True)]
            return tuple(out)

        zero = (jnp.zeros((HD, BLOCK), F32), jnp.zeros((1, BLOCK), F32)) * H
        done = lax.fori_loop(0, qb + 1, keys, zero)
        for h in range(H):
            inverse = 1.0 / done[2 * h + 1]
            o = done[2 * h] * inverse
            r.l_inv[h, :, cols] = jnp.broadcast_to(inverse, (8, BLOCK))
            r.o_t[h, :, cols] = o
            r.o_sorted[runs_of(qb), :, h * HD : (h + 1) * HD] = o.T.astype(BF).reshape(-1, RUN, HD)

    loop(0, NB, attend)
    def unsort(i):
        r.o[rows_of(i * RUN, RUN), :] = r.o_sorted[r.order[0, i]]

    loop(0, NR, unsort)

    deal_arrive(OUT)
    scatter(0, lambda i: nn(r.o[rows_of(partner(i) * 2 * T, 2 * T), :], r.w_o[...]))
    hop_inner(GATE, 1)
    gather_relay(G, 3)
    scatter_mid(0)
    hop_inner(UP, 0)
    y1 = own_x() + scatter_sum(0)
    r.y1[...] = y1
    h2_own = (y1 * inverse_root(y1) * r.gain2[...]).astype(BF)
    r.h2_all[rows_of(c * T, T), :] = h2_own
    gather_send(H2, block(H2, c))

    hop_inner(UP, 1)
    weight_start(DOWN, r.wd_in)
    hop_inner(GATE, 2)
    for w in (GATE, UP):
        for t in range(S - 1):
            hop_outer(w, t)
    hop_inner(UP, 2)
    arrived(block(H2, sibling), r.ag_recv.at[H2, sibling])

    def feed(i):
        @pl.when(i == 1)
        def _():
            gather_relay(H2, 1)
            gather_relay(H2, 2)
            hop_inner(DOWN, 0)

        @pl.when(i == 3)
        def _():
            gather_relay(H2, 3)
            hop_inner(DOWN, 1)

        @pl.when(i > 0)
        def _():
            gather_other(H2, i)

        rows = rows_of(partner(i) * 2 * T, 2 * T)
        both = nn(r.h2_all[rows, :], r.w_gu[...])
        gate, up = both[:, :U], both[:, U:]
        sig = 1.0 / (1.0 + jnp.exp(-gate))
        silu = gate * sig
        r.act[rows, :] = (silu * up).astype(BF)
        r.slope[rows, :] = up * sig * (1.0 + gate * (1.0 - sig))
        r.silu[rows, :] = silu

    loop(0, CH, feed)
    arrived(block(G, c), r.local_sem.at[2])
    arrived(block(G, sibling), r.ag_recv.at[G, sibling])
    loop(1, CH, lambda i: gather_other(G, i))

    def down_grad(m):
        cols = rows_of(m * HD, HD)
        r.g_d[cols, :] = tn(r.act[:, cols], r.g_all[...]).astype(BF)

    loop(0, U // HD, down_grad)
    loop(0, S, lambda i: grad_out(DOWN, grad_order(i)))
    hop_outer(DOWN, 0)
    hop_outer(DOWN, 1)
    weight_hop(DOWN, 2)
    arrived(plane(DOWN, s), r.local_sem.at[3])
    scatter_done(0)

    def feed_back(i):
        rows = rows_of(partner(i) * 2 * T, 2 * T)
        d_act = nt(r.g_all[rows, :], r.w_d[...])
        r.d_gu[rows, :U] = (d_act * r.slope[rows, :]).astype(BF)
        r.d_gu[rows, U:] = (d_act * r.silu[rows, :]).astype(BF)
        return nt(r.d_gu[rows, :], r.w_gu[...])

    scatter(2, feed_back)

    def gu_grad(i):
        p = grad_order(i)
        cols = rows_of(p * PR, PR)
        r.g_gu[cols, :] = tn(r.h2_all[:, cols], r.d_gu[...]).astype(BF)
        grad_out(GU, p)

    loop(0, S, gu_grad)
    scatter_mid(2)
    grad_combine(DOWN, 0)
    d_h2 = scatter_sum(2)
    y1 = r.y1[...]
    r2 = inverse_root(y1)
    normed = y1 * r2
    term2 = jnp.sum(d_h2 * normed, axis=0, keepdims=True)
    d_y1 = r.g_all[rows_of(c * T, T), :].astype(F32) + norm_backward(d_h2 * r.gain2[...], normed, r2)
    r.d_y1[...] = d_y1
    r.dy_all[rows_of(c * T, T), :] = d_y1.astype(BF)
    gather_send(DY, block(DY, c))
    scatter_done(2)
    scatter_pairs(1, lambda i: nn(r.act[rows_of(partner(i) * 2 * T, 2 * T), :], r.w_d[...]))
    WT = D // HD
    for k in range(WT):
        r.terms[WT + k : WT + k + 1, :] = term2[:, k * HD : (k + 1) * HD]

    arrived(block(DY, sibling), r.ag_recv.at[DY, sibling])

    def out_grad(i):
        @pl.when(i == 1)
        def _():
            gather_relay(DY, 1)
            gather_relay(DY, 2)

        @pl.when(i == 3)
        def _():
            gather_relay(DY, 3)

        @pl.when(i > 0)
        def _():
            gather_other(DY, i)

        rows = rows_of(partner(i) * 2 * T, 2 * T)
        d_o = nt(r.dy_all[rows, :], r.w_o[...]).astype(BF)
        r.d_o[pl.ds(partner(i) * (2 * T // RUN), 2 * T // RUN)] = d_o.reshape(-1, RUN, H * HD)

    loop(0, CH, out_grad)

    def out_weight(m):
        cols = rows_of(m * HD, HD)
        r.g_o[cols, :] = tn(r.o[:, cols], r.dy_all[...]).astype(BF)

    loop(0, H * HD // HD, out_weight)
    undeal(OUT)
    for i in (3, 1, 2):
        scatter_chip(1, i)
    grad_combine(DOWN, 1)
    grad_combine(GU, 0)

    def sort(k):
        r.d_o_sorted[rows_of(k * RUN, RUN), :] = r.d_o[r.order[1, k]]

    loop(0, NR, sort)
    r.d_k[...] = jnp.zeros_like(r.d_k)
    r.d_v[...] = jnp.zeros_like(r.d_v)
    r.sums[...] = jnp.zeros_like(r.sums)

    def attend_back(qb):
        @pl.when(qb == NB - 1)
        def _():
            undeal_arrive(OUT)
            loop(0, S, lambda i: grad_out(OUT, grad_order(i)))

        cols = rows_of(qb * BLOCK, BLOCK)
        d_o_t, d_o_low, row, factor = [], [], [], []
        for h in range(H):
            t = r.d_o_sorted[cols, h * HD : (h + 1) * HD].astype(F32).T
            inverse = r.l_inv[h, 0:1, cols]
            row.append(jnp.sum(t * r.o_t[h, :, cols], axis=0, keepdims=True))
            factor.append(inverse * scale)
            r.do_t[h] = t.astype(BF)
            r.do_l[h] = (t * inverse).T.astype(BF)

        def keys(kb, carry):
            rows = rows_of(kb * BLOCK, BLOCK)
            value = r.v[rows, :]
            key_t = r.k_t[:, rows]
            out = []
            d_k = r.d_k[rows, :]
            d_v = r.d_v[rows, :]
            for h in range(H):
                e = r.e[h, rows, cols]
                dp = nn(value, r.do_t[h])
                de = (e.astype(F32) * ((dp - row[h]) * factor[h])).astype(BF)
                out.append(carry[h] + nn(key_t, de))
                d_k = d_k + nn(de, r.q_rot[h, cols, :])
                d_v = d_v + nn(e, r.do_l[h])
            r.d_k[rows, :] = d_k
            r.d_v[rows, :] = d_v
            return tuple(out)

        done = lax.fori_loop(0, qb + 1, keys, (jnp.zeros((HD, BLOCK), F32),) * H)
        for h in range(H):
            d_g = rotate_back(done[h].T, cols)
            u = r.q_lin[h, cols, :]
            inverse = inverse_root(u)
            normed = u * inverse
            r.sums[0:1, :] += jnp.sum(d_g * normed, axis=0, keepdims=True)
            d_lin = norm_backward(d_g * r.gainq[...], normed, inverse).astype(BF)
            r.d_qkv[runs_of(qb), :, h * HD : (h + 1) * HD] = d_lin.reshape(-1, RUN, HD)

    loop(0, NB, attend_back)

    def key_back(b):
        rows = rows_of(b * BLOCK, BLOCK)
        d_g = rotate_back(r.d_k[rows, :], rows)
        u = r.k_lin[rows, :]
        inverse = inverse_root(u)
        normed = u * inverse
        r.sums[1:2, :] += jnp.sum(d_g * normed, axis=0, keepdims=True)
        d_lin = norm_backward(d_g * r.gaink[...], normed, inverse).astype(BF)
        r.d_qkv[runs_of(b), :, H * HD : (H + 1) * HD] = d_lin.reshape(-1, RUN, HD)
        r.d_qkv[runs_of(b), :, (H + 1) * HD :] = r.d_v[rows, :].astype(BF).reshape(-1, RUN, HD)

    loop(0, NB, key_back)
    scatter_mid(1)

    def qkv_grad(i):
        p = grad_order(i)
        cols = rows_of(p * PR, PR)
        both = tn(r.h1[:, cols], r.d_qkv[...].reshape(L, AC)).astype(BF)
        r.g_q[cols, :] = both[:, : H * HD]
        r.g_kv[cols, :] = both[:, H * HD :]
        grad_out(QKV, p)

    loop(0, S, qkv_grad)
    loop(0, S, lambda i: grad_out(QKV2, grad_order(i)))
    grad_combine(GU, 1)
    r.y_out[...] = (r.y1[...] + scatter_sum(1)).astype(BF)
    local(r.y_out, r.layer_out, r.out_sem.at[0]).start()
    scatter_done(1)

    def in_chip(i):
        j = partner(i) * 2
        parts = []
        for k in range(2 * T // RUN):
            parts.append(r.d_qkv[r.order[0, j * (T // RUN) + k]])
        return nt(jnp.concatenate(parts, axis=0), r.w_qkv[...])

    scatter(3, in_chip)
    grad_combine(OUT, 0)
    scatter_mid(3)
    grad_sum(GU)
    columns_send(1, GU)
    grad_combine(OUT, 1)
    d_h1 = scatter_sum(3)
    x = own_x()
    r1 = inverse_root(x)
    normed = x * r1
    term1 = jnp.sum(d_h1 * normed, axis=0, keepdims=True)
    r.x_grad[...] = r.d_y1[...] + norm_backward(d_h1 * r.gain1[...], normed, r1)
    local(r.x_grad, r.hidden_grad, r.out_sem.at[1]).start()
    for k in range(WT):
        r.terms[k : k + 1, :] = term1[:, k * HD : (k + 1) * HD]
    r.terms[2 * WT : 2 * WT + 8, :] = r.sums[...]

    def terms_far(i):
        remote(r.terms, r.terms_z.at[s], r.t_send.at[i], r.t_recv.at[s],
               seq=lax.rem(s + i, S)).start()

    loop(1, S, terms_far)
    scatter_done(3)
    grad_combine(QKV, 0)
    grad_sum(DOWN)
    local(r.u_d, r.down_out, r.out_sem.at[2]).start()
    grad_combine(QKV, 1)
    grad_sum(OUT)
    local(r.u_o, r.o_out, r.out_sem.at[4]).start()
    grad_combine(QKV2, 0)
    columns_arrive(1, GU)
    local(r.f_gu, r.gu_out, r.out_sem.at[3]).start()
    grad_combine(QKV2, 1)
    grad_sum(QKV)
    columns_send(0, QKV)
    grad_sum(QKV2)
    columns_send(2, QKV2)
    total = r.terms[...]
    for i in range(1, S):
        p = lax.rem(s + i, S)
        arrived(r.terms_z.at[p], r.t_recv.at[p])
        total = total + r.terms_z[p]
    r.terms_sum[...] = total

    def terms_near(i):
        remote(r.terms_sum, r.terms_p.at[c], r.t_send.at[S + i], r.t_recv.at[S + c],
               ctx=lax.rem(c + i, C)).start()

    loop(1, C, terms_near)

    columns_arrive(0, QKV)
    local(r.f_q, r.q_out, r.out_sem.at[5]).start()
    total = r.terms_sum[...]
    for i in range(1, C):
        j = lax.rem(c + i, C)
        arrived(r.terms_p.at[j], r.t_recv.at[S + j])
        total = total + r.terms_p[j]
    r.terms_all[...] = total
    local(r.terms_all, r.terms_out, r.out_sem.at[6]).start()
    columns_arrive(2, QKV2)
    local(r.f_kv, r.kv_out, r.out_sem.at[7]).start()

    loop(1, C, lambda i: arrived(gains_own, r.gain_send.at[i]))
    loop(1, S, lambda i: arrived(r.gains_all.at[pl.ds(0, C)], r.gain_send.at[C + i]))
    for kind in (X, G, H2, DY):
        gather_done(kind)
    spread_done(0, QKV)
    spread_done(1, GU)
    deal_done(OUT)
    undeal_done(OUT)
    for w in (QKV, QKV2, GATE, UP, OUT, DOWN):
        weight_done(w)
    for w in (QKV, QKV2, OUT, GU, DOWN):
        grad_done(w)
    columns_done(0, QKV)
    columns_done(2, QKV2)
    columns_done(1, GU)
    loop(1, S, lambda i: arrived(r.terms, r.t_send.at[i]))
    loop(1, C, lambda i: arrived(r.terms, r.t_send.at[S + i]))
    pairs = (
        (r.y_out, r.layer_out), (r.x_grad, r.hidden_grad), (r.u_d, r.down_out), (r.f_gu, r.gu_out),
        (r.u_o, r.o_out), (r.f_q, r.q_out), (r.terms_all, r.terms_out), (r.f_kv, r.kv_out),
    )
    for k, (src, dst) in enumerate(pairs):
        local(src, dst, r.out_sem.at[k]).wait()


def finish_kernel(dims, refs):
    S, C, D, H, U = dims.S, dims.C, dims.D, dims.H, dims.U
    HD = HEAD_DIMENSION
    r = refs
    me = lax.axis_index("seq") * C + lax.axis_index("ctx")
    r.layer_res[...] = r.layer_out[...]
    r.hidden_res[...] = r.hidden_grad[...]
    r.delta_down[...] = r.down_out[...].astype(F32)
    r.delta_out[...] = r.o_out[...].astype(F32)
    for j in range(C):
        r.delta_query[:, j * H * HD : (j + 1) * H * HD] = r.q_out[j].astype(F32)
        r.delta_key[:, j * HD : (j + 1) * HD] = r.kv_out[j, :, :HD].astype(F32)
        r.delta_value[:, j * HD : (j + 1) * HD] = r.kv_out[j, :, HD:].astype(F32)

    for k, ref in ((0, r.delta_gate), (1, r.delta_up)):
        for d in range(0, S * C, 4):
            parts = []
            for e in range(d, d + 4):
                first = k * U + (e // C) * dims.DR
                parts.append(r.gu_out[e % C, :, first : first + dims.DR].astype(F32))
            ref[:, d * dims.DR : (d + 4) * dims.DR] = jnp.concatenate(parts, axis=1)

    def own(ref, first_row, count):
        start = me * count
        row = r.terms_out[pl.ds(first_row + lax.div(start, HD), 1), :]
        back = lax.rem(HD - lax.rem(start, HD), HD)
        ref[...] = pltpu.roll(jnp.broadcast_to(row, (8, HD)), back, 1)[0:1, :count]

    n1, n3 = D // (S * C), HD // (S * C)
    own(r.change1, 0, n1)
    own(r.change2, D // HD, n1)
    own(r.changeq, 2 * (D // HD), n3)
    own(r.changek, 2 * (D // HD) + 1, n3)


def fused_layer(mesh, args):
    (x, positions, gain1, wq, wk, wv, gainq, gaink, wo, gain2, wg, wu, wd, g) = args
    S, C = mesh.shape["seq"], mesh.shape["ctx"]
    T, D = x.shape[1:]
    L = positions.shape[1]
    HD = HEAD_DIMENSION
    H = QUERY_HEAD_COUNT // C
    RW, OR, DR = wq.shape[0], wo.shape[0], wd.shape[0]
    U = wg.shape[1] // C
    AC = (H + 2) * HD
    PR = C * RW
    CH = C // 2
    dims = types.SimpleNamespace(S=S, C=C, T=T, L=L, D=D, H=H, RW=RW, OR=OR, DR=DR, AC=AC, U=U)
    packed = jnp.concatenate([gain1, gain2, gainq, gaink]).astype(F32)
    packed = jnp.pad(packed[None, :], ((0, 7), (0, HD - packed.shape[0])))
    half = HD // 2
    frequency = np.power(THETA, -np.arange(half) * (2.0 / HD))
    phases = np.arange(L)[:, None] * frequency[None, :]
    table = jnp.asarray(np.concatenate([np.cos(phases), np.sin(phases)], axis=1), F32)
    TR = 2 * (D // HD) + 8
    run = positions[0, ::RUN] // RUN
    spot = jnp.arange(L // RUN, dtype=jnp.int32)
    place = jnp.sum(jnp.where(run[None, :] == spot[:, None], spot[None, :], 0), axis=1)
    order = jnp.stack([run, place]).astype(jnp.int32)
    inputs = dict(
        order=order, x_in=x.reshape(T // RUN, RUN, D), g_in=g[0], gains_in=packed, wq_in=wq, wk_in=wk, wv_in=wv, wo_in=wo,
        wg_in=wg, wu_in=wu, wd_in=wd, table_in=table,
    )
    TR_shape = ((TR, HD), F32)
    outputs = dict(
        layer_out=((T, D), BF), hidden_grad=((T, D), F32), q_out=((C, RW, H * HD), BF), kv_out=((C, RW, 2 * HD), BF), o_out=((OR, D), BF),
        gu_out=((C, RW, 2 * U), BF), down_out=((DR, D), BF), terms_out=TR_shape,
    )
    n1, n3 = D // (S * C), HD // (S * C)
    final = dict(
        layer_res=((T, D), BF), hidden_res=((T, D), F32), change1=((1, n1), F32),
        delta_query=((RW, C * H * HD), F32), delta_key=((RW, C * HD), F32), delta_value=((RW, C * HD), F32),
        changeq=((1, n3), F32), changek=((1, n3), F32), delta_out=((OR, D), F32), change2=((1, n1), F32),
        delta_gate=((RW, C * U), F32), delta_up=((RW, C * U), F32), delta_down=((DR, D), F32),
    )
    V, DMA = pltpu.VMEM, pltpu.SemaphoreType.DMA
    scratch = dict(
        x_all=V((L // RUN, RUN, D), BF), g_all=V((L, D), BF), h2_all=V((L, D), BF), dy_all=V((L, D), BF),
        h1=V((L, D), BF), w_qkv=V((D, AC), BF), w_o=V((H * HD, D), BF), w_gu=V((D, 2 * U), BF),
        w_d=V((U, D), BF), gains_all=V((S * C, 8, HD), F32), table=V((L, HD), F32),
        cosine=V((L, HD), F32), sine=V((L, HD), F32), gain1=V((1, D), F32), gain2=V((1, D), F32),
        gainq=V((1, HD), F32), gaink=V((1, HD), F32), q_lin=V((H, L, HD), F32), k_lin=V((L, HD), F32),
        q_rot=V((H, L, HD), BF), k_rot=V((L, HD), BF), v=V((L, HD), BF), k_t=V((HD, L), BF),
        v_t=V((HD, L), BF), e=V((H, L, L), BF), l_inv=V((H, 8, L), F32), o_t=V((H, HD, L), F32),
        o_sorted=V((L // RUN, RUN, H * HD), BF), o=V((L, H * HD), BF), y1=V((T, D), F32), slope=V((L, U), F32), silu=V((L, U), F32),
        act=V((L, U), BF), d_gu=V((L, 2 * U), BF), d_y1=V((T, D), F32), d_o=V((L // RUN, RUN, H * HD), BF),
        d_o_sorted=V((L, H * HD), BF), do_t=V((H, HD, BLOCK), BF), do_l=V((H, BLOCK, HD), BF),
        d_k=V((L, HD), F32), d_v=V((L, HD), F32), d_qkv=V((L // RUN, RUN, AC), BF), sums=V((8, HD), F32),
        pair=V((CH, 2 * T, D), F32), s1=V((CH, T, D), BF), r1=V((2, CH, T, D), BF),
        s2=V((CH, T, D), BF), r2=V((2, 3, T, D), BF), s3=V((T, D), BF),
        g_q=V((D, H * HD), BF), g_kv=V((D, 2 * HD), BF), g_o=V((H * HD, D), BF), g_gu=V((D, 2 * U), BF), g_d=V((U, D), BF),
        t_q=V((2, PR, H * HD), BF), t_kv=V((2, PR, 2 * HD), BF), t_o=V((2, OR, D), BF), t_gu=V((2, PR, 2 * U), BF), t_d=V((2, DR, D), BF),
        c_q=V((2, PR, H * HD), BF), c_kv=V((2, PR, 2 * HD), BF), c_o=V((2, OR, D), BF), c_gu=V((2, PR, 2 * U), BF), c_d=V((2, DR, D), BF),
        z_o=V((S, OR, D), BF), y_out=V((T, D), BF), x_grad=V((T, D), F32), terms_all=V(*TR_shape),
        u_q=V((PR, H * HD), BF), u_kv=V((PR, 2 * HD), BF), u_o=V((OR, D), BF), u_gu=V((PR, 2 * U), BF), u_d=V((DR, D), BF),
        f_q=V((C, RW, H * HD), BF), f_kv=V((C, RW, 2 * HD), BF), h_o=V((S * OR, D), BF), f_gu=V((C, RW, 2 * U), BF), gu_own=V((C, RW, 2 * U), BF),
        wg_own=V((RW, C * U), BF), wu_own=V((RW, C * U), BF),
        terms=V((TR, HD), F32), terms_z=V((S, TR, HD), F32), terms_sum=V((TR, HD), F32),
        terms_p=V((C, TR, HD), F32),
        ag_send=DMA((4, 2 * CH)), ag_recv=DMA((4, C)), rs_send=DMA((4, CH + 6)), r1_recv=DMA((4, CH)),
        r2_recv=DMA((4, 6)), z_send=DMA((6, 2, S)), z_recv=DMA((6, S)), gz_send=DMA((6, S)),
        gz_recv=DMA((6, 2)), gc_recv=DMA((6, 2)), gp_send=DMA((3, C)), gp_recv=DMA((3, C)), u_send=DMA((1, S)),
        u_recv=DMA((1,)), w_send=DMA((2,)), w_recv=DMA((2,)), m_send=DMA((1, S)), m_recv=DMA((1,)),
        gain_send=DMA((C + S,)), gain_recv=DMA((S,)), t_send=DMA((S + C,)), t_recv=DMA((S + C,)),
        local_sem=DMA((6,)), out_sem=DMA((8,)),
    )
    names = list(inputs) + list(outputs) + list(scratch)

    def kernel(*refs):
        layer_kernel(dims, types.SimpleNamespace(**dict(zip(names, refs))))

    in_specs = [
        pl.BlockSpec(memory_space=pltpu.SMEM if name == "order" else pl.ANY) for name in inputs
    ]
    results = pl.pallas_call(
        kernel,
        out_shape=[jax.ShapeDtypeStruct(*v) for v in outputs.values()],
        in_specs=in_specs,
        out_specs=[pl.BlockSpec(memory_space=pl.ANY)] * len(outputs),
        scratch_shapes=list(scratch.values()),
        compiler_params=pltpu.CompilerParams(
            collective_id=0, has_side_effects=True, vmem_limit_bytes=67043328
        ),
        name="layer",
    )(*inputs.values())
    finish_names = list(outputs) + list(final)

    def finish(*refs):
        finish_kernel(dims, types.SimpleNamespace(**dict(zip(finish_names, refs))))

    out = pl.pallas_call(
        finish,
        out_shape=[jax.ShapeDtypeStruct(*v) for v in final.values()],
        in_specs=[pl.BlockSpec(memory_space=pltpu.VMEM)] * len(outputs),
        out_specs=[pl.BlockSpec(memory_space=pltpu.VMEM)] * len(final),
        name="finish",
    )(*results)
    one_axis = [k for k, v in enumerate(final.values()) if v[0][0] == 1]
    out = [o.reshape(-1) if k in one_axis else o for k, o in enumerate(out)]
    return (out[0][None], out[1][None], *out[2:])


def angles(places, head_size):
    half_size = head_size // 2
    frequency = jnp.power(THETA, -jnp.arange(half_size, dtype=F32) * (2.0 / head_size))
    phases = places.astype(F32)[:, None] * frequency[None, :]
    phases = jnp.concatenate([phases, phases], axis=-1)
    return (jnp.cos(phases), jnp.sin(phases))


def rotate(values, cosines, sines):
    half_size = values.shape[-1] // 2
    turned = jnp.concatenate([-values[..., half_size:], values[..., :half_size]], axis=-1)
    return values * cosines + turned * sines


def rotate_back(upstream, cosines, sines):
    half_size = upstream.shape[-1] // 2
    scaled = upstream * sines
    turned = jnp.concatenate([scaled[..., half_size:], -scaled[..., :half_size]], axis=-1)
    return upstream * cosines + turned


def dot(a, b):
    return jnp.dot(a, b, preferred_element_type=F32)


def local_of(mesh):
    seqs, ranks = mesh.shape["seq"], mesh.shape["ctx"]
    devices = seqs * ranks
    axes = ("seq", "ctx")

    def spread(shard, heads):
        rows, columns = shard.shape
        if heads and heads < ranks:
            blocks = shard.reshape(rows, heads, 1, columns // heads)
            blocks = jnp.broadcast_to(blocks, (rows, heads, ranks // heads, columns // heads))
            return blocks.reshape(rows, ranks, columns // heads)
        return shard.reshape(rows, ranks, columns // ranks)

    def fold(blocks, heads):
        rows, count, width = blocks.shape
        if heads and heads < ranks:
            return blocks.reshape(rows, heads, count // heads, width).sum(2).reshape(rows, heads * width)
        return blocks.reshape(rows, count * width)

    forth = [(seqs * r + j, j * ranks + r) for r in range(ranks) for j in range(seqs)]
    back = [(b, a) for a, b in forth]

    def local(
        hidden_states, positions, gain_first, weight_query, key_weight_matrix, value_weight_matrix,
        gain_query, gain_key, weight_output, gain_second, weight_gate, weight_up, weight_down,
        output_cotangent,
    ):
        tokens = hidden_states.shape[1]
        length = positions.shape[1]
        size = HEAD_DIMENSION
        group = QUERY_HEAD_COUNT // KEY_VALUE_HEADS
        my_q = QUERY_HEAD_COUNT // ranks
        my_k = max(1, KEY_VALUE_HEADS // ranks)
        scale = size ** (-0.5)
        places = positions[0]
        cosines, sines = angles(places, size)
        cosines, sines = cosines[:, None, :], sines[:, None, :]

        gains = jnp.concatenate([gain_first, gain_second, gain_query, gain_key])
        gains = lax.all_gather(gains, axes, axis=0).astype(F32)
        n1, n2, n3, n4 = (g.shape[0] for g in (gain_first, gain_second, gain_query, gain_key))
        first_scale = gains[:, :n1].reshape(-1)
        second_scale = gains[:, n1 : n1 + n2].reshape(-1)
        query_scale = gains[:, n1 + n2 : n1 + n2 + n3].reshape(-1)
        key_scale = gains[:, n1 + n2 + n3 :].reshape(-1)

        column_weights = jnp.concatenate(
            [
                spread(weight_query, 0),
                spread(key_weight_matrix, KEY_VALUE_HEADS),
                spread(value_weight_matrix, KEY_VALUE_HEADS),
                spread(weight_gate, 0),
                spread(weight_up, 0),
            ],
            axis=2,
        )
        column_weights = lax.all_to_all(column_weights, "ctx", split_axis=1, concat_axis=0, tiled=True)
        column_weights = lax.all_gather(column_weights[:, 0], "seq", axis=0, tiled=True)
        row_weights = jnp.concatenate([weight_output, weight_down], axis=0)
        row_weights = lax.all_gather(lax.ppermute(row_weights, axes, forth), "seq", axis=0)
        o_rows, d_rows = weight_output.shape[0], weight_down.shape[0]
        width = weight_output.shape[1]
        w_o = row_weights[:, :o_rows].reshape(-1, width)
        w_d = row_weights[:, o_rows:].reshape(-1, width)
        units = w_d.shape[0]
        attn_columns = (my_q + 2 * my_k) * size
        w_qkv = column_weights[:, :attn_columns]
        w_gu = column_weights[:, attn_columns:]

        x = lax.all_gather(hidden_states[0], "ctx", axis=0, tiled=True).astype(F32)
        g_low = lax.all_gather(output_cotangent[0], "ctx", axis=0, tiled=True)
        first_inverse = inverse_root(x)
        h1 = (x * first_inverse * first_scale).astype(BF)
        qkv = dot(h1, w_qkv)
        q_lin = qkv[:, : my_q * size].reshape(length, my_q, size)
        k_lin = qkv[:, my_q * size : (my_q + my_k) * size].reshape(length, my_k, size)
        v = qkv[:, (my_q + my_k) * size :].astype(BF).reshape(length, my_k, size)
        rq, rk = inverse_root(q_lin), inverse_root(k_lin)
        nq, nk = q_lin * rq, k_lin * rk
        qr = rotate(nq * query_scale, cosines, sines).astype(BF)
        kr = rotate(nk * key_scale, cosines, sines).astype(BF)
        mask = places[None, :] <= places[:, None]

        def scores(h):
            e = lax.dot_general(
                qr[:, h], kr[:, h // group], (((1,), (1,)), ((), ())), preferred_element_type=F32
            )
            return jnp.where(mask, e * scale, NEGATIVE)

        outs, probs = [], []
        for h in range(my_q):
            e = scores(h)
            p = jnp.exp(e - jnp.max(e, axis=-1, keepdims=True))
            p = p / jnp.sum(p, axis=-1, keepdims=True)
            probs.append(p)
            outs.append(dot(p.astype(BF), v[:, h // group]))
        o = jnp.concatenate(outs, axis=1).astype(BF)

        def scatter(part):
            return lax.psum_scatter(part.astype(BF), "ctx", scatter_dimension=0, tiled=True).astype(F32)

        x_own = hidden_states[0].astype(F32)
        y1 = x_own + scatter(dot(o, w_o))
        r2 = inverse_root(y1)
        second_normed = y1 * r2
        h2 = lax.all_gather((second_normed * second_scale).astype(BF), "ctx", axis=0, tiled=True)
        gu = dot(h2, w_gu)
        gate, up = gu[:, :units], gu[:, units:]
        sig = jax.nn.sigmoid(gate)
        silu = gate * sig
        act = (silu * up).astype(BF)
        layer_output = (y1 + scatter(dot(act, w_d))).astype(BF)

        d_act = dot(g_low, w_d.T)
        d_gate = (d_act * up * sig * (1.0 + gate * (1.0 - sig))).astype(BF)
        d_up = (d_act * silu).astype(BF)
        d_gu = jnp.concatenate([d_gate, d_up], axis=1)
        d_h2 = scatter(dot(d_gu, w_gu.T))
        second_term = jnp.sum(d_h2 * second_normed, axis=0)
        d_y1 = output_cotangent[0].astype(F32) + norm_backward(d_h2 * second_scale, second_normed, r2)
        d_y1_low = lax.all_gather(d_y1.astype(BF), "ctx", axis=0, tiled=True)
        d_o = dot(d_y1_low, w_o.T).astype(BF).reshape(length, my_q, size)

        d_q, d_k, d_v = [], [0.0] * my_k, [0.0] * my_k
        for h in range(my_q):
            p = probs[h]
            dp = lax.dot_general(
                d_o[:, h], v[:, h // group], (((1,), (1,)), ((), ())), preferred_element_type=F32
            )
            row = jnp.sum(p * dp, axis=-1, keepdims=True)
            de = (p * (dp - row) * scale).astype(BF)
            d_q.append(dot(de, kr[:, h // group]))
            d_k[h // group] += dot(de.T, qr[:, h])
            d_v[h // group] += dot(p.astype(BF).T, d_o[:, h])
        d_q, d_k, d_v = jnp.stack(d_q, 1), jnp.stack(d_k, 1), jnp.stack(d_v, 1)
        d_gq, d_gk = rotate_back(d_q, cosines, sines), rotate_back(d_k, cosines, sines)
        query_term = jnp.sum(d_gq * nq, axis=(0, 1))
        key_term = jnp.sum(d_gk * nk, axis=(0, 1))
        d_qlin = norm_backward(d_gq * query_scale, nq, rq).reshape(length, -1)
        d_klin = norm_backward(d_gk * key_scale, nk, rk).reshape(length, -1)
        d_qkv = jnp.concatenate([d_qlin, d_klin, d_v.reshape(length, -1)], axis=1).astype(BF)
        d_h1 = scatter(dot(d_qkv, w_qkv.T))
        r1 = inverse_root(x_own)
        first_normed = x_own * r1
        first_term = jnp.sum(d_h1 * first_normed, axis=0)
        hidden_gradient = d_y1 + norm_backward(d_h1 * first_scale, first_normed, r1)

        def rows_sum(part):
            part = lax.psum_scatter(part.astype(BF), "seq", scatter_dimension=0, tiled=True)
            return lax.ppermute(part, axes, back).astype(F32)

        delta_rows = jnp.concatenate(
            [dot(o.T, d_y1_low).reshape(seqs, o_rows, width), dot(act.T, g_low).reshape(seqs, d_rows, width)],
            axis=1,
        ).reshape(-1, width)
        delta_rows = rows_sum(delta_rows)
        delta_columns = jnp.concatenate([dot(h1.T, d_qkv), dot(h2.T, d_gu)], axis=1).astype(BF)
        delta_columns = lax.psum_scatter(delta_columns, "seq", scatter_dimension=0, tiled=True)
        own = delta_columns.shape[0] // ranks
        delta_columns = lax.all_to_all(
            delta_columns.reshape(ranks, own, -1), "ctx", split_axis=0, concat_axis=0, tiled=True
        )
        delta_columns = jnp.moveaxis(delta_columns, 0, 1).astype(F32)
        cuts = [my_q * size, (my_q + my_k) * size, (my_q + 2 * my_k) * size, attn_columns + units]
        parts = jnp.split(delta_columns, cuts, axis=2)
        delta_query = fold(parts[0], 0)
        delta_key = fold(parts[1], KEY_VALUE_HEADS)
        delta_value = fold(parts[2], KEY_VALUE_HEADS)
        delta_gate, delta_up = fold(parts[3], 0), fold(parts[4], 0)

        terms = lax.psum(jnp.concatenate([first_term, second_term, query_term, key_term]), axes)
        me = lax.axis_index("seq") * ranks + lax.axis_index("ctx")
        w = width

        def mine(start, n):
            return lax.dynamic_slice_in_dim(terms, start + me * n, n)

        return (
            layer_output[None],
            hidden_gradient[None],
            mine(0, n1),
            delta_query,
            delta_key,
            delta_value,
            mine(2 * w, n3),
            mine(2 * w + size, n4),
            delta_rows[:o_rows],
            mine(w, n2),
            delta_gate,
            delta_up,
            delta_rows[o_rows:],
        )

    return local


def solution(mesh):
    token = P("seq", "ctx", None)
    flat = P(("seq", "ctx"))
    rows = P(("seq", "ctx"), None)
    general = local_of(mesh)

    def body(*args):
        tokens, length = args[0].shape[1], args[1].shape[1]
        fits = (
            mesh.shape["ctx"] == KEY_VALUE_HEADS == 8
            and mesh.shape["seq"] == 4
            and length <= 1024
            and length % BLOCK == 0
            and tokens % RUN == 0
            and HEAD_DIMENSION % (mesh.shape["seq"] * mesh.shape["ctx"]) == 0
        )
        return fused_layer(mesh, args) if fits else general(*args)

    return jax.shard_map(
        body,
        mesh=mesh,
        in_specs=(token, P("seq", None), flat, rows, rows, rows, flat, flat, rows, flat, rows, rows, rows, token),
        out_specs=(token, token, flat, rows, rows, rows, flat, flat, rows, flat, rows, rows, rows),
        check_vma=False,
    )
```

```python
import types

import jax
import jax.numpy as jnp
import numpy as np
from jax import lax
from jax.experimental import pallas as pl
from jax.experimental.pallas import tpu as pltpu
from jax.sharding import PartitionSpec as P

QUERY_HEAD_COUNT = 16
KEY_VALUE_HEADS = 8
HEAD_DIMENSION = 128

EPS = 1e-06
THETA = 1000000.0
NEGATIVE = -1e30
BF = jnp.bfloat16
F32 = jnp.float32
MESH = pl.DeviceIdType.MESH
RUN = 64
BLOCK = 256


def nn(a, b):
    return jnp.dot(a, b, preferred_element_type=F32)


def nt(a, b):
    return lax.dot_general(a, b, (((1,), (1,)), ((), ())), preferred_element_type=F32)


def tn(a, b):
    return lax.dot_general(a, b, (((0,), (0,)), ((), ())), preferred_element_type=F32)


def loop(low, high, body):
    def step(i, carry):
        body(i)
        return carry

    lax.fori_loop(low, high, step, 0)


def rows_of(start, size):
    return pl.ds(pl.multiple_of(start, size), size)


def inverse_root(values):
    return lax.rsqrt(jnp.mean(values * values, axis=-1, keepdims=True) + EPS)


def norm_backward(normed_grad, normed, inverse):
    return inverse * (normed_grad - normed * jnp.mean(normed_grad * normed, axis=-1, keepdims=True))


def layer_kernel(dims, refs):
    S, C, T, L, D = dims.S, dims.C, dims.T, dims.L, dims.D
    H, RW, OR, DR, AC, U = dims.H, dims.RW, dims.OR, dims.DR, dims.AC, dims.U
    HD = HEAD_DIMENSION
    PR = C * RW
    NR = L // RUN
    NB = L // BLOCK
    CH = C // 2
    scale = HD ** (-0.5)
    r = refs
    s = lax.axis_index("seq")
    c = lax.axis_index("ctx")
    chip = lax.div(c, 2)
    core = lax.rem(c, 2)
    chip_y, chip_x = lax.div(chip, 2), lax.rem(chip, 2)
    sibling = chip * 2 + (1 - core)
    def partner(i):
        x = lax.rem(chip_x + lax.rem(i, 2), 2)
        y = lax.rem(chip_y + lax.div(i, 2), 2)
        return y * 2 + x

    def remote(src, dst, send, recv, **where):
        return pltpu.make_async_remote_copy(
            src_ref=src, dst_ref=dst, send_sem=send, recv_sem=recv, device_id=where, device_id_type=MESH
        )

    def local(src, dst, sem):
        return pltpu.make_async_copy(src, dst, sem)

    def arrived(dst, sem):
        pltpu.make_async_copy(dst, dst, sem).wait()

    def left(elements, sem):
        arrived(r.h2_all.at[pl.ds(0, elements // D)], sem)

    barrier = pltpu.get_barrier_semaphore()

    def hello(**where):
        pl.semaphore_signal(barrier, inc=1, device_id=where, device_id_type=MESH)

    loop(1, C, lambda i: hello(ctx=lax.rem(c + i, C)))
    loop(1, S, lambda i: hello(seq=lax.rem(s + i, S)))

    pl.semaphore_wait(barrier, C - 1 + S - 1)

    def runs_of(b):
        return pl.ds(b * (BLOCK // RUN), BLOCK // RUN)

    def own_x():
        return r.x_all[pl.ds(c * (T // RUN), T // RUN)].reshape(T, D).astype(F32)

    X, G, H2, DY = 0, 1, 2, 3
    whole = {X: r.x_all, G: r.g_all, H2: r.h2_all, DY: r.dy_all}

    def block(kind, j):
        if kind == X:
            return whole[kind].at[pl.ds(j * (T // RUN), T // RUN)]
        return whole[kind].at[rows_of(j * T, T)]

    def half(ref, k):
        part = pl.ds(k * (D // 2), D // 2)
        return ref.at[:, :, part] if len(ref.shape) == 3 else ref.at[:, part]

    def gather_send(kind, src):
        for i in (1, 2):
            remote(src, block(kind, c), r.ag_send.at[kind], r.ag_recv.at[kind, c],
                   ctx=partner(i) * 2 + core).start()
        remote(src, block(kind, c), r.ag_send.at[kind], r.ag_recv.at[kind, c], ctx=sibling).start()

    def gather_relay(kind, i):
        j = partner(i) * 2 + core
        arrived(block(kind, j), r.ag_recv.at[kind, j])

        @pl.when(i == 1)
        def _():
            part = half(block(kind, j), 0)
            remote(part, part, r.ag_send.at[kind], r.ag_recv.at[kind, j], ctx=partner(2) * 2 + core).start()

        @pl.when(i == 2)
        def _():
            part = half(block(kind, j), 1)
            remote(part, part, r.ag_send.at[kind], r.ag_recv.at[kind, j], ctx=partner(1) * 2 + core).start()

        remote(block(kind, j), block(kind, j), r.ag_send.at[kind], r.ag_recv.at[kind, j],
               ctx=sibling).start()

    def gather_other(kind, i):
        j = partner(i) * 2 + (1 - core)
        arrived(block(kind, j), r.ag_recv.at[kind, j])

    def gather_done(kind):
        left(7 * T * D, r.ag_send.at[kind])

    def scatter_pair(kind, i, partial):
        r.pair[i] = partial
        r.s1[i] = r.pair[i, rows_of((1 - core) * T, T), :].astype(BF)
        remote(r.s1.at[i], r.r1.at[1 if kind == 1 else 0, i], r.rs_send.at[kind],
               r.r1_recv.at[kind, i], ctx=sibling).start()

    def scatter_chip(kind, i):
        bank = 1 if kind == 1 else 0
        arrived(r.r1.at[bank, i], r.r1_recv.at[kind, i])
        mine = r.pair[i, rows_of(core * T, T), :] + r.r1[bank, i].astype(F32)
        r.s2[i] = mine.astype(BF)

        def to(k, slot, send, recv):
            remote(half(r.s2.at[i], k), half(r.r2.at[bank, slot], k), r.rs_send.at[kind],
                   r.r2_recv.at[kind, recv], ctx=partner(1 + k) * 2 + core).start()

        @pl.when(i == 1)
        def _():
            to(0, 0, CH, 0)

        @pl.when(i == 2)
        def _():
            to(1, 0, CH + 1, 1)

        @pl.when(i == 3)
        def _():
            to(0, 1, CH + 2, 2)
            to(1, 1, CH + 3, 3)

    def scatter(kind, partial):
        def go(k):
            i = jnp.where(k == 0, 3, jnp.where(k == 3, 0, k))
            scatter_pair(kind, i, partial(i))

            @pl.when(k > 0)
            def _():
                scatter_chip(kind, jnp.where(k == 1, 3, k - 1))

        loop(0, CH, go)

    def scatter_pairs(kind, partial):
        loop(0, CH, lambda i: scatter_pair(kind, i, partial(i)))

    def scatter_mid(kind):
        bank = 1 if kind == 1 else 0
        for k in (0, 1):
            i = 2 - k
            part = slice(k * (D // 2), (k + 1) * (D // 2))
            arrived(half(r.r2.at[bank, 1], k), r.r2_recv.at[kind, 2 + k])
            mine = r.pair[i, rows_of(core * T, T), part] + r.r1[bank, i, :, part].astype(F32)
            r.s3[:, part] = (mine + r.r2[bank, 1, :, part].astype(F32)).astype(BF)
            remote(half(r.s3, k), half(r.r2.at[bank, 2], k), r.rs_send.at[kind],
                   r.r2_recv.at[kind, 4 + k], ctx=partner(i) * 2 + core).start()

    def scatter_sum(kind):
        bank = 1 if kind == 1 else 0
        arrived(r.r1.at[bank, 0], r.r1_recv.at[kind, 0])
        for k in (0, 1):
            arrived(half(r.r2.at[bank, 0], k), r.r2_recv.at[kind, k])
            arrived(half(r.r2.at[bank, 2], k), r.r2_recv.at[kind, 4 + k])
        total = r.pair[0, rows_of(core * T, T), :] + r.r1[bank, 0].astype(F32)
        return total + r.r2[bank, 0].astype(F32) + r.r2[bank, 2].astype(F32)

    def scatter_done(kind):
        left(7 * T * D, r.rs_send.at[kind])

    QKV, GATE, UP, OUT, DOWN, QKV2 = 0, 1, 2, 3, 4, 5
    PH = PR // 2

    def plane(w, b):
        if w == QKV:
            return r.w_qkv.at[rows_of(b * PR, PH)]
        if w == QKV2:
            return r.w_qkv.at[rows_of(b * PR + PH, PH)]
        if w == GATE:
            return r.w_gu.at[rows_of(b * PR, PR), pl.ds(0, U)]
        if w == UP:
            return r.w_gu.at[rows_of(b * PR, PR), pl.ds(U, U)]
        if w == DOWN:
            return r.w_d.at[rows_of(b * DR, DR)]
        return r.z_o.at[b]

    def weight_start(w, src=None):
        src = plane(w, s) if src is None else src

        @pl.when(s < S - 1)
        def _():
            remote(src, plane(w, s), r.z_send.at[w], r.z_recv.at[w, s], seq=s + 1).start()

        @pl.when(s > 0)
        def _():
            remote(src, plane(w, s), r.z_send.at[w], r.z_recv.at[w, s], seq=s - 1).start()

    rows_ref = {OUT: (0, r.w_o, OR)}

    def deal(w, b, src=None):
        n, ref, size = rows_ref[w]
        src = plane(w, b) if src is None else src
        d = C * b + c
        rank, spot = lax.div(d, S), lax.rem(d, S)
        dst = ref.at[rows_of(spot * size, size)]

        @pl.when(rank != c)
        def _():
            remote(src, dst, r.m_send.at[n, b], r.m_recv.at[n], ctx=rank).start()

        @pl.when(rank == c)
        def _():
            local(src, dst, r.m_recv.at[n]).start()

    def deal_arrive(w):
        n, ref, size = rows_ref[w]
        arrived(ref, r.m_recv.at[n])

    def deal_done(w):
        n, ref, size = rows_ref[w]

        def go(b):
            @pl.when(lax.div(C * b + c, S) != c)
            def _():
                arrived(plane(w, 0), r.m_send.at[n, b])

        loop(0, S, go)

    def weight_hop(w, t):
        below, above = s - 1 - t, s + 1 + t

        @pl.when(below >= 0)
        def _():
            arrived(plane(w, below), r.z_recv.at[w, below])

            @pl.when(s < S - 1)
            def _():
                remote(plane(w, below), plane(w, below), r.z_send.at[w],
                       r.z_recv.at[w, below], seq=s + 1).start()

        @pl.when(above <= S - 1)
        def _():
            arrived(plane(w, above), r.z_recv.at[w, above])

            @pl.when(s > 0)
            def _():
                remote(plane(w, above), plane(w, above), r.z_send.at[w],
                       r.z_recv.at[w, above], seq=s - 1).start()

    inner = jnp.logical_and(s > 0, s < S - 1)

    def hop_inner(w, t):
        @pl.when(inner)
        def _():
            weight_hop(w, t)

    def hop_outer(w, t):
        @pl.when(jnp.logical_not(inner))
        def _():
            weight_hop(w, t)

    def deal_hop(w, t):
        below, above = s - 1 - t, s + 1 + t

        @pl.when(below >= 0)
        def _():
            deal(w, below)

        @pl.when(above <= S - 1)
        def _():
            deal(w, above)

    def weight_done(w):
        size = {QKV: PH * AC, QKV2: PH * AC, GATE: PR * U, UP: PR * U, OUT: OR * D, DOWN: DR * D}[w]

        @pl.when(inner)
        def _():
            left((S + 1) * size, r.z_send.at[w])

        @pl.when(jnp.logical_not(inner))
        def _():
            left(size, r.z_send.at[w])

    GU = GATE
    sent = {QKV: (r.g_q, PR), QKV2: (r.g_kv, PR), OUT: (r.h_o, OR), GU: (r.g_gu, PR), DOWN: (r.g_d, DR)}
    got = {QKV: r.t_q, QKV2: r.t_kv, OUT: r.t_o, GU: r.t_gu, DOWN: r.t_d}
    halfway = {QKV: r.c_q, QKV2: r.c_kv, OUT: r.c_o, GU: r.c_gu, DOWN: r.c_d}
    summed = {QKV: r.u_q, QKV2: r.u_kv, OUT: r.u_o, GU: r.u_gu, DOWN: r.u_d}
    side = jnp.where(s >= 2, 1, 0)

    def grad_rows(w, p):
        ref, size = sent[w]
        return ref.at[rows_of(p * size, size)]

    def grad_order(i):
        return jnp.where(s < 2, lax.rem(3 - i + s, S), lax.rem(i + (3 - s) * 3, S))

    def grad_direct(w, p):
        remote(grad_rows(w, p), got[w].at[side], r.gz_send.at[w], r.gz_recv.at[w, side], seq=p).start()

    def grad_out(w, p):
        far_up = jnp.logical_and(s == 0, p >= 2)
        far_down = jnp.logical_and(s == S - 1, p <= 1)
        later = jnp.logical_or(
            jnp.logical_and(s == 1, p >= 2), jnp.logical_and(s == 2, p <= 1)
        )

        @pl.when(far_up)
        def _():
            remote(grad_rows(w, p), halfway[w].at[p - 2], r.gz_send.at[w], r.gc_recv.at[w, p - 2],
                   seq=1).start()

        @pl.when(far_down)
        def _():
            remote(grad_rows(w, p), halfway[w].at[p], r.gz_send.at[w], r.gc_recv.at[w, p], seq=2).start()

        others = jnp.logical_or(jnp.logical_or(far_up, far_down), jnp.logical_or(later, p == s))

        @pl.when(jnp.logical_not(others))
        def _():
            grad_direct(w, p)

    def grad_combine(w, k):
        @pl.when(jnp.logical_or(s == 1, s == 2))
        def _():
            p = jnp.where(s == 1, 3 - k, k)
            slot = jnp.where(s == 1, 1 - k, k)
            ref, size = sent[w]
            rows = rows_of(p * size, size)
            arrived(halfway[w].at[slot], r.gc_recv.at[w, slot])
            ref[rows, :] = (ref[rows, :].astype(F32) + halfway[w][slot].astype(F32)).astype(BF)
            grad_direct(w, p)

    def grad_sum(w):
        ref, size = sent[w]
        total = ref[rows_of(s * size, size), :].astype(F32)
        for i in range(2):
            arrived(got[w].at[i], r.gz_recv.at[w, i])
            total = total + got[w][i].astype(F32)
        summed[w][...] = total.astype(BF)

    def grad_done(w):
        size = {QKV: PR * H * HD, QKV2: PR * 2 * HD, GU: 2 * PR * U, OUT: OR * D, DOWN: DR * D}[w]
        left((S - 1) * size, r.gz_send.at[w])

    final = {QKV: r.f_q, QKV2: r.f_kv, GU: r.f_gu}

    def columns_send(n, w):
        def go(i):
            j = lax.rem(c + i, C)
            remote(summed[w].at[rows_of(j * RW, RW)], final[w].at[c], r.gp_send.at[n],
                   r.gp_recv.at[n], ctx=j).start()

        loop(1, C, go)
        final[w][c] = summed[w][rows_of(c * RW, RW), :]

    def columns_arrive(n, w):
        arrived(final[w].at[pl.ds(0, C - 1)], r.gp_recv.at[n])

    def columns_done(n, w):
        arrived(final[w].at[pl.ds(0, C - 1)], r.gp_send.at[n])

    undealt = {OUT: (0, r.g_o, r.h_o, OR)}

    def undeal(w):
        n, src, dst, size = undealt[w]

        def go(j):
            d = S * c + j
            b, place = lax.div(d, C), lax.rem(d, C)
            here, there = src.at[rows_of(j * size, size)], dst.at[rows_of(b * size, size)]

            @pl.when(place != c)
            def _():
                remote(here, there, r.u_send.at[n, j], r.u_recv.at[n], ctx=place).start()

            @pl.when(place == c)
            def _():
                local(here, there, r.u_recv.at[n]).start()

        loop(0, S, go)

    def undeal_arrive(w):
        n, src, dst, size = undealt[w]
        arrived(dst, r.u_recv.at[n])

    def undeal_done(w):
        n, src, dst, size = undealt[w]

        def go(j):
            @pl.when(lax.rem(S * c + j, C) != c)
            def _():
                arrived(src.at[pl.ds(0, size)], r.u_send.at[n, j])

        loop(0, S, go)

    gains_own = r.gains_all.at[c]
    gain_copy = local(r.gains_in, gains_own, r.gain_recv.at[S])
    gain_copy.start()

    def gain_go(i):
        remote(r.gains_in, gains_own, r.gain_send.at[0], r.gain_recv.at[S],
               ctx=lax.rem(c + i, C)).start()

    loop(1, C, gain_go)

    def qkv_piece(j):
        return (
            (r.wq_in.at[:, rows_of(j * H * HD, H * HD)], slice(0, H * HD)),
            (r.wk_in.at[:, rows_of(j * HD, HD)], slice(H * HD, (H + 1) * HD)),
            (r.wv_in.at[:, rows_of(j * HD, HD)], slice((H + 1) * HD, (H + 2) * HD)),
        )

    def gu_piece(j):
        return ((r.gu_own.at[j], slice(0, 2 * U)),)

    def gu_order(k, ref):
        for j in range(C):
            parts = [ref[:, (C * b + j) * DR : (C * b + j + 1) * DR] for b in range(S)]
            r.gu_own[j, :, k * U : (k + 1) * U] = jnp.concatenate(parts, axis=1)

    columns_of = {QKV: r.w_qkv, GU: r.w_gu}

    def spread(n, w, piece):
        ref = columns_of[w]
        own = rows_of(s * PR + c * RW, RW)

        def go(i):
            j = lax.rem(c + i, C)
            for src, columns in piece(j):
                remote(src, ref.at[own, columns], r.w_send.at[n], r.w_recv.at[n], ctx=j).start()

        loop(1, C, go)
        for src, columns in piece(c):
            local(src, ref.at[own, columns], r.w_recv.at[n]).start()

    def spread_arrive(n, w):
        arrived(columns_of[w].at[rows_of(s * PR, PR)], r.w_recv.at[n])

    def spread_done(n, w):
        arrived(columns_of[w].at[pl.ds(0, (C - 1) * RW)], r.w_send.at[n])

    weight_start(OUT, r.wo_in)
    spread(0, QKV, qkv_piece)
    local(r.x_in, block(X, c), r.local_sem.at[0]).start()
    local(r.table_in, r.table, r.local_sem.at[1]).start()
    local(r.wg_in, r.wg_own, r.local_sem.at[4]).start()
    local(r.wu_in, r.wu_own, r.local_sem.at[5]).start()
    gather_send(X, r.x_in)
    arrived(r.wg_own, r.local_sem.at[4])
    gu_order(0, r.wg_own)
    arrived(r.wu_own, r.local_sem.at[5])
    gu_order(1, r.wu_own)
    weight_hop(OUT, 0)
    spread_arrive(0, QKV)
    weight_start(QKV)
    weight_start(QKV2)
    arrived(r.gains_all, r.gain_recv.at[S])
    r.gains_z[s] = jnp.sum(r.gains_all[...], axis=1)

    def gain_far(i):
        remote(r.gains_z.at[s], r.gains_z.at[s], r.gain_send.at[1], r.gain_recv.at[s],
               seq=lax.rem(s + i, S)).start()

    loop(1, S, gain_far)

    arrived(r.table, r.local_sem.at[1])

    def tables(b):
        rows = rows_of(b * T, T)
        both = r.table[rows, :]
        other = pltpu.roll(both, HD // 2, 1)
        first = lax.broadcasted_iota(jnp.int32, (T, HD), 1) < HD // 2
        r.cosine[rows, :] = jnp.where(first, both, other)
        r.sine[rows, :] = jnp.where(first, -other, both)

    loop(0, L // T, tables)
    arrived(block(X, c), r.local_sem.at[0])
    gather_relay(X, 1)
    gather_relay(X, 2)
    weight_hop(QKV, 0)
    weight_hop(QKV2, 0)
    gather_relay(X, 3)
    spread(1, GU, gu_piece)
    deal(OUT, s, r.wo_in)
    deal_hop(OUT, 0)
    local(r.g_in, block(G, c), r.local_sem.at[2]).start()
    gather_send(G, r.g_in)

    def gain_block(i):
        p = lax.rem(s + i, S)
        arrived(r.gains_z.at[p], r.gain_recv.at[p])

    loop(1, S, gain_block)
    gains = r.gains_z[...].reshape(S * C, HD).astype(BF)

    def gain_vector(offset, count):
        width = count * S * C
        shift = count.bit_length() - 1
        column = lax.broadcasted_iota(jnp.int32, (HD, width), 1)
        row = lax.broadcasted_iota(jnp.int32, (HD, width), 0)
        pick = jnp.where(row == offset + (column & (count - 1)), 1.0, 0.0).astype(BF)
        spread_out = nn(gains, pick)
        owner = lax.broadcasted_iota(jnp.int32, (S * C, width), 0)
        place = lax.broadcasted_iota(jnp.int32, (S * C, width), 1) >> shift
        return jnp.sum(jnp.where(owner == place, spread_out, 0.0), axis=0, keepdims=True)

    n1 = D // (S * C)
    n3 = HD // (S * C)
    r.gain1[...] = gain_vector(0, n1)
    r.gain2[...] = gain_vector(n1, n1)
    r.gainq[...] = gain_vector(2 * n1, n3)
    r.gaink[...] = gain_vector(2 * n1 + n3, n3)

    arrived(block(X, sibling), r.ag_recv.at[X, sibling])
    loop(1, CH, lambda i: gather_other(X, i))

    def first_norm(k):
        x = r.x_all[r.order[1, k]].astype(F32)
        r.h1[rows_of(k * RUN, RUN), :] = (x * inverse_root(x) * r.gain1[...]).astype(BF)

    loop(0, NR, first_norm)
    weight_hop(QKV, 1)
    weight_hop(QKV2, 1)
    weight_hop(OUT, 1)
    spread_arrive(1, GU)
    weight_start(GATE)
    local(r.wd_in, plane(DOWN, s), r.local_sem.at[3]).start()
    deal_hop(OUT, 1)
    weight_hop(QKV, 2)
    weight_hop(QKV2, 2)

    def rotate(u, rows):
        return u * r.cosine[rows, :] + pltpu.roll(u, HD // 2, 1) * r.sine[rows, :]

    def rotate_back(u, rows):
        return u * r.cosine[rows, :] - pltpu.roll(u, HD // 2, 1) * r.sine[rows, :]

    def project(b):
        rows = rows_of(b * BLOCK, BLOCK)
        acc = nn(r.h1[rows, :], r.w_qkv[...])
        for h in range(H):
            u = acc[:, h * HD : (h + 1) * HD]
            r.q_lin[h, rows, :] = u
            r.q_rot[h, rows, :] = rotate(u * inverse_root(u) * r.gainq[...], rows).astype(BF)
        u = acc[:, H * HD : (H + 1) * HD]
        r.k_lin[rows, :] = u
        k = rotate(u * inverse_root(u) * r.gaink[...], rows)
        r.k_rot[rows, :] = k.astype(BF)
        r.k_t[:, rows] = k.T.astype(BF)
        v = acc[:, (H + 1) * HD :]
        r.v[rows, :] = v.astype(BF)
        r.v_t[:, rows] = v.T.astype(BF)

    loop(0, NB, project)
    weight_hop(OUT, 2)
    deal_hop(OUT, 2)

    def attend(qb):
        @pl.when(qb == NB - 2)
        def _():
            gather_relay(G, 1)
            gather_relay(G, 2)

        @pl.when(qb == NB - 1)
        def _():
            hop_inner(GATE, 0)
            weight_start(UP)

        cols = rows_of(qb * BLOCK, BLOCK)

        def keys(kb, carry):
            rows = rows_of(kb * BLOCK, BLOCK)
            key = r.k_rot[rows, :]
            value_t = r.v_t[:, rows]
            ahead = lax.broadcasted_iota(jnp.int32, (BLOCK, BLOCK), 0) - lax.broadcasted_iota(
                jnp.int32, (BLOCK, BLOCK), 1
            )
            allowed = ahead <= (qb - kb) * BLOCK
            out = []
            for h in range(H):
                acc, total = carry[2 * h], carry[2 * h + 1]
                e = jnp.exp(nt(key, r.q_rot[h, cols, :]) * scale)
                e = jnp.where(allowed, e, 0.0)
                low = e.astype(BF)
                r.e[h, rows, cols] = low
                out += [acc + nn(value_t, low), total + jnp.sum(e, axis=0, keepdims=True)]
            return tuple(out)

        zero = (jnp.zeros((HD, BLOCK), F32), jnp.zeros((1, BLOCK), F32)) * H
        done = lax.fori_loop(0, qb + 1, keys, zero)
        for h in range(H):
            inverse = 1.0 / done[2 * h + 1]
            o = done[2 * h] * inverse
            r.l_inv[h, :, cols] = jnp.broadcast_to(inverse, (8, BLOCK))
            r.o_t[h, :, cols] = o
            r.o_sorted[runs_of(qb), :, h * HD : (h + 1) * HD] = o.T.astype(BF).reshape(-1, RUN, HD)

    loop(0, NB, attend)
    def unsort(i):
        r.o[rows_of(i * RUN, RUN), :] = r.o_sorted[r.order[0, i]]

    loop(0, NR, unsort)

    deal_arrive(OUT)
    scatter(0, lambda i: nn(r.o[rows_of(partner(i) * 2 * T, 2 * T), :], r.w_o[...]))
    hop_inner(GATE, 1)
    gather_relay(G, 3)
    scatter_mid(0)
    hop_inner(UP, 0)
    y1 = own_x() + scatter_sum(0)
    r.y1[...] = y1
    h2_own = (y1 * inverse_root(y1) * r.gain2[...]).astype(BF)
    r.h2_all[rows_of(c * T, T), :] = h2_own
    gather_send(H2, block(H2, c))

    hop_inner(UP, 1)
    weight_start(DOWN, r.wd_in)
    hop_inner(GATE, 2)
    for w in (GATE, UP):
        for t in range(S - 1):
            hop_outer(w, t)
    hop_inner(UP, 2)
    arrived(block(H2, sibling), r.ag_recv.at[H2, sibling])

    def feed(i):
        @pl.when(i == 1)
        def _():
            gather_relay(H2, 1)
            gather_relay(H2, 2)
            hop_inner(DOWN, 0)

        @pl.when(i == 3)
        def _():
            gather_relay(H2, 3)
            hop_inner(DOWN, 1)

        @pl.when(i > 0)
        def _():
            gather_other(H2, i)

        rows = rows_of(partner(i) * 2 * T, 2 * T)
        both = nn(r.h2_all[rows, :], r.w_gu[...])
        gate, up = both[:, :U], both[:, U:]
        sig = 1.0 / (1.0 + jnp.exp(-gate))
        silu = gate * sig
        r.act[rows, :] = (silu * up).astype(BF)
        r.slope[rows, :] = up * sig * (1.0 + gate * (1.0 - sig))
        r.silu[rows, :] = silu

    loop(0, CH, feed)
    arrived(block(G, c), r.local_sem.at[2])
    arrived(block(G, sibling), r.ag_recv.at[G, sibling])
    loop(1, CH, lambda i: gather_other(G, i))

    def down_grad(m):
        cols = rows_of(m * HD, HD)
        r.g_d[cols, :] = tn(r.act[:, cols], r.g_all[...]).astype(BF)

    loop(0, U // HD, down_grad)
    loop(0, S, lambda i: grad_out(DOWN, grad_order(i)))
    hop_outer(DOWN, 0)
    hop_outer(DOWN, 1)
    weight_hop(DOWN, 2)
    arrived(plane(DOWN, s), r.local_sem.at[3])
    scatter_done(0)

    def feed_back(i):
        rows = rows_of(partner(i) * 2 * T, 2 * T)
        d_act = nt(r.g_all[rows, :], r.w_d[...])
        r.d_gu[rows, :U] = (d_act * r.slope[rows, :]).astype(BF)
        r.d_gu[rows, U:] = (d_act * r.silu[rows, :]).astype(BF)
        return nt(r.d_gu[rows, :], r.w_gu[...])

    scatter(2, feed_back)

    def gu_grad(i):
        p = grad_order(i)
        cols = rows_of(p * PR, PR)
        r.g_gu[cols, :] = tn(r.h2_all[:, cols], r.d_gu[...]).astype(BF)
        grad_out(GU, p)

    loop(0, S, gu_grad)
    scatter_mid(2)
    grad_combine(DOWN, 0)
    d_h2 = scatter_sum(2)
    y1 = r.y1[...]
    r2 = inverse_root(y1)
    normed = y1 * r2
    term2 = jnp.sum(d_h2 * normed, axis=0, keepdims=True)
    d_y1 = r.g_all[rows_of(c * T, T), :].astype(F32) + norm_backward(d_h2 * r.gain2[...], normed, r2)
    r.d_y1[...] = d_y1
    r.dy_all[rows_of(c * T, T), :] = d_y1.astype(BF)
    gather_send(DY, block(DY, c))
    scatter_done(2)
    scatter_pairs(1, lambda i: nn(r.act[rows_of(partner(i) * 2 * T, 2 * T), :], r.w_d[...]))
    WT = D // HD
    for k in range(WT):
        r.terms[WT + k : WT + k + 1, :] = term2[:, k * HD : (k + 1) * HD]

    arrived(block(DY, sibling), r.ag_recv.at[DY, sibling])

    def out_grad(i):
        @pl.when(i == 1)
        def _():
            gather_relay(DY, 1)
            gather_relay(DY, 2)

        @pl.when(i == 3)
        def _():
            gather_relay(DY, 3)

        @pl.when(i > 0)
        def _():
            gather_other(DY, i)

        rows = rows_of(partner(i) * 2 * T, 2 * T)
        d_o = nt(r.dy_all[rows, :], r.w_o[...]).astype(BF)
        r.d_o[pl.ds(partner(i) * (2 * T // RUN), 2 * T // RUN)] = d_o.reshape(-1, RUN, H * HD)

    loop(0, CH, out_grad)

    def out_weight(m):
        cols = rows_of(m * HD, HD)
        r.g_o[cols, :] = tn(r.o[:, cols], r.dy_all[...]).astype(BF)

    loop(0, H * HD // HD, out_weight)
    undeal(OUT)
    for i in (3, 1, 2):
        scatter_chip(1, i)
    grad_combine(DOWN, 1)
    grad_combine(GU, 0)

    def sort(k):
        r.d_o_sorted[rows_of(k * RUN, RUN), :] = r.d_o[r.order[1, k]]

    loop(0, NR, sort)
    r.d_k[...] = jnp.zeros_like(r.d_k)
    r.d_v[...] = jnp.zeros_like(r.d_v)
    r.sums[...] = jnp.zeros_like(r.sums)

    def attend_back(qb):
        @pl.when(qb == NB - 1)
        def _():
            undeal_arrive(OUT)
            loop(0, S, lambda i: grad_out(OUT, grad_order(i)))

        cols = rows_of(qb * BLOCK, BLOCK)
        d_o_t, d_o_low, row, factor = [], [], [], []
        for h in range(H):
            t = r.d_o_sorted[cols, h * HD : (h + 1) * HD].astype(F32).T
            inverse = r.l_inv[h, 0:1, cols]
            row.append(jnp.sum(t * r.o_t[h, :, cols], axis=0, keepdims=True))
            factor.append(inverse * scale)
            r.do_t[h] = t.astype(BF)
            r.do_l[h] = (t * inverse).T.astype(BF)

        def keys(kb, carry):
            rows = rows_of(kb * BLOCK, BLOCK)
            value = r.v[rows, :]
            key_t = r.k_t[:, rows]
            out = []
            d_k = r.d_k[rows, :]
            d_v = r.d_v[rows, :]
            for h in range(H):
                e = r.e[h, rows, cols]
                dp = nn(value, r.do_t[h])
                de = (e.astype(F32) * ((dp - row[h]) * factor[h])).astype(BF)
                out.append(carry[h] + nn(key_t, de))
                d_k = d_k + nn(de, r.q_rot[h, cols, :])
                d_v = d_v + nn(e, r.do_l[h])
            r.d_k[rows, :] = d_k
            r.d_v[rows, :] = d_v
            return tuple(out)

        done = lax.fori_loop(0, qb + 1, keys, (jnp.zeros((HD, BLOCK), F32),) * H)
        for h in range(H):
            d_g = rotate_back(done[h].T, cols)
            u = r.q_lin[h, cols, :]
            inverse = inverse_root(u)
            normed = u * inverse
            r.sums[0:1, :] += jnp.sum(d_g * normed, axis=0, keepdims=True)
            d_lin = norm_backward(d_g * r.gainq[...], normed, inverse).astype(BF)
            r.d_qkv[runs_of(qb), :, h * HD : (h + 1) * HD] = d_lin.reshape(-1, RUN, HD)

    loop(0, NB, attend_back)

    def key_back(b):
        rows = rows_of(b * BLOCK, BLOCK)
        d_g = rotate_back(r.d_k[rows, :], rows)
        u = r.k_lin[rows, :]
        inverse = inverse_root(u)
        normed = u * inverse
        r.sums[1:2, :] += jnp.sum(d_g * normed, axis=0, keepdims=True)
        d_lin = norm_backward(d_g * r.gaink[...], normed, inverse).astype(BF)
        r.d_qkv[runs_of(b), :, H * HD : (H + 1) * HD] = d_lin.reshape(-1, RUN, HD)
        r.d_qkv[runs_of(b), :, (H + 1) * HD :] = r.d_v[rows, :].astype(BF).reshape(-1, RUN, HD)

    loop(0, NB, key_back)
    scatter_mid(1)

    def qkv_grad(i):
        p = grad_order(i)
        cols = rows_of(p * PR, PR)
        both = tn(r.h1[:, cols], r.d_qkv[...].reshape(L, AC)).astype(BF)
        r.g_q[cols, :] = both[:, : H * HD]
        r.g_kv[cols, :] = both[:, H * HD :]
        grad_out(QKV, p)

    loop(0, S, qkv_grad)
    loop(0, S, lambda i: grad_out(QKV2, grad_order(i)))
    grad_combine(GU, 1)
    r.y_out[...] = (r.y1[...] + scatter_sum(1)).astype(BF)
    local(r.y_out, r.layer_out, r.out_sem.at[0]).start()
    scatter_done(1)

    def in_chip(i):
        j = partner(i) * 2
        parts = []
        for k in range(2 * T // RUN):
            parts.append(r.d_qkv[r.order[0, j * (T // RUN) + k]])
        return nt(jnp.concatenate(parts, axis=0), r.w_qkv[...])

    scatter(3, in_chip)
    grad_combine(OUT, 0)
    scatter_mid(3)
    grad_combine(OUT, 1)
    grad_combine(QKV, 0)
    grad_sum(GU)
    columns_send(1, GU)
    grad_combine(QKV, 1)
    d_h1 = scatter_sum(3)
    x = own_x()
    r1 = inverse_root(x)
    normed = x * r1
    term1 = jnp.sum(d_h1 * normed, axis=0, keepdims=True)
    r.x_grad[...] = r.d_y1[...] + norm_backward(d_h1 * r.gain1[...], normed, r1)
    local(r.x_grad, r.hidden_grad, r.out_sem.at[1]).start()
    for k in range(WT):
        r.terms[k : k + 1, :] = term1[:, k * HD : (k + 1) * HD]
    r.terms[2 * WT : 2 * WT + 8, :] = r.sums[...]

    def terms_far(i):
        remote(r.terms, r.terms_z.at[s], r.t_send.at[0], r.t_recv.at[0],
               seq=lax.rem(s + i, S)).start()

    loop(1, S, terms_far)
    scatter_done(3)
    grad_combine(QKV2, 0)
    grad_sum(DOWN)
    local(r.u_d, r.down_out, r.out_sem.at[2]).start()
    grad_combine(QKV2, 1)
    grad_sum(OUT)
    local(r.u_o, r.o_out, r.out_sem.at[4]).start()
    columns_arrive(1, GU)
    local(r.f_gu, r.gu_out, r.out_sem.at[3]).start()
    grad_sum(QKV)
    columns_send(0, QKV)
    grad_sum(QKV2)
    columns_send(2, QKV2)
    total = r.terms[...]
    arrived(r.terms_z.at[pl.ds(0, S - 1)], r.t_recv.at[0])
    for i in range(1, S):
        total = total + r.terms_z[lax.rem(s + i, S)]
    r.terms_sum[...] = total

    def terms_near(i):
        remote(r.terms_sum, r.terms_p.at[c], r.t_send.at[1], r.t_recv.at[1],
               ctx=lax.rem(c + i, C)).start()

    loop(1, C, terms_near)

    columns_arrive(0, QKV)
    local(r.f_q, r.q_out, r.out_sem.at[5]).start()
    total = r.terms_sum[...]
    arrived(r.terms_p.at[pl.ds(0, C - 1)], r.t_recv.at[1])
    for i in range(1, C):
        total = total + r.terms_p[lax.rem(c + i, C)]
    r.terms_all[...] = total
    local(r.terms_all, r.terms_out, r.out_sem.at[6]).start()
    columns_arrive(2, QKV2)
    local(r.f_kv, r.kv_out, r.out_sem.at[7]).start()

    arrived(r.gains_all.at[pl.ds(0, C - 1)], r.gain_send.at[0])
    arrived(r.gains_z.at[pl.ds(0, S - 1)], r.gain_send.at[1])
    for kind in (X, G, H2, DY):
        gather_done(kind)
    spread_done(0, QKV)
    spread_done(1, GU)
    deal_done(OUT)
    undeal_done(OUT)
    for w in (QKV, QKV2, GATE, UP, OUT, DOWN):
        weight_done(w)
    for w in (QKV, QKV2, OUT, GU, DOWN):
        grad_done(w)
    columns_done(0, QKV)
    columns_done(2, QKV2)
    columns_done(1, GU)
    arrived(r.terms_z.at[pl.ds(0, S - 1)], r.t_send.at[0])
    arrived(r.terms_p.at[pl.ds(0, C - 1)], r.t_send.at[1])
    pairs = (
        (r.y_out, r.layer_out), (r.x_grad, r.hidden_grad), (r.u_d, r.down_out), (r.f_gu, r.gu_out),
        (r.u_o, r.o_out), (r.f_q, r.q_out), (r.terms_all, r.terms_out), (r.f_kv, r.kv_out),
    )
    for k, (src, dst) in enumerate(pairs):
        local(src, dst, r.out_sem.at[k]).wait()


def finish_kernel(dims, inputs, outputs, refs):
    S, C, D, H, U = dims.S, dims.C, dims.D, dims.H, dims.U
    HD = HEAD_DIMENSION
    r = refs
    me = lax.axis_index("seq") * C + lax.axis_index("ctx")

    def read(k):
        return pltpu.make_async_copy(r.far_in[k], r.near_in[k], r.in_sem.at[k])

    def write(src, k):
        return pltpu.make_async_copy(src, r.far_out[k], r.out_sem.at[k])

    source = dict(zip(inputs, r.near_in))
    target = dict(zip(outputs, r.near_out))
    i = types.SimpleNamespace(**source)
    o = types.SimpleNamespace(**target)
    for k in range(len(inputs)):
        read(k).start()
    read(0).wait()
    write(i.layer_out, 0).start()
    read(1).wait()
    write(i.hidden_grad, 1).start()
    read(2).wait()
    for j in range(C):
        o.delta_query[:, j * H * HD : (j + 1) * H * HD] = i.q_out[j].astype(F32)
    write(o.delta_query, 3).start()
    read(3).wait()
    for j in range(C):
        o.delta_key[:, j * HD : (j + 1) * HD] = i.kv_out[j, :, :HD].astype(F32)
        o.delta_value[:, j * HD : (j + 1) * HD] = i.kv_out[j, :, HD:].astype(F32)
    write(o.delta_key, 4).start()
    write(o.delta_value, 5).start()
    read(4).wait()
    o.delta_out[...] = i.o_out[...].astype(F32)
    write(o.delta_out, 8).start()
    read(5).wait()
    for k, ref in ((0, o.delta_gate), (1, o.delta_up)):
        for d in range(0, S * C, 4):
            parts = []
            for e in range(d, d + 4):
                first = k * U + (e // C) * dims.DR
                parts.append(i.gu_out[e % C, :, first : first + dims.DR].astype(F32))
            ref[:, d * dims.DR : (d + 4) * dims.DR] = jnp.concatenate(parts, axis=1)
        write(ref, 10 + k).start()
    read(6).wait()
    o.delta_down[...] = i.down_out[...].astype(F32)
    write(o.delta_down, 12).start()
    read(7).wait()

    def own(ref, first_row, count, k):
        start = me * count
        row = i.terms_out[pl.ds(first_row + lax.div(start, HD), 1), :]
        back = lax.rem(HD - lax.rem(start, HD), HD)
        ref[...] = pltpu.roll(jnp.broadcast_to(row, (8, HD)), back, 1)[0:1, :count]
        write(ref, k).start()

    n1, n3 = D // (S * C), HD // (S * C)
    own(o.change1, 0, n1, 2)
    own(o.change2, D // HD, n1, 9)
    own(o.changeq, 2 * (D // HD), n3, 6)
    own(o.changek, 2 * (D // HD) + 1, n3, 7)
    for k in range(len(outputs)):
        write(i.layer_out if k == 0 else i.hidden_grad if k == 1 else r.near_out[k], k).wait()


def fused_layer(mesh, args):
    (x, positions, gain1, wq, wk, wv, gainq, gaink, wo, gain2, wg, wu, wd, g) = args
    S, C = mesh.shape["seq"], mesh.shape["ctx"]
    T, D = x.shape[1:]
    L = positions.shape[1]
    HD = HEAD_DIMENSION
    H = QUERY_HEAD_COUNT // C
    RW, OR, DR = wq.shape[0], wo.shape[0], wd.shape[0]
    U = wg.shape[1] // C
    AC = (H + 2) * HD
    PR = C * RW
    CH = C // 2
    dims = types.SimpleNamespace(S=S, C=C, T=T, L=L, D=D, H=H, RW=RW, OR=OR, DR=DR, AC=AC, U=U)
    packed = jnp.concatenate([gain1, gain2, gainq, gaink]).astype(F32)
    packed = jnp.pad(packed[None, :], ((0, 7), (0, HD - packed.shape[0])))
    half = HD // 2
    frequency = np.power(THETA, -np.arange(half) * (2.0 / HD))
    phases = np.arange(L)[:, None] * frequency[None, :]
    table = jnp.asarray(np.concatenate([np.cos(phases), np.sin(phases)], axis=1), F32)
    TR = 2 * (D // HD) + 8
    run = positions[0, ::RUN] // RUN
    spot = jnp.arange(L // RUN, dtype=jnp.int32)
    place = jnp.sum(jnp.where(run[None, :] == spot[:, None], spot[None, :], 0), axis=1)
    order = jnp.stack([run, place]).astype(jnp.int32)
    inputs = dict(
        order=order, x_in=x.reshape(T // RUN, RUN, D), g_in=g[0], gains_in=packed, wq_in=wq, wk_in=wk, wv_in=wv, wo_in=wo,
        wg_in=wg, wu_in=wu, wd_in=wd, table_in=table,
    )
    TR_shape = ((TR, HD), F32)
    outputs = dict(
        layer_out=((T, D), BF), hidden_grad=((T, D), F32), q_out=((C, RW, H * HD), BF), kv_out=((C, RW, 2 * HD), BF), o_out=((OR, D), BF),
        gu_out=((C, RW, 2 * U), BF), down_out=((DR, D), BF), terms_out=TR_shape,
    )
    n1, n3 = D // (S * C), HD // (S * C)
    final = dict(
        layer_res=((T, D), BF), hidden_res=((T, D), F32), change1=((1, n1), F32),
        delta_query=((RW, C * H * HD), F32), delta_key=((RW, C * HD), F32), delta_value=((RW, C * HD), F32),
        changeq=((1, n3), F32), changek=((1, n3), F32), delta_out=((OR, D), F32), change2=((1, n1), F32),
        delta_gate=((RW, C * U), F32), delta_up=((RW, C * U), F32), delta_down=((DR, D), F32),
    )
    V, DMA = pltpu.VMEM, pltpu.SemaphoreType.DMA
    scratch = dict(
        x_all=V((L // RUN, RUN, D), BF), g_all=V((L, D), BF), h2_all=V((L, D), BF), dy_all=V((L, D), BF),
        h1=V((L, D), BF), w_qkv=V((D, AC), BF), w_o=V((H * HD, D), BF), w_gu=V((D, 2 * U), BF),
        w_d=V((U, D), BF), gains_all=V((C, 8, HD), F32), gains_z=V((S, C, HD), F32), table=V((L, HD), F32),
        cosine=V((L, HD), F32), sine=V((L, HD), F32), gain1=V((1, D), F32), gain2=V((1, D), F32),
        gainq=V((1, HD), F32), gaink=V((1, HD), F32), q_lin=V((H, L, HD), F32), k_lin=V((L, HD), F32),
        q_rot=V((H, L, HD), BF), k_rot=V((L, HD), BF), v=V((L, HD), BF), k_t=V((HD, L), BF),
        v_t=V((HD, L), BF), e=V((H, L, L), BF), l_inv=V((H, 8, L), F32), o_t=V((H, HD, L), F32),
        o_sorted=V((L // RUN, RUN, H * HD), BF), o=V((L, H * HD), BF), y1=V((T, D), F32), slope=V((L, U), F32), silu=V((L, U), F32),
        act=V((L, U), BF), d_gu=V((L, 2 * U), BF), d_y1=V((T, D), F32), d_o=V((L // RUN, RUN, H * HD), BF),
        d_o_sorted=V((L, H * HD), BF), do_t=V((H, HD, BLOCK), BF), do_l=V((H, BLOCK, HD), BF),
        d_k=V((L, HD), F32), d_v=V((L, HD), F32), d_qkv=V((L // RUN, RUN, AC), BF), sums=V((8, HD), F32),
        pair=V((CH, 2 * T, D), F32), s1=V((CH, T, D), BF), r1=V((2, CH, T, D), BF),
        s2=V((CH, T, D), BF), r2=V((2, 3, T, D), BF), s3=V((T, D), BF),
        g_q=V((D, H * HD), BF), g_kv=V((D, 2 * HD), BF), g_o=V((H * HD, D), BF), g_gu=V((D, 2 * U), BF), g_d=V((U, D), BF),
        t_q=V((2, PR, H * HD), BF), t_kv=V((2, PR, 2 * HD), BF), t_o=V((2, OR, D), BF), t_gu=V((2, PR, 2 * U), BF), t_d=V((2, DR, D), BF),
        c_q=V((2, PR, H * HD), BF), c_kv=V((2, PR, 2 * HD), BF), c_o=V((2, OR, D), BF), c_gu=V((2, PR, 2 * U), BF), c_d=V((2, DR, D), BF),
        z_o=V((S, OR, D), BF), y_out=V((T, D), BF), x_grad=V((T, D), F32), terms_all=V(*TR_shape),
        u_q=V((PR, H * HD), BF), u_kv=V((PR, 2 * HD), BF), u_o=V((OR, D), BF), u_gu=V((PR, 2 * U), BF), u_d=V((DR, D), BF),
        f_q=V((C, RW, H * HD), BF), f_kv=V((C, RW, 2 * HD), BF), h_o=V((S * OR, D), BF), f_gu=V((C, RW, 2 * U), BF), gu_own=V((C, RW, 2 * U), BF),
        wg_own=V((RW, C * U), BF), wu_own=V((RW, C * U), BF),
        terms=V((TR, HD), F32), terms_z=V((S, TR, HD), F32), terms_sum=V((TR, HD), F32),
        terms_p=V((C, TR, HD), F32),
        ag_send=DMA((4,)), ag_recv=DMA((4, C)), rs_send=DMA((4,)), r1_recv=DMA((4, CH)),
        r2_recv=DMA((4, 6)), z_send=DMA((6,)), z_recv=DMA((6, S)), gz_send=DMA((6,)),
        gz_recv=DMA((6, 2)), gc_recv=DMA((6, 2)), gp_send=DMA((3,)), gp_recv=DMA((3,)), u_send=DMA((1, S)),
        u_recv=DMA((1,)), w_send=DMA((2,)), w_recv=DMA((2,)), m_send=DMA((1, S)), m_recv=DMA((1,)),
        gain_send=DMA((2,)), gain_recv=DMA((S + 1,)), t_send=DMA((2,)), t_recv=DMA((2,)),
        local_sem=DMA((6,)), out_sem=DMA((8,)),
    )
    names = list(inputs) + list(outputs) + list(scratch)

    def kernel(*refs):
        layer_kernel(dims, types.SimpleNamespace(**dict(zip(names, refs))))

    in_specs = [
        pl.BlockSpec(memory_space=pltpu.SMEM if name == "order" else pl.ANY) for name in inputs
    ]
    results = pl.pallas_call(
        kernel,
        out_shape=[jax.ShapeDtypeStruct(*v) for v in outputs.values()],
        in_specs=in_specs,
        out_specs=[pl.BlockSpec(memory_space=pl.ANY)] * len(outputs),
        scratch_shapes=list(scratch.values()),
        compiler_params=pltpu.CompilerParams(
            collective_id=0, has_side_effects=True, vmem_limit_bytes=67043328
        ),
        name="layer",
    )(*inputs.values())
    n_in, n_out = len(outputs), len(final)

    def finish(*refs):
        parts = types.SimpleNamespace(
            far_in=refs[:n_in], far_out=refs[n_in : n_in + n_out],
            near_in=refs[n_in + n_out : 2 * n_in + n_out], near_out=refs[2 * n_in + n_out : -2],
            in_sem=refs[-2], out_sem=refs[-1],
        )
        finish_kernel(dims, list(outputs), list(final), parts)

    out = pl.pallas_call(
        finish,
        out_shape=[jax.ShapeDtypeStruct(*v) for v in final.values()],
        in_specs=[pl.BlockSpec(memory_space=pl.ANY)] * n_in,
        out_specs=[pl.BlockSpec(memory_space=pl.ANY)] * n_out,
        scratch_shapes=[V(*v) for v in outputs.values()]
        + [V((8, HD), F32) if k < 2 else V(*v) for k, v in enumerate(final.values())]
        + [DMA((n_in,)), DMA((n_out,))],
        name="finish",
    )(*results)
    one_axis = [k for k, v in enumerate(final.values()) if v[0][0] == 1]
    out = [o.reshape(-1) if k in one_axis else o for k, o in enumerate(out)]
    return (out[0][None], out[1][None], *out[2:])


def angles(places, head_size):
    half_size = head_size // 2
    frequency = jnp.power(THETA, -jnp.arange(half_size, dtype=F32) * (2.0 / head_size))
    phases = places.astype(F32)[:, None] * frequency[None, :]
    phases = jnp.concatenate([phases, phases], axis=-1)
    return (jnp.cos(phases), jnp.sin(phases))


def rotate(values, cosines, sines):
    half_size = values.shape[-1] // 2
    turned = jnp.concatenate([-values[..., half_size:], values[..., :half_size]], axis=-1)
    return values * cosines + turned * sines


def rotate_back(upstream, cosines, sines):
    half_size = upstream.shape[-1] // 2
    scaled = upstream * sines
    turned = jnp.concatenate([scaled[..., half_size:], -scaled[..., :half_size]], axis=-1)
    return upstream * cosines + turned


def dot(a, b):
    return jnp.dot(a, b, preferred_element_type=F32)


def local_of(mesh):
    seqs, ranks = mesh.shape["seq"], mesh.shape["ctx"]
    devices = seqs * ranks
    axes = ("seq", "ctx")

    def spread(shard, heads):
        rows, columns = shard.shape
        if heads and heads < ranks:
            blocks = shard.reshape(rows, heads, 1, columns // heads)
            blocks = jnp.broadcast_to(blocks, (rows, heads, ranks // heads, columns // heads))
            return blocks.reshape(rows, ranks, columns // heads)
        return shard.reshape(rows, ranks, columns // ranks)

    def fold(blocks, heads):
        rows, count, width = blocks.shape
        if heads and heads < ranks:
            return blocks.reshape(rows, heads, count // heads, width).sum(2).reshape(rows, heads * width)
        return blocks.reshape(rows, count * width)

    forth = [(seqs * r + j, j * ranks + r) for r in range(ranks) for j in range(seqs)]
    back = [(b, a) for a, b in forth]

    def local(
        hidden_states, positions, gain_first, weight_query, key_weight_matrix, value_weight_matrix,
        gain_query, gain_key, weight_output, gain_second, weight_gate, weight_up, weight_down,
        output_cotangent,
    ):
        tokens = hidden_states.shape[1]
        length = positions.shape[1]
        size = HEAD_DIMENSION
        group = QUERY_HEAD_COUNT // KEY_VALUE_HEADS
        my_q = QUERY_HEAD_COUNT // ranks
        my_k = max(1, KEY_VALUE_HEADS // ranks)
        scale = size ** (-0.5)
        places = positions[0]
        cosines, sines = angles(places, size)
        cosines, sines = cosines[:, None, :], sines[:, None, :]

        gains = jnp.concatenate([gain_first, gain_second, gain_query, gain_key])
        gains = lax.all_gather(gains, axes, axis=0).astype(F32)
        n1, n2, n3, n4 = (g.shape[0] for g in (gain_first, gain_second, gain_query, gain_key))
        first_scale = gains[:, :n1].reshape(-1)
        second_scale = gains[:, n1 : n1 + n2].reshape(-1)
        query_scale = gains[:, n1 + n2 : n1 + n2 + n3].reshape(-1)
        key_scale = gains[:, n1 + n2 + n3 :].reshape(-1)

        column_weights = jnp.concatenate(
            [
                spread(weight_query, 0),
                spread(key_weight_matrix, KEY_VALUE_HEADS),
                spread(value_weight_matrix, KEY_VALUE_HEADS),
                spread(weight_gate, 0),
                spread(weight_up, 0),
            ],
            axis=2,
        )
        column_weights = lax.all_to_all(column_weights, "ctx", split_axis=1, concat_axis=0, tiled=True)
        column_weights = lax.all_gather(column_weights[:, 0], "seq", axis=0, tiled=True)
        row_weights = jnp.concatenate([weight_output, weight_down], axis=0)
        row_weights = lax.all_gather(lax.ppermute(row_weights, axes, forth), "seq", axis=0)
        o_rows, d_rows = weight_output.shape[0], weight_down.shape[0]
        width = weight_output.shape[1]
        w_o = row_weights[:, :o_rows].reshape(-1, width)
        w_d = row_weights[:, o_rows:].reshape(-1, width)
        units = w_d.shape[0]
        attn_columns = (my_q + 2 * my_k) * size
        w_qkv = column_weights[:, :attn_columns]
        w_gu = column_weights[:, attn_columns:]

        x = lax.all_gather(hidden_states[0], "ctx", axis=0, tiled=True).astype(F32)
        g_low = lax.all_gather(output_cotangent[0], "ctx", axis=0, tiled=True)
        first_inverse = inverse_root(x)
        h1 = (x * first_inverse * first_scale).astype(BF)
        qkv = dot(h1, w_qkv)
        q_lin = qkv[:, : my_q * size].reshape(length, my_q, size)
        k_lin = qkv[:, my_q * size : (my_q + my_k) * size].reshape(length, my_k, size)
        v = qkv[:, (my_q + my_k) * size :].astype(BF).reshape(length, my_k, size)
        rq, rk = inverse_root(q_lin), inverse_root(k_lin)
        nq, nk = q_lin * rq, k_lin * rk
        qr = rotate(nq * query_scale, cosines, sines).astype(BF)
        kr = rotate(nk * key_scale, cosines, sines).astype(BF)
        mask = places[None, :] <= places[:, None]

        def scores(h):
            e = lax.dot_general(
                qr[:, h], kr[:, h // group], (((1,), (1,)), ((), ())), preferred_element_type=F32
            )
            return jnp.where(mask, e * scale, NEGATIVE)

        outs, probs = [], []
        for h in range(my_q):
            e = scores(h)
            p = jnp.exp(e - jnp.max(e, axis=-1, keepdims=True))
            p = p / jnp.sum(p, axis=-1, keepdims=True)
            probs.append(p)
            outs.append(dot(p.astype(BF), v[:, h // group]))
        o = jnp.concatenate(outs, axis=1).astype(BF)

        def scatter(part):
            return lax.psum_scatter(part.astype(BF), "ctx", scatter_dimension=0, tiled=True).astype(F32)

        x_own = hidden_states[0].astype(F32)
        y1 = x_own + scatter(dot(o, w_o))
        r2 = inverse_root(y1)
        second_normed = y1 * r2
        h2 = lax.all_gather((second_normed * second_scale).astype(BF), "ctx", axis=0, tiled=True)
        gu = dot(h2, w_gu)
        gate, up = gu[:, :units], gu[:, units:]
        sig = jax.nn.sigmoid(gate)
        silu = gate * sig
        act = (silu * up).astype(BF)
        layer_output = (y1 + scatter(dot(act, w_d))).astype(BF)

        d_act = dot(g_low, w_d.T)
        d_gate = (d_act * up * sig * (1.0 + gate * (1.0 - sig))).astype(BF)
        d_up = (d_act * silu).astype(BF)
        d_gu = jnp.concatenate([d_gate, d_up], axis=1)
        d_h2 = scatter(dot(d_gu, w_gu.T))
        second_term = jnp.sum(d_h2 * second_normed, axis=0)
        d_y1 = output_cotangent[0].astype(F32) + norm_backward(d_h2 * second_scale, second_normed, r2)
        d_y1_low = lax.all_gather(d_y1.astype(BF), "ctx", axis=0, tiled=True)
        d_o = dot(d_y1_low, w_o.T).astype(BF).reshape(length, my_q, size)

        d_q, d_k, d_v = [], [0.0] * my_k, [0.0] * my_k
        for h in range(my_q):
            p = probs[h]
            dp = lax.dot_general(
                d_o[:, h], v[:, h // group], (((1,), (1,)), ((), ())), preferred_element_type=F32
            )
            row = jnp.sum(p * dp, axis=-1, keepdims=True)
            de = (p * (dp - row) * scale).astype(BF)
            d_q.append(dot(de, kr[:, h // group]))
            d_k[h // group] += dot(de.T, qr[:, h])
            d_v[h // group] += dot(p.astype(BF).T, d_o[:, h])
        d_q, d_k, d_v = jnp.stack(d_q, 1), jnp.stack(d_k, 1), jnp.stack(d_v, 1)
        d_gq, d_gk = rotate_back(d_q, cosines, sines), rotate_back(d_k, cosines, sines)
        query_term = jnp.sum(d_gq * nq, axis=(0, 1))
        key_term = jnp.sum(d_gk * nk, axis=(0, 1))
        d_qlin = norm_backward(d_gq * query_scale, nq, rq).reshape(length, -1)
        d_klin = norm_backward(d_gk * key_scale, nk, rk).reshape(length, -1)
        d_qkv = jnp.concatenate([d_qlin, d_klin, d_v.reshape(length, -1)], axis=1).astype(BF)
        d_h1 = scatter(dot(d_qkv, w_qkv.T))
        r1 = inverse_root(x_own)
        first_normed = x_own * r1
        first_term = jnp.sum(d_h1 * first_normed, axis=0)
        hidden_gradient = d_y1 + norm_backward(d_h1 * first_scale, first_normed, r1)

        def rows_sum(part):
            part = lax.psum_scatter(part.astype(BF), "seq", scatter_dimension=0, tiled=True)
            return lax.ppermute(part, axes, back).astype(F32)

        delta_rows = jnp.concatenate(
            [dot(o.T, d_y1_low).reshape(seqs, o_rows, width), dot(act.T, g_low).reshape(seqs, d_rows, width)],
            axis=1,
        ).reshape(-1, width)
        delta_rows = rows_sum(delta_rows)
        delta_columns = jnp.concatenate([dot(h1.T, d_qkv), dot(h2.T, d_gu)], axis=1).astype(BF)
        delta_columns = lax.psum_scatter(delta_columns, "seq", scatter_dimension=0, tiled=True)
        own = delta_columns.shape[0] // ranks
        delta_columns = lax.all_to_all(
            delta_columns.reshape(ranks, own, -1), "ctx", split_axis=0, concat_axis=0, tiled=True
        )
        delta_columns = jnp.moveaxis(delta_columns, 0, 1).astype(F32)
        cuts = [my_q * size, (my_q + my_k) * size, (my_q + 2 * my_k) * size, attn_columns + units]
        parts = jnp.split(delta_columns, cuts, axis=2)
        delta_query = fold(parts[0], 0)
        delta_key = fold(parts[1], KEY_VALUE_HEADS)
        delta_value = fold(parts[2], KEY_VALUE_HEADS)
        delta_gate, delta_up = fold(parts[3], 0), fold(parts[4], 0)

        terms = lax.psum(jnp.concatenate([first_term, second_term, query_term, key_term]), axes)
        me = lax.axis_index("seq") * ranks + lax.axis_index("ctx")
        w = width

        def mine(start, n):
            return lax.dynamic_slice_in_dim(terms, start + me * n, n)

        return (
            layer_output[None],
            hidden_gradient[None],
            mine(0, n1),
            delta_query,
            delta_key,
            delta_value,
            mine(2 * w, n3),
            mine(2 * w + size, n4),
            delta_rows[:o_rows],
            mine(w, n2),
            delta_gate,
            delta_up,
            delta_rows[o_rows:],
        )

    return local


def solution(mesh):
    token = P("seq", "ctx", None)
    flat = P(("seq", "ctx"))
    rows = P(("seq", "ctx"), None)
    general = local_of(mesh)

    def body(*args):
        tokens, length = args[0].shape[1], args[1].shape[1]
        fits = (
            mesh.shape["ctx"] == KEY_VALUE_HEADS == 8
            and mesh.shape["seq"] == 4
            and length <= 1024
            and length % BLOCK == 0
            and tokens % RUN == 0
            and HEAD_DIMENSION % (mesh.shape["seq"] * mesh.shape["ctx"]) == 0
        )
        return fused_layer(mesh, args) if fits else general(*args)

    return jax.shard_map(
        body,
        mesh=mesh,
        in_specs=(token, P("seq", None), flat, rows, rows, rows, flat, flat, rows, flat, rows, rows, rows, token),
        out_specs=(token, token, flat, rows, rows, rows, flat, flat, rows, flat, rows, rows, rows),
        check_vma=False,
    )
```
